32 devices in a mesh: expert: 4 (over y, x), tensor: 4 (over z), rep: 2 (over core).
Axes of the slice: x: 2, y: 2, z: 4, core: 2. Of those that a mesh axis runs over, the one named last changes fastest.
Arguments:
- requests: bfloat16 [512, 1536], P('expert', ('tensor', 'rep')), may hold values from -6 to 6
- expert_ids: int32 [512, 2], P('expert'), may hold values from 0 to 3, all different within a row; in each aligned block of 128 rows (0 to 127, 128 to 255, ...) at most 96 rows name the same one
- gate_values: float32 [512, 2], P('expert'), may hold values from 0.2 to 1
- w_up: bfloat16 [4, 1536, 6144], P(None, 'expert', ('tensor', 'rep')), may hold values from -0.15625 to 0.15625
- w_down: bfloat16 [4, 1536, 6144], P(None, 'expert', ('tensor', 'rep')), may hold values from -0.078125 to 0.078125
- tower_in: bfloat16 [1536, 768], P(('tensor', 'rep')), may hold values from -0.15625 to 0.15625
- tower_bias: float32 [768], replicated, may hold values from -3 to 3
- tower_out: float32 [3, 256], replicated, may hold values from -0.375 to 0.375
- out_bias: float32 [3], replicated, may hold values from -3 to 3
Outputs:
- mixed: bfloat16 [512, 1536], P('expert', ('tensor', 'rep'))
- scores: float32 [3, 512], P(None, ('expert', 'tensor', 'rep'))
The draws below stay inside these ranges and needn't reach their ends.
Inputs may be any that keep to these rules, and one draw needn't show every extreme that they name: `expert_ids`: each row names two different experts. In the rows of one device (128 requests) no expert is named more than 96 times, a bound that some block reaches.
All inputs are finite; a program needn't handle non-finite values.
Results may differ from the reference program's by a relative error of at most 0.015.
Values may be sent and summed in bfloat16 or wider, within the bound.
A program may use at most 64 MiB of HBM per device.

```python
import math
import jax
import jax.numpy as jnp
import numpy as np
from jax import lax

D = 1536
HID = 6144
TH = 256
TASKS = 3
TOK_DEV = 128
EXPERTS = 4
CAP = 96
TOKENS = 512
N_TENSOR = 4
N_REP = 2


def block_scale(key, dims, shards, smallest, largest):
    def one(position, blocks):
        steps = jax.random.uniform(jax.random.fold_in(jax.random.fold_in(key, 6), position), (blocks,), jnp.float32, smallest / len(shards), largest / len(shards))
        return jnp.repeat(jnp.exp(steps), dims[position] // blocks).reshape((-1,) + (1,) * (len(dims) - position - 1))

    loudness = one(*shards[0])
    for cut in shards[1:]:
        loudness = loudness * one(*cut)
    return loudness


def assign_block(own_key, own, number, rows, number_of, top, bound, slope):
    order = jax.random.permutation(own_key, number_of)
    packed, common = shares(number_of, rows * top, bound, slope, True), shares(number_of, rows * top, bound, slope, False)
    places = jnp.arange(number_of)

    def named(sizes, turn):
        used = int((sizes > 0).sum())
        fixed = max(1, used // 4)
        moved = fixed + (places - fixed + turn * (used - fixed)) % max(1, number_of - fixed)
        return jnp.zeros((number_of,), jnp.int32).at[order[jnp.where(places < fixed, places, moved)]].set(jnp.asarray(sizes, jnp.int32))

    sizes = jnp.where(number % 4 == 0, named(packed, number // 4), named(common, number - number // 4 - 1))
    mixed = jax.random.permutation(jax.random.fold_in(own, 3), number_of)
    donor, receiver = mixed[0:number_of // 2 * 2:2], mixed[1:number_of // 2 * 2:2]
    room = jnp.minimum(sizes[donor] - 1, bound - sizes[receiver]) // 2
    room = jnp.where((donor == order[0]) | (receiver == order[0]) | (sizes[receiver] == 0), 0, jnp.maximum(room, 0))
    moved = jax.random.randint(jax.random.fold_in(own, 4), (number_of // 2,), 0, 1 << 20) % (room + 1)
    sizes = sizes.at[donor].add(-moved).at[receiver].add(moved)
    items = jnp.searchsorted(jnp.cumsum(sizes), jnp.arange(rows * top), side="right").astype(jnp.int32)
    table = items.reshape(top, rows).T
    table = table[jax.random.permutation(jax.random.fold_in(own, 1), rows)]
    turn = jax.random.randint(jax.random.fold_in(own, 2), (rows, 1), 0, top)
    return jnp.take_along_axis(table, (jnp.arange(top)[None, :] + turn) % top, axis=1)


def shares(number_of, total, most, slope, full):
    weights = [(1 << 20) // math.isqrt(standing ** slope) + 1 for standing in range(1, number_of + 1)]
    largest = most if full else min(most, max(-(-total // number_of), total * weights[0] // sum(weights)))
    least = 1 if total - largest >= number_of - 1 else 0
    holding, surplus = [largest] + [least] * (number_of - 1), total - largest - least * (number_of - 1)
    while surplus > 0:
        movable = [i for i in range(1, number_of) if holding[i] < largest] or [i for i in range(1, number_of) if holding[i] < most]
        mass, budget = sum([weights[i] for i in movable]), surplus
        for i in movable:
            extra = min(most - holding[i], max(1, budget * weights[i] // mass), surplus)
            holding[i] = holding[i] + extra
            surplus = surplus - extra
    return np.array(holding)


def normal_values(stream_key, extent, scale, reach, cuts=(), held_as=jnp.bfloat16):
    factor_of = block_scale(stream_key, extent, cuts, -0.22, 0.18) if cuts else 1.0
    values = jax.random.normal(stream_key, extent, jnp.float32) * scale * factor_of
    return jnp.minimum(jnp.maximum(values, -reach), reach).astype(held_as)


def setup_inputs(seed: int = 0) -> dict:
    key_list = jax.random.split(jax.random.key(seed), 10)
    requests = normal_values(key_list[0], (TOKENS, D), 1.0, 6.0, ((0, 4), (1, 8)))
    expert_ids_keys = jax.random.split(jax.random.fold_in(key_list[1], 1), TOKENS // TOK_DEV)
    expert_ids_turns = jax.random.permutation(jax.random.fold_in(key_list[1], 3), TOKENS // TOK_DEV)
    expert_ids = jax.vmap(lambda own, number: assign_block(jax.random.fold_in(key_list[1], 2), own, number, TOK_DEV, EXPERTS, 2, CAP, 2))(expert_ids_keys, expert_ids_turns).reshape((TOKENS, 2))
    gate_values = jnp.clip(0.2 + 0.8 * jax.random.uniform(key_list[2], (TOKENS, 2), jnp.float32) ** block_scale(key_list[2], (TOKENS, 2), ((0, 4),), -0.2, 0.2), 0.2, 1.0)
    w_up = normal_values(key_list[3], (EXPERTS, D, HID), D ** -0.5, 0.15625, ((1, 4), (2, 8)))
    w_down = normal_values(key_list[4], (EXPERTS, D, HID), HID ** -0.5, 0.078125, ((1, 4), (2, 8)))
    tower_in = normal_values(key_list[5], (D, TASKS * TH), D ** -0.5, 0.15625, ((0, 8),))
    tower_bias = normal_values(key_list[6], (TASKS * TH,), 0.5, 3.0, (), jnp.float32)
    tower_out = normal_values(key_list[7], (TASKS, TH), TH ** -0.5, 0.375, (), jnp.float32)
    out_bias = normal_values(key_list[8], (TASKS,), 1.0, 3.0, (), jnp.float32)
    return {"requests": requests, "expert_ids": expert_ids, "gate_values": gate_values, "w_up": w_up, "w_down": w_down, "tower_in": tower_in, "tower_bias": tower_bias, "tower_out": tower_out, "out_bias": out_bias}


def slot_table(expert_ids):
    blocks = expert_ids.reshape(-1, TOK_DEV * 2)
    onehot = (blocks[:, :, None] == jnp.arange(EXPERTS, dtype=jnp.int32)[None, None, :]).astype(jnp.int32)
    before = jnp.cumsum(onehot, axis=1) - onehot
    slot_rank = jnp.sum(before * onehot, axis=2)
    return (blocks * CAP + slot_rank).reshape(-1, 2)


def reference(requests, expert_ids, gate_values, w_up, w_down, tower_in, tower_bias, tower_out, out_bias):
    slots = slot_table(expert_ids)
    nblocks = TOKENS // TOK_DEV
    block_of = jnp.arange(TOKENS, dtype=jnp.int32) // TOK_DEV
    flat_index = (block_of[:, None] * (EXPERTS * CAP) + slots).astype(jnp.int32)
    dispatched = jnp.zeros((nblocks * EXPERTS * CAP, D), jnp.bfloat16)
    dispatched = dispatched.at[flat_index.reshape(-1)].set(jnp.repeat(requests, 2, axis=0))
    grouped = dispatched.reshape(nblocks, EXPERTS, CAP, D).transpose(1, 0, 2, 3).reshape(EXPERTS, nblocks * CAP, D)
    groups_hid = N_TENSOR * N_REP
    width = HID // groups_hid

    def expert_ffn(operands):
        rows, up_mat, down_mat = operands
        hidden = jax.nn.relu(jnp.dot(rows, up_mat, preferred_element_type=jnp.float32)).astype(jnp.bfloat16)
        total = jnp.zeros((rows.shape[0], D), jnp.float32)
        for group in range(groups_hid):
            part = jnp.dot(hidden[:, group * width:(group + 1) * width],
                           down_mat[:, group * width:(group + 1) * width].T,
                           preferred_element_type=jnp.float32)
            rounded = lax.optimization_barrier(part.astype(jnp.bfloat16))
            total = total + rounded.astype(jnp.float32)
        return total.astype(jnp.bfloat16)

    expert_out = lax.map(expert_ffn, (grouped, w_up, w_down))
    back = expert_out.reshape(EXPERTS, nblocks, CAP, D).transpose(1, 0, 2, 3).reshape(nblocks * EXPERTS * CAP, D)
    first = back[flat_index[:, 0]].astype(jnp.float32)
    second = back[flat_index[:, 1]].astype(jnp.float32)
    mixed = (gate_values[:, 0:1] * first + gate_values[:, 1:2] * second).astype(jnp.bfloat16)
    pre = jnp.dot(mixed, tower_in, preferred_element_type=jnp.float32) + tower_bias[None, :]
    active = jax.nn.relu(pre).reshape(TOKENS, TASKS, TH)
    logits = jnp.sum(active * tower_out[None, :, :], axis=2) + out_bias[None, :]
    scores = jax.nn.sigmoid(logits).T
    return mixed, scores
```

```python
import functools
import jax
import jax.numpy as jnp
from jax import lax
from jax.experimental import pallas as pl
from jax.experimental.pallas import tpu as pltpu
from jax.sharding import PartitionSpec as P

MESH = pl.DeviceIdType.MESH
CHUNKS = 4
F32 = jnp.float32
BF16 = jnp.bfloat16


def stay_kernel(
    dims, req_hbm, ids_hbm, gates_hbm, up_hbm, down_hbm, tin_hbm, bias_hbm, tout_hbm, ob_ref,
    mixed_ref, scores_ref,
    req_ref, ids_ref, gates_ref, bias_ref, tout_ref, up, down, tin, meta_ref, meta, xin, xs, hp, r1, s2, r2, hid, mine, dsend0, drecv0, dsend, gat, zrec,
    fsend, frecv, mixed_rows, lsem, me_s, me_r, x_s, x_r, q_s, q_r, s1_s, s1_r, s2_s, s2_r, h_s, h_r,
    p_s, p_r, g_s, g_r, z_s, z_r, f_s, f_r,
):
    nx, nt, nr, experts, tok, feat, hcols, tasks, th = dims
    xe, t, r = lax.axis_index("expert"), lax.axis_index("tensor"), lax.axis_index("rep")
    sub = tok // CHUNKS
    started = []

    def remote(src, dst, ssem, rsem, dev):
        return pltpu.make_async_remote_copy(
            src_ref=src, dst_ref=dst, send_sem=ssem, recv_sem=rsem, device_id=dev,
            device_id_type=MESH)

    def send(src, dst, ssem, rsem, dev):
        copy = remote(src, dst, ssem, rsem, dev)
        copy.start()
        started.append((None, copy))

    def send_if(cond, src, dst, ssem, rsem, dev):
        copy = remote(src, dst, ssem, rsem, dev)

        @pl.when(cond)
        def _():
            copy.start()
        started.append((cond, copy))

    def drain():
        for cond, copy in started:
            if cond is None:
                copy.wait_send()
            else:
                @pl.when(cond)
                def _(copy=copy):
                    copy.wait_send()
        started.clear()

    def got(ref, ssem, rsem):
        remote(ref, ref, ssem, rsem, (xe, t, r)).wait_recv()

    first = [
        pltpu.make_async_copy(req_hbm, req_ref, lsem.at[3]),
        pltpu.make_async_copy(ids_hbm, ids_ref, lsem.at[4]),
        pltpu.make_async_copy(gates_hbm, gates_ref, lsem.at[5]),
    ]
    loads = [
        pltpu.make_async_copy(up_hbm, up, lsem.at[0]),
        pltpu.make_async_copy(down_hbm, down, lsem.at[1]),
        pltpu.make_async_copy(tin_hbm, tin, lsem.at[2]),
        pltpu.make_async_copy(bias_hbm, bias_ref, lsem.at[6]),
        pltpu.make_async_copy(tout_hbm, tout_ref, lsem.at[7]),
    ]
    for load in first + loads:
        load.start()
    here = t == xe
    away = jnp.logical_not(here)
    partner = (xe, t, 1 - r)
    barrier = pltpu.get_barrier_semaphore()

    def greet(dev):
        pl.semaphore_signal(barrier, inc=1, device_id=dev, device_id_type=MESH)

    me = t * nr + r
    for d in range(1, nt * nr):
        other = me ^ d
        greet((xe, lax.div(other, nr), lax.rem(other, nr)))
    for d in range(1, nx):
        greet((xe ^ d, t, r))
    for b in range(nx):
        @pl.when(jnp.logical_not(jnp.logical_and(here, xe == b)))
        def _():
            greet((b, xe, r))
    for load in first:
        load.wait()
    meta_ref[...] = jnp.concatenate(
        [ids_ref[...].astype(F32), gates_ref[...], jnp.zeros((4, tok), F32)], axis=0)
    greeted = (nt * nr - 1) + (nx - 1) + nt

    with jax.named_scope("barr"):
        @pl.when(here)
        def _():
            pl.semaphore_wait(barrier, greeted - 1)

        @pl.when(away)
        def _():
            pl.semaphore_wait(barrier, greeted)

    def half(b, k):
        return xin.at[b, pl.ds(pl.multiple_of(k * feat, feat), feat)]

    for tt in reversed(range(nt)):
        send_if(jnp.logical_not(jnp.logical_and(here, t == tt)), req_ref, half(xe, r),
                x_s.at[tt], x_r.at[xe], (t, tt, r))
    for d in range(1, nx):
        send(meta_ref, meta.at[xe], me_s.at[d], me_r.at[xe], (xe ^ d, t, r))
    meta[xe] = meta_ref[...]

    @pl.when(here)
    def _():
        half(xe, r)[...] = req_ref[...]

    with jax.named_scope("xin"):
        for d in range(nx):
            b = xe ^ d
            if d == 0:
                @pl.when(away)
                def _():
                    got(half(b, r), x_s.at[0], x_r.at[b])
                send_if(here, req_ref, half(b, r), q_s.at[d], q_r.at[b], partner)
                send_if(away, half(b, r), half(b, r), q_s.at[d], q_r.at[b], partner)
            else:
                got(half(b, r), x_s.at[0], x_r.at[b])
                send(half(b, r), half(b, r), q_s.at[d], q_r.at[b], partner)
    with jax.named_scope("xpart"):
        for d in range(1, nx):
            got(meta.at[xe ^ d], me_s.at[0], me_r.at[xe ^ d])
        info = [meta[b].T for b in range(nx)]
        for d in range(nx):
            b = xe ^ d
            got(half(b, 1 - r), q_s.at[0], q_r.at[b])
            xs[b] = xin[b].T

    def column(c, j):
        return jnp.concatenate([info[b][c * sub:(c + 1) * sub, j:j + 1] for b in range(nx)], axis=0)

    loads[0].wait()
    quarter = xe
    near = (1, 2)
    def up_chunk(c):
        rows = xs[:, c * sub:(c + 1) * sub, :].reshape(nx * sub, nr * feat)
        ids = (column(c, 0), column(c, 1))
        for h in range(2):
            picked = [jnp.zeros((nx * sub, hcols), F32)] * 2
            for e in range(experts):
                part = jnp.dot(rows, up[e, :, h * hcols:(h + 1) * hcols], preferred_element_type=F32)
                picked = [jnp.where(ids[k] == float(e), part, picked[k]) for k in range(2)]
            for k in range(2):
                hp[c, h, :, k * sub:(k + 1) * sub, :] = picked[k].astype(BF16).reshape(nx, sub, hcols)
            fa, fb = near[h], near[1 - h]
            for i, q in enumerate((quarter ^ fa ^ fb, quarter ^ fa)):
                send(hp.at[c, h, q], r1.at[c, h, i], s1_s.at[c, h, i], s1_r.at[c, h, i],
                     (xe ^ fa, t, r))

    def reduce_first(c, h):
        fa, fb = near[h], near[1 - h]
        got(r1.at[c, h, 0], s1_s.at[c, h, 0], s1_r.at[c, h, 0])
        s2[c, h] = (hp[c, h, quarter ^ fb].astype(F32) + r1[c, h, 0].astype(F32)).astype(BF16)
        send(s2.at[c, h], r2.at[c, h], s2_s.at[c, h], s2_r.at[c, h], (xe ^ fb, t, r))

    def reduce_second(c, h):
        fa, fb = near[h], near[1 - h]
        got(r1.at[c, h, 1], s1_s.at[c, h, 1], s1_r.at[c, h, 1])
        got(r2.at[c, h], s2_s.at[c, h], s2_r.at[c, h])
        total = (hp[c, h, quarter].astype(F32) + r1[c, h, 1].astype(F32)) + r2[c, h].astype(F32)
        hid[c, h, quarter] = jnp.maximum(total, 0.0).astype(BF16)
        for i, f in enumerate((fb, fa)):
            send(hid.at[c, h, quarter], hid.at[c, h, quarter], h_s.at[c, h, i],
                 h_r.at[c, h, quarter], (xe ^ f, t, r))

    def forward(c, h):
        fa, fb = near[h], near[1 - h]
        q = quarter ^ fb
        got(hid.at[c, h, q], h_s.at[c, h, 2], h_r.at[c, h, q])
        send(hid.at[c, h, q], hid.at[c, h, q], h_s.at[c, h, 2], h_r.at[c, h, q], (xe ^ fa, t, r))

    def collect(c, h):
        fa, fb = near[h], near[1 - h]
        for q in (quarter ^ fa, quarter ^ fa ^ fb):
            got(hid.at[c, h, q], h_s.at[c, h, 2], h_r.at[c, h, q])

    def down_chunk(c):
        ids = (column(c, 0), column(c, 1))
        gates = (column(c, 2), column(c, 3))
        total = jnp.zeros((nx * sub, nr * feat), F32)
        for e in range(experts):
            hit = (ids[0] == float(e), ids[1] == float(e))
            weight = jnp.where(hit[0], gates[0], 0.0) + jnp.where(hit[1], gates[1], 0.0)
            part = None
            for h in range(2):
                values = [hid[c, h, :, k * sub:(k + 1) * sub, :].reshape(nx * sub, hcols)
                          for k in range(2)]
                chosen = jnp.where(hit[0], values[0], jnp.where(hit[1], values[1], jnp.zeros_like(values[1])))
                one = lax.dot_general(chosen, down[e, :, h * hcols:(h + 1) * hcols],
                                      (((1,), (1,)), ((), ())), preferred_element_type=F32)
                part = one if part is None else part + one
            total = total + weight * part
        low, high = total[:, :feat], total[:, feat:]
        mine[c] = jnp.where(r == 0, low, high).reshape(nx, sub, feat)
        dsend0[c] = jnp.where(r == 0, high, low).astype(BF16).reshape(nx, sub, feat)
        send(dsend0.at[c], drecv0.at[c], p_s.at[c], p_r.at[c], partner)

    def pair_chunk(c):
        got(drecv0.at[c], p_s.at[c], p_r.at[c])
        dsend[c] = (mine[c] + drecv0[c].astype(F32)).astype(BF16)
        for d in (3, 1, 2):
            send(dsend.at[c, xe ^ d], gat.at[c, xe], g_s.at[c, d], g_r.at[c, xe], (xe ^ d, t, r))
        gat[c, xe] = dsend[c, xe]
        send_if(away, dsend.at[c, xe], zrec.at[c, t], z_s.at[c, 0], z_r.at[c, t], (xe, xe, r))

    def pass_chunk(c):
        for d in (1, 2, 3):
            q = xe ^ d
            got(gat.at[c, q], g_s.at[c, 0], g_r.at[c, q])
            send_if(q != t, gat.at[c, q], zrec.at[c, t], z_s.at[c, d], z_r.at[c, t], (xe, q, r))

    def mixed_chunk(c):
        total = gat[c, t].astype(F32)
        for d in range(1, nt):
            src = t ^ d
            got(zrec.at[c, src], z_s.at[c, 0], z_r.at[c, src])
            total = total + zrec[c, src].astype(F32)
        value = total.astype(BF16)
        mixed_rows[c * sub:(c + 1) * sub, :] = value
        part = jnp.dot(value, tin[...], preferred_element_type=F32).astype(BF16)
        each = tok // (nt * nr)
        per = sub // each
        fsend[c * per:(c + 1) * per] = part.reshape(per, each, part.shape[1])
        for to in range(c * per, (c + 1) * per):
            send_if(me != to, fsend.at[to], frecv.at[me], f_s.at[to], f_r.at[me],
                    (xe, to // nr, to % nr))

    def both(stage, c):
        for h in range(2):
            stage(c, h)

    def one(stage, c):
        stage(c)

    stages = (
        ("fw", both, forward, 4), ("rb", both, reduce_second, 3), ("ra", both, reduce_first, 2),
        ("up", one, up_chunk, 0), ("co", both, collect, 5), ("dn", one, down_chunk, 5),
        ("ps", one, pass_chunk, 6), ("pr", one, pair_chunk, 5), ("mx", one, mixed_chunk, 7),
    )
    for i in range(CHUNKS + 7):
        if i == 5:
            for load in loads[1:]:
                load.wait()
        if i == CHUNKS + 6:
            with jax.named_scope("drain"):
                drain()
        for name, kind, stage, lag in stages:
            if 0 <= i - lag < CHUNKS:
                with jax.named_scope(f"{name}{i - lag}"):
                    kind(stage, i - lag)
    mixed_ref[...] = mixed_rows[...].T
    with jax.named_scope("fin"):
        pre = fsend[me].astype(F32)
        for d in range(1, nt * nr):
            frm = me ^ d
            got(frecv.at[frm], f_s.at[0], f_r.at[frm])
            pre = pre + frecv[frm].astype(F32)
    active = jnp.maximum(pre + bias_ref[...].reshape(1, tasks * th), 0.0)
    outs = []
    for j in range(tasks):
        outs.append(jnp.sum(active[:, j * th:(j + 1) * th] * tout_ref[j:j + 1, :], axis=1, keepdims=True))
    each = pre.shape[0]
    lane = lax.broadcasted_iota(jnp.int32, (each, 128), 1)
    logits = jnp.zeros((each, 128), F32)
    for j in range(tasks):
        logits = jnp.where(lane == j, outs[j] + ob_ref[j], logits)
    scores_ref[...] = jax.nn.sigmoid(logits.T[:tasks, :])
    with jax.named_scope("end"):
        drain()


def stay_device(requests, expert_ids, gate_values, w_up, w_down, tower_in, tower_bias, tower_out,
                out_bias):
    nx, nt, nr = lax.axis_size("expert"), lax.axis_size("tensor"), lax.axis_size("rep")
    experts, _, hid_cols = w_up.shape
    tok, feat = requests.shape
    tasks, th = tower_out.shape
    hcols = hid_cols // 2
    sub = tok // CHUNKS
    each = tok // (nt * nr)
    dims = (nx, nt, nr, experts, tok, feat, hcols, tasks, th)
    vmem = pl.BlockSpec(memory_space=pltpu.VMEM)
    hbm = pl.BlockSpec(memory_space=pltpu.HBM)
    smem = pl.BlockSpec(memory_space=pltpu.SMEM)
    dma = pltpu.SemaphoreType.DMA
    C = CHUNKS
    scratch = [
        pltpu.VMEM((feat, tok), BF16), pltpu.VMEM((2, tok), jnp.int32), pltpu.VMEM((2, tok), F32),
        pltpu.VMEM(tower_bias.shape, F32), pltpu.VMEM(tower_out.shape, F32),
        pltpu.VMEM(w_up.shape, BF16), pltpu.VMEM(w_down.shape, BF16),
        pltpu.VMEM(tower_in.shape, BF16),
        pltpu.VMEM((8, tok), F32), pltpu.VMEM((nx, 8, tok), F32),
        pltpu.VMEM((nx, nr * feat, tok), BF16), pltpu.VMEM((nx, tok, nr * feat), BF16),
        pltpu.VMEM((C, 2, nx, 2 * sub, hcols), BF16),
        pltpu.VMEM((C, 2, 2, 2 * sub, hcols), BF16),
        pltpu.VMEM((C, 2, 2 * sub, hcols), BF16), pltpu.VMEM((C, 2, 2 * sub, hcols), BF16),
        pltpu.VMEM((C, 2, nx, 2 * sub, hcols), BF16),
        pltpu.VMEM((C, nx, sub, feat), F32), pltpu.VMEM((C, nx, sub, feat), BF16),
        pltpu.VMEM((C, nx, sub, feat), BF16), pltpu.VMEM((C, nx, sub, feat), BF16),
        pltpu.VMEM((C, nx, sub, feat), BF16), pltpu.VMEM((C, nt, sub, feat), BF16),
        pltpu.VMEM((nt * nr, each, tasks * th), BF16), pltpu.VMEM((nt * nr, each, tasks * th), BF16),
        pltpu.VMEM((tok, feat), BF16),
        dma((8,)), dma((nx,)), dma((nx,)), dma((nt,)), dma((nx,)), dma((nx,)), dma((nx,)),
        dma((C, 2, 2)), dma((C, 2, 2)), dma((C, 2)), dma((C, 2)), dma((C, 2, 3)), dma((C, 2, nx)),
        dma((C,)), dma((C,)), dma((C, nx)), dma((C, nx)), dma((C, nx)), dma((C, nt)),
        dma((nt * nr,)), dma((nt * nr,)),
    ]
    mixed, scores = pl.pallas_call(
        functools.partial(stay_kernel, dims),
        out_shape=(pltpu.VMEM((feat, tok), BF16), pltpu.VMEM((tasks, each), F32)),
        in_specs=[hbm] * 8 + [smem],
        out_specs=(vmem, vmem),
        scratch_shapes=scratch,
        compiler_params=pltpu.CompilerParams(
            has_side_effects=True, collective_id=0, vmem_limit_bytes=60 << 20),
        name="stay",
    )(requests.T, expert_ids.T, gate_values.T, w_up, w_down, tower_in, tower_bias, tower_out, out_bias)
    return mixed.T, scores


def weights_stay(mesh):
    return mesh.shape["expert"] == 4 and mesh.shape["tensor"] == 4 and mesh.shape["rep"] == 2


def tower_head(pre, tower_bias, tower_out, out_bias):
    active = jax.nn.relu(pre + tower_bias[None, :])
    active = active.reshape(pre.shape[0], tower_out.shape[0], tower_out.shape[1])
    logits = jnp.sum(active * tower_out[None, :, :], axis=2) + out_bias[None, :]
    return jax.nn.sigmoid(logits).T


def per_device(
    requests, expert_ids, gate_values, w_up, w_down, tower_in, tower_bias, tower_out, out_bias
):
    groups = lax.axis_size("expert")
    experts = w_up.shape[0]
    local_experts = experts // groups
    tok_rows = requests.shape[0]
    capacity = 3 * tok_rows // experts
    serve_up, serve_down = (
        lax.all_to_all(w_up, "expert", split_axis=0, concat_axis=1, tiled=True),
        lax.all_to_all(w_down, "expert", split_axis=0, concat_axis=1, tiled=True),
    )
    flat_ids = expert_ids.reshape(-1)
    onehot = (flat_ids[:, None] == jnp.arange(experts, dtype=jnp.int32)[None, :]).astype(jnp.int32)
    before = jnp.cumsum(onehot, axis=0) - onehot
    slot_rank = jnp.sum(before * onehot, axis=1)
    slots = (flat_ids * capacity + slot_rank).reshape(tok_rows, 2)
    slot_index = jnp.arange(experts * capacity, dtype=jnp.int32)
    spread = (
        (slot_index[:, None] == slots[None, :, 0]) | (slot_index[:, None] == slots[None, :, 1])
    ).astype(jnp.bfloat16)
    full_rows = lax.all_gather(requests, ("tensor", "rep"), axis=1, tiled=True)
    outgoing = jnp.dot(spread, full_rows, preferred_element_type=jnp.float32).astype(jnp.bfloat16)
    incoming = lax.all_to_all(outgoing, "expert", split_axis=0, concat_axis=0, tiled=True)
    shaped = incoming.reshape(groups, local_experts, capacity, incoming.shape[1])
    hidden_pre = jnp.einsum("secd,edh->sech", shaped, serve_up, preferred_element_type=jnp.float32)
    hidden = jax.nn.relu(hidden_pre).astype(jnp.bfloat16)
    partial_value = jnp.einsum(
        "sech,edh->secd", hidden, serve_down, preferred_element_type=jnp.float32
    )
    summed = lax.psum_scatter(
        partial_value.astype(jnp.bfloat16), ("tensor", "rep"), scatter_dimension=3, tiled=True
    ).astype(jnp.float32)
    expert_out = summed.astype(jnp.bfloat16).reshape(
        groups * local_experts * capacity, summed.shape[3]
    )
    returned = lax.all_to_all(expert_out, "expert", split_axis=0, concat_axis=0, tiled=True)
    pick_first = (slots[:, 0:1] == slot_index[None, :]).astype(jnp.bfloat16)
    pick_second = (slots[:, 1:2] == slot_index[None, :]).astype(jnp.bfloat16)
    first = jnp.dot(pick_first, returned, preferred_element_type=jnp.float32)
    second = jnp.dot(pick_second, returned, preferred_element_type=jnp.float32)
    mixed = (gate_values[:, 0:1] * first + gate_values[:, 1:2] * second).astype(jnp.bfloat16)
    pre = lax.psum_scatter(
        jnp.dot(mixed, tower_in, preferred_element_type=jnp.float32).astype(jnp.bfloat16),
        ("tensor", "rep"),
        scatter_dimension=0,
        tiled=True,
    ).astype(jnp.float32)
    scores = tower_head(pre, tower_bias, tower_out, out_bias)
    return (mixed, scores)


def solution(mesh):
    in_specs = (
        P("expert", ("tensor", "rep")),
        P("expert", None),
        P("expert", None),
        P(None, "expert", ("tensor", "rep")),
        P(None, "expert", ("tensor", "rep")),
        P(("tensor", "rep"), None),
        P(),
        P(),
        P(),
    )
    out_specs = (P("expert", ("tensor", "rep")), P(None, ("expert", "tensor", "rep")))
    body = stay_device if weights_stay(mesh) else per_device
    return jax.shard_map(
        body, mesh=mesh, in_specs=in_specs, out_specs=out_specs, check_vma=False
    )
```

```python
import functools
import jax
import jax.numpy as jnp
from jax import lax
from jax.experimental import pallas as pl
from jax.experimental.pallas import tpu as pltpu
from jax.sharding import PartitionSpec as P

MESH = pl.DeviceIdType.MESH
F32 = jnp.float32
BF16 = jnp.bfloat16


def stay_kernel(
    dims, req_hbm, ids_hbm, gates_hbm, up_hbm, down_hbm, tin_hbm, bias_hbm, tout_hbm, ob_ref,
    mixed_ref, scores_ref,
    req_ref, ids_ref, gates_ref, bias_ref, tout_ref, up, down, tin, meta_ref, meta, rt, xs,
    hp, r1, s2, r2, hid, mine, dsend0, drecv0, dsend, gat, zrec, fsend, frecv, rows_out,
    lsem, me_s, me_r, x_s, x_r, q_s, q_r, s1_s, s1_r, s2_s, s2_r, h_s, h_r,
    p_s, p_r, g_s, g_r, z_s, z_r, m_s, m_r, t_s, t_r, f_s, f_r,
):
    nx, nt, nr, experts, tok, feat, hcols, tasks, th, unit, sizes = dims
    xe, t, r = lax.axis_index("expert"), lax.axis_index("tensor"), lax.axis_index("rep")
    chunks = len(sizes)
    offs = [sum(sizes[:c]) * unit for c in range(chunks)]
    subs = [n * unit for n in sizes]

    def remote(src, dst, ssem, rsem, dev):
        return pltpu.make_async_remote_copy(
            src_ref=src, dst_ref=dst, send_sem=ssem, recv_sem=rsem, device_id=dev,
            device_id_type=MESH)

    def send(src, dst, ssem, rsem, dev):
        remote(src, dst, ssem, rsem, dev).start()

    def got(ref, rsem):
        remote(ref, ref, lsem.at[0], rsem, (xe, t, r)).wait_recv()

    def sent(ref, ssem):
        remote(ref, ref, ssem, lsem.at[0], (xe, t, r)).wait_send()

    first = [
        pltpu.make_async_copy(req_hbm, req_ref, lsem.at[3]),
        pltpu.make_async_copy(ids_hbm, ids_ref, lsem.at[4]),
        pltpu.make_async_copy(gates_hbm, gates_ref, lsem.at[5]),
    ]

    def own_rows(ref, k):
        return ref.at[pl.ds(pl.multiple_of(k * feat, feat), feat)]

    loads = [
        pltpu.make_async_copy(up_hbm, up, lsem.at[0]),
        pltpu.make_async_copy(down_hbm, down, lsem.at[1]),
        pltpu.make_async_copy(tin_hbm, own_rows(tin, r), lsem.at[2]),
        pltpu.make_async_copy(bias_hbm, bias_ref, lsem.at[6]),
        pltpu.make_async_copy(tout_hbm, tout_ref, lsem.at[7]),
    ]
    for load in first + loads:
        load.start()
    here = t == xe
    away = jnp.logical_not(here)
    partner = (xe, t, 1 - r)
    barrier = pltpu.get_barrier_semaphore()

    def greet(dev):
        pl.semaphore_signal(barrier, inc=1, device_id=dev, device_id_type=MESH)

    me = t * nr + r
    for d in range(1, nt * nr):
        other = me ^ d
        greet((xe, lax.div(other, nr), lax.rem(other, nr)))
    for d in range(1, nx):
        greet((xe ^ d, t, r))
    for b in range(nx):
        @pl.when(jnp.logical_not(jnp.logical_and(here, xe == b)))
        def _():
            greet((b, xe, r))
    for load in first:
        load.wait()
    rt[...] = req_ref[...].T
    meta_ref[...] = jnp.concatenate(
        [ids_ref[...].astype(F32), gates_ref[...], jnp.zeros((4, tok), F32)], axis=0)
    greeted = (nt * nr - 1) + (nx - 1) + nt

    with jax.named_scope("barr"):
        @pl.when(here)
        def _():
            pl.semaphore_wait(barrier, greeted - 1)

        @pl.when(away)
        def _():
            pl.semaphore_wait(barrier, greeted)

    def span(c):
        return pl.ds(offs[c], subs[c])

    for c in range(chunks):
        for tt in reversed(range(nt)):
            @pl.when(jnp.logical_not(jnp.logical_and(here, t == tt)))
            def _():
                send(rt.at[span(c)], xs.at[r, xe, span(c)], x_s, x_r.at[c], (t, tt, r))
        if c == 0:
            for d in range(1, nx):
                send(meta_ref, meta.at[xe], me_s, me_r, (xe ^ d, t, r))
    send(tin_hbm, own_rows(tin, r), t_s, t_r, partner)
    meta[xe] = meta_ref[...]

    @pl.when(here)
    def _():
        xs[r, xe] = rt[...]

    def take(c):
        @pl.when(here)
        def _():
            got(xs.at[r, pl.ds(0, nx - 1), span(c)], x_r.at[c])

        @pl.when(away)
        def _():
            got(xs.at[r, :, span(c)], x_r.at[c])
        send(xs.at[r, :, span(c)], xs.at[r, :, span(c)], q_s, q_r.at[c], partner)

    with jax.named_scope("take0"):
        take(0)
    with jax.named_scope("meta"):
        got(meta.at[pl.ds(0, nx - 1)], me_r)
        info = [meta[b].T for b in range(nx)]

    def column(c, j):
        return jnp.concatenate(
            [info[b][offs[c]:offs[c] + subs[c], j:j + 1] for b in range(nx)], axis=0)

    near = (1, 2)

    def picks(c, k=None):
        if k is None:
            return pl.ds(2 * offs[c], 2 * subs[c])
        return pl.ds(2 * offs[c] + k * subs[c], subs[c])

    def up_chunk(c):
        sub = subs[c]
        if c + 1 < chunks:
            take(c + 1)
        got(xs.at[1 - r, :, span(c)], q_r.at[c])
        if c == 0:
            loads[0].wait()
        rows = [xs[k, :, offs[c]:offs[c] + sub, :].reshape(nx * sub, feat) for k in range(nr)]
        ids = (column(c, 0), column(c, 1))
        for h in range(2):
            picked = [jnp.zeros((nx * sub, hcols), F32)] * 2
            for e in range(experts):
                part = None
                for k in range(nr):
                    one = jnp.dot(rows[k], up[e, k * feat:(k + 1) * feat, h * hcols:(h + 1) * hcols],
                                  preferred_element_type=F32)
                    part = one if part is None else part + one
                picked = [jnp.where(ids[k] == float(e), part, picked[k]) for k in range(2)]
            for k in range(2):
                hp[h, :, picks(c, k), :] = picked[k].astype(BF16).reshape(nx, sub, hcols)
            fa, fb = near[h], near[1 - h]
            for i, q in enumerate((xe ^ fa ^ fb, xe ^ fa)):
                send(hp.at[h, q, picks(c)], r1.at[h, i, picks(c)], s1_s, s1_r.at[c, h, i],
                     (xe ^ fa, t, r))

    def reduce_first(c, h):
        fa, fb = near[h], near[1 - h]
        got(r1.at[h, 0, picks(c)], s1_r.at[c, h, 0])
        s2[h, picks(c)] = (hp[h, xe ^ fb, picks(c)].astype(F32)
                           + r1[h, 0, picks(c)].astype(F32)).astype(BF16)
        send(s2.at[h, picks(c)], r2.at[h, picks(c)], s2_s, s2_r.at[c, h], (xe ^ fb, t, r))

    def reduce_second(c, h):
        fa, fb = near[h], near[1 - h]
        got(r1.at[h, 1, picks(c)], s1_r.at[c, h, 1])
        got(r2.at[h, picks(c)], s2_r.at[c, h])
        total = (hp[h, xe, picks(c)].astype(F32) + r1[h, 1, picks(c)].astype(F32)
                 + r2[h, picks(c)].astype(F32))
        hid[h, xe, picks(c)] = jnp.maximum(total, 0.0).astype(BF16)
        mine_ref = hid.at[h, xe, picks(c)]
        send(mine_ref, mine_ref, h_s.at[0], h_r.at[c, h, 0], (xe ^ fb, t, r))
        send(mine_ref, mine_ref, h_s.at[0], h_r.at[c, h, 1], (xe ^ fa, t, r))

    def forward(c, h):
        fa, fb = near[h], near[1 - h]
        ref = hid.at[h, xe ^ fb, picks(c)]
        got(ref, h_r.at[c, h, 0])
        send(ref, ref, h_s.at[1], h_r.at[c, h, 2], (xe ^ fa, t, r))

    def collect(c, h):
        fa, fb = near[h], near[1 - h]
        got(hid.at[h, xe ^ fa, picks(c)], h_r.at[c, h, 1])
        got(hid.at[h, xe ^ fa ^ fb, picks(c)], h_r.at[c, h, 2])

    def parity(c):
        return sum(sizes[:c]) % nr if sizes[c] == 1 else None

    def slot(c, core):
        return (sum(sizes[:c]) + (sizes[c] - 1 if sizes[c] > 1 else 0)) // nr - (
            core if sizes[c] > 1 else 0)

    def if_core(c, other, body):
        p = parity(c)
        if p is None:
            body()
        else:
            pl.when(r == (1 - p if other else p))(body)

    def down_chunk(c):
        sub = subs[c]
        ids = (column(c, 0), column(c, 1))
        gates = (column(c, 2), column(c, 3))
        total = jnp.zeros((nx * sub, nr * feat), F32)
        for e in range(experts):
            hit = (ids[0] == float(e), ids[1] == float(e))
            weight = jnp.where(hit[0], gates[0], 0.0) + jnp.where(hit[1], gates[1], 0.0)
            part = None
            for h in range(2):
                values = [hid[h, :, picks(c, k), :].reshape(nx * sub, hcols) for k in range(2)]
                chosen = jnp.where(hit[0], values[0], jnp.where(hit[1], values[1], jnp.zeros_like(values[1])))
                one = lax.dot_general(chosen, down[e, :, h * hcols:(h + 1) * hcols],
                                      (((1,), (1,)), ((), ())), preferred_element_type=F32)
                part = one if part is None else part + one
            total = total + weight * part
        total = total.reshape(nx, sub, nr * feat)
        if sizes[c] == 1:
            keep = give = total
        else:
            odd, even = total[:, :unit], total[:, unit:]
            keep = jnp.where(r == 0, even, odd)
            give = jnp.where(r == 0, odd, even)

        def store():
            mine[slot(c, r)] = keep

        def give_away():
            at = slot(c, 1 - r)
            dsend0[c] = give.astype(BF16)
            send(dsend0.at[c], drecv0.at[at], p_s, p_r.at[at], partner)
        if_core(c, True, give_away)
        if_core(c, False, store)

    def pair_chunk(c):
        def body():
            s = slot(c, r)
            got(drecv0.at[s], p_r.at[s])
            dsend[s] = (mine[s] + drecv0[s].astype(F32)).astype(BF16)
            for d in (3, 1, 2):
                send(dsend.at[s, xe ^ d], gat.at[s, xe], g_s, g_r.at[s, d - 1], (xe ^ d, t, r))
            gat[s, xe] = dsend[s, xe]

            @pl.when(away)
            def _():
                send(dsend.at[s, xe], zrec.at[s, t], z_s, z_r.at[s], (xe, xe, r))
        if_core(c, False, body)

    def pass_chunk(c):
        def body():
            s = slot(c, r)
            for d in (1, 2, 3):
                q = xe ^ d
                got(gat.at[s, q], g_r.at[s, d - 1])

                @pl.when(q != t)
                def _():
                    send(gat.at[s, q], zrec.at[s, t], z_s, z_r.at[s], (xe, q, r))
        if_core(c, False, body)

    def mixed_chunk(c):
        def body():
            s = slot(c, r)
            got(zrec.at[s, pl.ds(0, nt - 1)], z_r.at[s])
            total = gat[s, t].astype(F32)
            for d in range(1, nt):
                total = total + zrec[s, t ^ d].astype(F32)
            value = total.astype(BF16)
            at = pl.ds(pl.multiple_of((s * nr + r) * unit, unit), unit)
            rows_out[at, :] = value
            send(rows_out.at[at], rows_out.at[at], m_s, m_r, partner)
            fsend[s] = jnp.dot(value, tin[...], preferred_element_type=F32).astype(BF16)

            @pl.when(t != s)
            def _():
                send(fsend.at[s], frecv.at[t], f_s, f_r, (xe, s, r))
        if_core(c, False, body)

    def both(stage, c):
        for h in range(2):
            stage(c, h)

    def one(stage, c):
        stage(c)

    stages = (
        ("fw", both, forward, 4), ("rb", both, reduce_second, 3), ("ra", both, reduce_first, 2),
        ("up", one, up_chunk, 0), ("co", both, collect, 5), ("dn", one, down_chunk, 5),
        ("ps", one, pass_chunk, 6), ("pr", one, pair_chunk, 5), ("mx", one, mixed_chunk, 7),
    )
    for i in range(chunks + 7):
        if i == 5:
            for load in loads[1:]:
                load.wait()
            got(own_rows(tin, 1 - r), t_r)
        if i == chunks + 6:
            with jax.named_scope("drain"):
                sent(r1, s1_s)
                sent(r2, s2_s)
                sent(r1, h_s.at[0])
                sent(r2, h_s.at[1])
                sent(meta.at[pl.ds(0, nx - 1)], me_s)
                sent(own_rows(tin, r), t_s)
                sent(xs.at[r], q_s)
                sent(drecv0, p_s)
                sent(gat.at[:, pl.ds(0, nx - 1)], g_s)

                @pl.when(here)
                def _():
                    sent(xs.at[r, pl.ds(0, nx - 1)], x_s)

                @pl.when(away)
                def _():
                    sent(xs.at[r], x_s)
        for name, kind, stage, lag in stages:
            if 0 <= i - lag < chunks:
                with jax.named_scope(f"{name}{i - lag}"):
                    kind(stage, i - lag)
    half = tok // nr
    with jax.named_scope("mout"):
        got(rows_out.at[pl.ds(0, half)], m_r)
    out = rows_out[...].T
    mixed_ref[...] = jnp.where(r == 0, out[:feat], out[feat:])
    with jax.named_scope("fin"):
        got(frecv.at[pl.ds(0, nt - 1)], f_r)
        pre = fsend[t].astype(F32)
        for d in range(1, nt):
            pre = pre + frecv[t ^ d].astype(F32)
    active = jnp.maximum(pre + bias_ref[...].reshape(1, tasks * th), 0.0)
    outs = []
    for j in range(tasks):
        outs.append(jnp.sum(active[:, j * th:(j + 1) * th] * tout_ref[j:j + 1, :], axis=1, keepdims=True))
    lane = lax.broadcasted_iota(jnp.int32, (unit, 128), 1)
    logits = jnp.zeros((unit, 128), F32)
    for j in range(tasks):
        logits = jnp.where(lane == j, outs[j] + ob_ref[j], logits)
    scores_ref[...] = jax.nn.sigmoid(logits.T[:tasks, :])
    with jax.named_scope("end"):
        sent(zrec.at[:, pl.ds(0, nt - 1)], z_s)
        sent(rows_out.at[pl.ds(0, half)], m_s)
        sent(frecv.at[pl.ds(0, nt - 1)], f_s)


def stay_device(requests, expert_ids, gate_values, w_up, w_down, tower_in, tower_bias, tower_out,
                out_bias):
    nx, nt, nr = lax.axis_size("expert"), lax.axis_size("tensor"), lax.axis_size("rep")
    experts, _, hid_cols = w_up.shape
    tok, feat = requests.shape
    tasks, th = tower_out.shape
    hcols = hid_cols // 2
    unit = tok // (nt * nr)
    sizes = (1,) + (nr,) * (nt - 1) + (1,)
    C = len(sizes)
    dims = (nx, nt, nr, experts, tok, feat, hcols, tasks, th, unit, sizes)
    vmem = pl.BlockSpec(memory_space=pltpu.VMEM)
    hbm = pl.BlockSpec(memory_space=pltpu.HBM)
    smem = pl.BlockSpec(memory_space=pltpu.SMEM)
    dma = pltpu.SemaphoreType.DMA
    wide = nr * feat
    scratch = [
        pltpu.VMEM((feat, tok), BF16), pltpu.VMEM((2, tok), jnp.int32), pltpu.VMEM((2, tok), F32),
        pltpu.VMEM(tower_bias.shape, F32), pltpu.VMEM(tower_out.shape, F32),
        pltpu.VMEM(w_up.shape, BF16), pltpu.VMEM(w_down.shape, BF16),
        pltpu.VMEM((wide, tower_in.shape[1]), BF16),
        pltpu.VMEM((8, tok), F32), pltpu.VMEM((nx, 8, tok), F32),
        pltpu.VMEM((tok, feat), BF16), pltpu.VMEM((nr, nx, tok, feat), BF16),
        pltpu.VMEM((2, nx, 2 * tok, hcols), BF16),
        pltpu.VMEM((2, 2, 2 * tok, hcols), BF16),
        pltpu.VMEM((2, 2 * tok, hcols), BF16), pltpu.VMEM((2, 2 * tok, hcols), BF16),
        pltpu.VMEM((2, nx, 2 * tok, hcols), BF16),
        pltpu.VMEM((nt, nx, unit, wide), F32), pltpu.VMEM((C, nx, unit, wide), BF16),
        pltpu.VMEM((nt, nx, unit, wide), BF16), pltpu.VMEM((nt, nx, unit, wide), BF16),
        pltpu.VMEM((nt, nx, unit, wide), BF16), pltpu.VMEM((nt, nt, unit, wide), BF16),
        pltpu.VMEM((nt, unit, tasks * th), BF16), pltpu.VMEM((nt, unit, tasks * th), BF16),
        pltpu.VMEM((tok, wide), BF16),
        dma((8,)), dma, dma, dma, dma((C,)), dma, dma((C,)),
        dma, dma((C, 2, 2)), dma, dma((C, 2)), dma((2,)), dma((C, 2, 3)),
        dma, dma((nt,)), dma, dma((nt, nx - 1)), dma, dma((nt,)), dma, dma, dma, dma, dma, dma,
    ]
    mixed, scores = pl.pallas_call(
        functools.partial(stay_kernel, dims),
        out_shape=(pltpu.VMEM((feat, tok), BF16), pltpu.VMEM((tasks, unit), F32)),
        in_specs=[hbm] * 8 + [smem],
        out_specs=(vmem, vmem),
        scratch_shapes=scratch,
        compiler_params=pltpu.CompilerParams(
            has_side_effects=True, collective_id=0, vmem_limit_bytes=60 << 20),
        name="stay",
    )(requests.T, expert_ids.T, gate_values.T, w_up, w_down, tower_in, tower_bias, tower_out, out_bias)
    return mixed.T, scores


def weights_stay(mesh):
    return mesh.shape["expert"] == 4 and mesh.shape["tensor"] == 4 and mesh.shape["rep"] == 2


def tower_head(pre, tower_bias, tower_out, out_bias):
    active = jax.nn.relu(pre + tower_bias[None, :])
    active = active.reshape(pre.shape[0], tower_out.shape[0], tower_out.shape[1])
    logits = jnp.sum(active * tower_out[None, :, :], axis=2) + out_bias[None, :]
    return jax.nn.sigmoid(logits).T


def per_device(
    requests, expert_ids, gate_values, w_up, w_down, tower_in, tower_bias, tower_out, out_bias
):
    groups = lax.axis_size("expert")
    experts = w_up.shape[0]
    local_experts = experts // groups
    tok_rows = requests.shape[0]
    capacity = 3 * tok_rows // experts
    serve_up, serve_down = (
        lax.all_to_all(w_up, "expert", split_axis=0, concat_axis=1, tiled=True),
        lax.all_to_all(w_down, "expert", split_axis=0, concat_axis=1, tiled=True),
    )
    flat_ids = expert_ids.reshape(-1)
    onehot = (flat_ids[:, None] == jnp.arange(experts, dtype=jnp.int32)[None, :]).astype(jnp.int32)
    before = jnp.cumsum(onehot, axis=0) - onehot
    slot_rank = jnp.sum(before * onehot, axis=1)
    slots = (flat_ids * capacity + slot_rank).reshape(tok_rows, 2)
    slot_index = jnp.arange(experts * capacity, dtype=jnp.int32)
    spread = (
        (slot_index[:, None] == slots[None, :, 0]) | (slot_index[:, None] == slots[None, :, 1])
    ).astype(jnp.bfloat16)
    full_rows = lax.all_gather(requests, ("tensor", "rep"), axis=1, tiled=True)
    outgoing = jnp.dot(spread, full_rows, preferred_element_type=jnp.float32).astype(jnp.bfloat16)
    incoming = lax.all_to_all(outgoing, "expert", split_axis=0, concat_axis=0, tiled=True)
    shaped = incoming.reshape(groups, local_experts, capacity, incoming.shape[1])
    hidden_pre = jnp.einsum("secd,edh->sech", shaped, serve_up, preferred_element_type=jnp.float32)
    hidden = jax.nn.relu(hidden_pre).astype(jnp.bfloat16)
    partial_value = jnp.einsum(
        "sech,edh->secd", hidden, serve_down, preferred_element_type=jnp.float32
    )
    summed = lax.psum_scatter(
        partial_value.astype(jnp.bfloat16), ("tensor", "rep"), scatter_dimension=3, tiled=True
    ).astype(jnp.float32)
    expert_out = summed.astype(jnp.bfloat16).reshape(
        groups * local_experts * capacity, summed.shape[3]
    )
    returned = lax.all_to_all(expert_out, "expert", split_axis=0, concat_axis=0, tiled=True)
    pick_first = (slots[:, 0:1] == slot_index[None, :]).astype(jnp.bfloat16)
    pick_second = (slots[:, 1:2] == slot_index[None, :]).astype(jnp.bfloat16)
    first = jnp.dot(pick_first, returned, preferred_element_type=jnp.float32)
    second = jnp.dot(pick_second, returned, preferred_element_type=jnp.float32)
    mixed = (gate_values[:, 0:1] * first + gate_values[:, 1:2] * second).astype(jnp.bfloat16)
    pre = lax.psum_scatter(
        jnp.dot(mixed, tower_in, preferred_element_type=jnp.float32).astype(jnp.bfloat16),
        ("tensor", "rep"),
        scatter_dimension=0,
        tiled=True,
    ).astype(jnp.float32)
    scores = tower_head(pre, tower_bias, tower_out, out_bias)
    return (mixed, scores)


def solution(mesh):
    in_specs = (
        P("expert", ("tensor", "rep")),
        P("expert", None),
        P("expert", None),
        P(None, "expert", ("tensor", "rep")),
        P(None, "expert", ("tensor", "rep")),
        P(("tensor", "rep"), None),
        P(),
        P(),
        P(),
    )
    out_specs = (P("expert", ("tensor", "rep")), P(None, ("expert", "tensor", "rep")))
    body = stay_device if weights_stay(mesh) else per_device
    return jax.shard_map(
        body, mesh=mesh, in_specs=in_specs, out_specs=out_specs, check_vma=False
    )
```

```python
import functools
import jax
import jax.numpy as jnp
from jax import lax
from jax.experimental import pallas as pl
from jax.experimental.pallas import tpu as pltpu
from jax.sharding import PartitionSpec as P

MESH = pl.DeviceIdType.MESH
F32 = jnp.float32
BF16 = jnp.bfloat16


def stay_kernel(
    dims, req_hbm, ids_hbm, gates_hbm, up_hbm, down_hbm, tin_hbm, bias_hbm, tout_hbm, ob_ref,
    mixed_ref, scores_ref,
    req_ref, ids_ref, gates_ref, bias_ref, tout_ref, up, down, tin, meta_ref, meta, rt, xs,
    hp, r1, s2, r2, hid, mine, dsend0, drecv0, dsend, gat, zrec, fsend, frecv, rows_out, lrec, lsum, zl,
    lsem, me_s, me_r, x_s, x_r, q_s, q_r, s1_s, s1_r, s2_s, s2_r, h_s, h_r,
    p_s, p_r, g_s, g_r, z_s, z_r, m_s, m_r, t_s, t_r, f_s, f_r, l_s, l_r, zl_s, zl_r,
):
    nx, nt, nr, experts, tok, feat, hcols, tasks, th, unit, sizes = dims
    xe, t, r = lax.axis_index("expert"), lax.axis_index("tensor"), lax.axis_index("rep")
    chunks = len(sizes)
    offs = [sum(sizes[:c]) * unit for c in range(chunks)]
    subs = [n * unit for n in sizes]

    def remote(src, dst, ssem, rsem, dev):
        return pltpu.make_async_remote_copy(
            src_ref=src, dst_ref=dst, send_sem=ssem, recv_sem=rsem, device_id=dev,
            device_id_type=MESH)

    def send(src, dst, ssem, rsem, dev):
        remote(src, dst, ssem, rsem, dev).start()

    def got(ref, rsem):
        remote(ref, ref, lsem.at[0], rsem, (xe, t, r)).wait_recv()

    def sent(ref, ssem):
        remote(ref, ref, ssem, lsem.at[0], (xe, t, r)).wait_send()

    first = [
        pltpu.make_async_copy(req_hbm, req_ref, lsem.at[3]),
        pltpu.make_async_copy(ids_hbm, ids_ref, lsem.at[4]),
        pltpu.make_async_copy(gates_hbm, gates_ref, lsem.at[5]),
    ]

    def own_rows(ref, k):
        return ref.at[pl.ds(pl.multiple_of(k * feat, feat), feat)]

    loads = [
        pltpu.make_async_copy(up_hbm, up, lsem.at[0]),
        pltpu.make_async_copy(down_hbm, down, lsem.at[1]),
        pltpu.make_async_copy(tin_hbm, own_rows(tin, r), lsem.at[2]),
        pltpu.make_async_copy(bias_hbm, bias_ref, lsem.at[6]),
        pltpu.make_async_copy(tout_hbm, tout_ref, lsem.at[7]),
    ]
    first[0].start()
    here = t == xe
    away = jnp.logical_not(here)
    partner = (xe, t, 1 - r)
    barrier = pltpu.get_barrier_semaphore()

    def greet(dev):
        pl.semaphore_signal(barrier, inc=1, device_id=dev, device_id_type=MESH)

    me = t * nr + r
    for d in reversed(range(1, nt * nr)):
        other = me ^ d
        greet((xe, lax.div(other, nr), lax.rem(other, nr)))
    for d in range(1, nx):
        for k in range(nr):
            greet((xe ^ d, t, k))
    for b in range(nx):
        @pl.when(jnp.logical_not(jnp.logical_and(here, xe == b)))
        def _():
            greet((b, xe, r))
    for load in first[1:] + loads:
        load.start()
    first[0].wait()
    rt[...] = req_ref[...].T
    greeted = (nt * nr - 1) + (nx - 1) * nr + nt

    with jax.named_scope("barr"):
        @pl.when(here)
        def _():
            pl.semaphore_wait(barrier, greeted - 1)

        @pl.when(away)
        def _():
            pl.semaphore_wait(barrier, greeted)

    def span(c):
        return pl.ds(offs[c], subs[c])

    for c in range(chunks):
        for tt in reversed(range(nt)):
            @pl.when(jnp.logical_not(jnp.logical_and(here, t == tt)))
            def _():
                send(rt.at[span(c)], xs.at[r, xe, span(c)], x_s, x_r.at[c], (t, tt, r))
        if c == 0:
            for load in first[1:]:
                load.wait()
            meta_ref[...] = jnp.concatenate(
                [ids_ref[...].astype(F32), gates_ref[...], jnp.zeros((4, tok), F32)], axis=0)
            for d in range(1, nx):
                send(meta_ref, meta.at[xe], me_s, me_r, (xe ^ d, t, r))
    send(tin_hbm, own_rows(tin, r), t_s, t_r, partner)
    meta[xe] = meta_ref[...]

    @pl.when(here)
    def _():
        xs[r, xe] = rt[...]

    def take(c):
        @pl.when(here)
        def _():
            got(xs.at[r, pl.ds(0, nx - 1), span(c)], x_r.at[c])

        @pl.when(away)
        def _():
            got(xs.at[r, :, span(c)], x_r.at[c])
        send(xs.at[r, :, span(c)], xs.at[r, :, span(c)], q_s, q_r.at[c], partner)

    with jax.named_scope("take0"):
        take(0)
    with jax.named_scope("meta"):
        got(meta.at[pl.ds(0, nx - 1)], me_r)
        info = [meta[b].T for b in range(nx)]

    def column(c, j):
        return jnp.concatenate(
            [info[b][offs[c]:offs[c] + subs[c], j:j + 1] for b in range(nx)], axis=0)

    near = (1, 2)

    def picks(c, k=None):
        if k is None:
            return pl.ds(2 * offs[c], 2 * subs[c])
        return pl.ds(2 * offs[c] + k * subs[c], subs[c])

    def up_chunk(c):
        sub = subs[c]
        got(xs.at[1 - r, :, span(c)], q_r.at[c])
        if c == 0:
            loads[0].wait()
        rows = [xs[k, :, offs[c]:offs[c] + sub, :].reshape(nx * sub, feat) for k in range(nr)]
        ids = (column(c, 0), column(c, 1))
        for h in range(2):
            picked = [jnp.zeros((nx * sub, hcols), F32)] * 2
            for e in range(experts):
                part = None
                for k in range(nr):
                    one = jnp.dot(rows[k], up[e, k * feat:(k + 1) * feat, h * hcols:(h + 1) * hcols],
                                  preferred_element_type=F32)
                    part = one if part is None else part + one
                picked = [jnp.where(ids[k] == float(e), part, picked[k]) for k in range(2)]
            for k in range(2):
                hp[h, :, picks(c, k), :] = picked[k].astype(BF16).reshape(nx, sub, hcols)
            fa, fb = near[h], near[1 - h]
            for i, q, sem in ((0, xe ^ fa ^ fb, s1_r), (1, xe ^ fa, s2_r)):
                send(hp.at[h, q, picks(c)], r1.at[h, i, picks(c)], s1_s, sem.at[c, h],
                     (xe ^ fa, t, r))
        if c + 1 < chunks:
            take(c + 1)

    def reduce_first(c, h):
        fa, fb = near[h], near[1 - h]
        got(r1.at[h, 0, picks(c)], s1_r.at[c, h])
        s2[h, picks(c)] = (hp[h, xe ^ fb, picks(c)].astype(F32)
                           + r1[h, 0, picks(c)].astype(F32)).astype(BF16)
        send(s2.at[h, picks(c)], r2.at[h, picks(c)], s2_s, s2_r.at[c, h], (xe ^ fb, t, r))

    def reduce_second(c, h):
        fa, fb = near[h], near[1 - h]
        got(r1.at[h, :, picks(c)], s2_r.at[c, h])
        total = (hp[h, xe, picks(c)].astype(F32) + r1[h, 1, picks(c)].astype(F32)
                 + r2[h, picks(c)].astype(F32))
        hid[h, xe, picks(c)] = jnp.maximum(total, 0.0).astype(BF16)
        mine_ref = hid.at[h, xe, picks(c)]
        send(mine_ref, mine_ref, h_s.at[0], h_r.at[c, h, 0], (xe ^ fb, t, r))
        send(mine_ref, mine_ref, h_s.at[0], h_r.at[c, h, 1], (xe ^ fa, t, r))

    def forward(c, h):
        fa, fb = near[h], near[1 - h]
        ref = hid.at[h, xe ^ fb, picks(c)]
        got(ref, h_r.at[c, h, 0])
        send(ref, ref, h_s.at[1], h_r.at[c, h, 1], (xe ^ fa, t, r))

    def collect(c, h):
        got(hid.at[h, pl.ds(0, 2), picks(c)], h_r.at[c, h, 1])

    last = chunks - 1
    end_core = (sum(sizes) - 1) % nr
    final_rows = pl.ds((sum(sizes) - 1) * unit, unit)

    def parity(c):
        return sum(sizes[:c]) % nr if sizes[c] == 1 else None

    def slot(c, core):
        return (sum(sizes[:c]) + (sizes[c] - 1 if sizes[c] > 1 else 0)) // nr - (
            core if sizes[c] > 1 else 0)

    def if_core(c, other, body, only=None):
        p = parity(c)
        if p is None:
            if only is None:
                body()
            else:
                pl.when(r == only)(body)
        elif only is None or only == p:
            pl.when(r == (1 - p if other else p))(body)

    def down_chunk(c):
        sub = subs[c]
        ids = (column(c, 0), column(c, 1))
        gates = (column(c, 2), column(c, 3))
        total = jnp.zeros((nx * sub, nr * feat), F32)
        for e in range(experts):
            hit = (ids[0] == float(e), ids[1] == float(e))
            weight = jnp.where(hit[0], gates[0], 0.0) + jnp.where(hit[1], gates[1], 0.0)
            part = None
            for h in range(2):
                values = [hid[h, :, picks(c, k), :].reshape(nx * sub, hcols) for k in range(2)]
                chosen = jnp.where(hit[0], values[0], jnp.where(hit[1], values[1], jnp.zeros_like(values[1])))
                one = lax.dot_general(chosen, down[e, :, h * hcols:(h + 1) * hcols],
                                      (((1,), (1,)), ((), ())), preferred_element_type=F32)
                part = one if part is None else part + one
            total = total + weight * part
        total = total.reshape(nx, sub, nr * feat)
        if c == last:
            dsend0[c] = total.astype(BF16)
            for d in (3, 1, 2):
                send(dsend0.at[c, xe ^ d], lrec.at[r, xe], l_s, l_r.at[d], (xe ^ d, t, end_core))

            @pl.when(r == end_core)
            def _():
                lrec[r, xe] = dsend0[c, xe]

            @pl.when(r != end_core)
            def _():
                send(dsend0.at[c, xe], lrec.at[r, xe], l_s, l_r.at[0], partner)
            return
        if sizes[c] == 1:
            keep = give = total
        else:
            odd, even = total[:, :unit], total[:, unit:]
            keep = jnp.where(r == 0, even, odd)
            give = jnp.where(r == 0, odd, even)

        def store():
            mine[slot(c, r)] = keep

        def give_away():
            at = slot(c, 1 - r)
            dsend0[c] = give.astype(BF16)
            send(dsend0.at[c], drecv0.at[at], p_s, p_r.at[at], partner)
        if_core(c, True, give_away)
        if_core(c, False, store)

    def last_sum(q):
        lsum[q] = (lrec[0, q].astype(F32) + lrec[1, q].astype(F32)).astype(BF16)
        send(lsum.at[q], zl.at[t], zl_s.at[0], zl_r, (xe, q, 1 - r))

        @pl.when(q != t)
        def _():
            send(lsum.at[q], zl.at[t], zl_s.at[1], zl_r, (xe, q, r))

        @pl.when(q == t)
        def _():
            zl[t] = lsum[q]

    def last_own(c):
        @pl.when(r == end_core)
        def _():
            got(lrec.at[1 - r, xe], l_r.at[0])
            last_sum(xe)

    def last_pass():
        for k in reversed(range(nt)):
            q = t ^ k

            @pl.when(q != xe)
            def _():
                got(lrec.at[:, q], l_r.at[q ^ xe])
                last_sum(q)

    def last_mixed():
        @pl.when(r == end_core)
        def _():
            got(zl.at[pl.ds(0, nt - 1)], zl_r)

        @pl.when(r != end_core)
        def _():
            got(zl, zl_r)
        total = zl[0].astype(F32)
        for src in range(1, nt):
            total = total + zl[src].astype(F32)
        value = total.astype(BF16)
        rows_out[final_rows, :] = value

        @pl.when(r == end_core)
        def _():
            s = nt - 1
            fsend[s] = jnp.dot(value, tin[...], preferred_element_type=F32).astype(BF16)

            @pl.when(t != s)
            def _():
                send(fsend.at[s], frecv.at[t], f_s, f_r, (xe, s, r))

    def pair_chunk(c, only=None):
        if c == last:
            return

        def body():
            s = slot(c, r)
            got(drecv0.at[s], p_r.at[s])
            dsend[s] = (mine[s] + drecv0[s].astype(F32)).astype(BF16)
            for d in (3, 1, 2):
                send(dsend.at[s, xe ^ d], gat.at[s, xe], g_s, g_r.at[s], (xe ^ d, t, r))
            gat[s, xe] = dsend[s, xe]

            @pl.when(away)
            def _():
                send(dsend.at[s, xe], zrec.at[s, t], z_s, z_r.at[s], (xe, xe, r))
        if_core(c, False, body, only)

    def pass_chunk(c, only=None):
        if c == last:
            pl.when(r == end_core)(last_pass)
            return

        def body():
            s = slot(c, r)
            got(gat.at[s, pl.ds(0, nx - 1)], g_r.at[s])
            for d in (1, 2, 3):
                q = xe ^ d

                @pl.when(q != t)
                def _():
                    send(gat.at[s, q], zrec.at[s, t], z_s, z_r.at[s], (xe, q, r))
        if_core(c, False, body, only)

    def mixed_chunk(c, only=None):
        if c == last:
            return last_mixed()

        def body():
            s = slot(c, r)
            got(zrec.at[s, pl.ds(0, nt - 1)], z_r.at[s])
            total = gat[s, t].astype(F32)
            for d in range(1, nt):
                total = total + zrec[s, t ^ d].astype(F32)
            value = total.astype(BF16)
            at = pl.ds(pl.multiple_of((s * nr + r) * unit, unit), unit)
            rows_out[at, :] = value
            send(rows_out.at[at], rows_out.at[at], m_s, m_r, partner)
            fsend[s] = jnp.dot(value, tin[...], preferred_element_type=F32).astype(BF16)

            @pl.when(t != s)
            def _():
                send(fsend.at[s], frecv.at[t], f_s, f_r, (xe, s, r))
        if_core(c, False, body, only)

    def drain(c):
        sent(r1, s1_s)
        sent(r2, s2_s)
        sent(r1, h_s.at[0])
        sent(r2, h_s.at[1])
        sent(meta.at[pl.ds(0, nx - 1)], me_s)
        sent(own_rows(tin, r), t_s)
        sent(xs.at[r], q_s)

        @pl.when(r == end_core)
        def _():
            sent(lrec.at[0, pl.ds(0, nx - 1)], l_s)
            sent(drecv0, p_s)
            sent(gat.at[pl.ds(0, nt - 1), pl.ds(0, nx - 1)], g_s)
            sent(zrec.at[pl.ds(0, nt - 1), pl.ds(0, nt - 1)], z_s)

        @pl.when(r != end_core)
        def _():
            sent(lrec.at[0], l_s)
            sent(drecv0.at[pl.ds(0, nt - 1)], p_s)
            sent(gat.at[:, pl.ds(0, nx - 1)], g_s)
            sent(zrec.at[:, pl.ds(0, nt - 1)], z_s)

        @pl.when(here)
        def _():
            sent(xs.at[r, pl.ds(0, nx - 1)], x_s)

        @pl.when(away)
        def _():
            sent(xs.at[r], x_s)

    stages = {
        "fw": forward, "rb": reduce_second, "ra": reduce_first, "up": up_chunk, "co": collect,
        "dn": down_chunk, "pr": pair_chunk, "ps": pass_chunk, "mx": mixed_chunk, "drain": drain,
        "pe": last_own,
    }
    for core in range(nr):
        for name in ("pr", "ps", "mx"):
            stages[f"{name}{core}"] = functools.partial(stages[name], only=core)
    order = []
    for i in range(chunks + 4):
        order += [("up", i), ("ra", i - 1), ("rb", i - 2), ("fw", i - 3), ("co", i - 4), ("dn", i - 4)]
        if i < chunks + 3:
            order += [("pr0", i - 4), ("pr1", i - 5), ("ps0", i - 5), ("ps1", i - 6), ("mx0", i - 6), ("mx1", i - 7)]
    n = last
    order += [("pr1", n - 1), ("ps0", n - 1), ("ps1", n - 2), ("mx0", n - 2), ("mx1", n - 3),
              ("ps1", n - 1), ("pe", n), ("mx1", n - 2), ("ps", n), ("mx0", n - 1), ("mx1", n - 1), ("drain", n), ("mx", n)]
    for name, c in order:
        if not 0 <= c < chunks or (c == last and name[-1].isdigit()):
            continue
        if name == "dn" and c == 0:
            for load in loads[1:]:
                load.wait()
            got(own_rows(tin, 1 - r), t_r)
        with jax.named_scope(f"{name}_{c}"):
            if name in ("fw", "rb", "ra", "co"):
                for h in range(2):
                    stages[name](c, h)
            else:
                stages[name](c)
    half = tok // nr
    fewer = half - unit
    with jax.named_scope("mout"):
        @pl.when(r == end_core)
        def _():
            got(rows_out.at[pl.ds(0, half)], m_r)

        @pl.when(r != end_core)
        def _():
            got(rows_out.at[pl.ds(0, fewer)], m_r)
    out = rows_out[...].T
    mixed_ref[...] = jnp.where(r == 0, out[:feat], out[feat:])
    with jax.named_scope("fin"):
        got(frecv.at[pl.ds(0, nt - 1)], f_r)
        pre = fsend[t].astype(F32)
        for d in range(1, nt):
            pre = pre + frecv[t ^ d].astype(F32)
    active = jnp.maximum(pre + bias_ref[...].reshape(1, tasks * th), 0.0)
    outs = []
    for j in range(tasks):
        outs.append(jnp.sum(active[:, j * th:(j + 1) * th] * tout_ref[j:j + 1, :], axis=1, keepdims=True))
    lane = lax.broadcasted_iota(jnp.int32, (unit, 128), 1)
    logits = jnp.zeros((unit, 128), F32)
    for j in range(tasks):
        logits = jnp.where(lane == j, outs[j] + ob_ref[j], logits)
    scores_ref[...] = jax.nn.sigmoid(logits.T[:tasks, :])
    with jax.named_scope("end"):
        @pl.when(r == end_core)
        def _():
            sent(zrec.at[0], zl_s.at[0])
            sent(zrec.at[1, pl.ds(0, nt - 1)], zl_s.at[1])
            sent(rows_out.at[pl.ds(0, fewer)], m_s)

        @pl.when(r != end_core)
        def _():
            sent(rows_out.at[pl.ds(0, half)], m_s)
        sent(frecv.at[pl.ds(0, nt - 1)], f_s)


def emit_kernel(mixed_in, scores_in, mixed_out, scores_out, sem):
    copies = [
        pltpu.make_async_copy(mixed_in, mixed_out, sem.at[0]),
        pltpu.make_async_copy(scores_in, scores_out, sem.at[1]),
    ]
    for copy in copies:
        copy.start()
    for copy in copies:
        copy.wait()


def stay_device(requests, expert_ids, gate_values, w_up, w_down, tower_in, tower_bias, tower_out,
                out_bias):
    nx, nt, nr = lax.axis_size("expert"), lax.axis_size("tensor"), lax.axis_size("rep")
    experts, _, hid_cols = w_up.shape
    tok, feat = requests.shape
    tasks, th = tower_out.shape
    hcols = hid_cols // 2
    unit = tok // (nt * nr)
    sizes = (1,) + (nr,) * (nt - 1) + (1,)
    C = len(sizes)
    dims = (nx, nt, nr, experts, tok, feat, hcols, tasks, th, unit, sizes)
    vmem = pl.BlockSpec(memory_space=pltpu.VMEM)
    hbm = pl.BlockSpec(memory_space=pltpu.HBM)
    smem = pl.BlockSpec(memory_space=pltpu.SMEM)
    dma = pltpu.SemaphoreType.DMA
    wide = nr * feat
    scratch = [
        pltpu.VMEM((feat, tok), BF16), pltpu.VMEM((2, tok), jnp.int32), pltpu.VMEM((2, tok), F32),
        pltpu.VMEM(tower_bias.shape, F32), pltpu.VMEM(tower_out.shape, F32),
        pltpu.VMEM(w_up.shape, BF16), pltpu.VMEM(w_down.shape, BF16),
        pltpu.VMEM((wide, tower_in.shape[1]), BF16),
        pltpu.VMEM((8, tok), F32), pltpu.VMEM((nx, 8, tok), F32),
        pltpu.VMEM((tok, feat), BF16), pltpu.VMEM((nr, nx, tok, feat), BF16),
        pltpu.VMEM((2, nx, 2 * tok, hcols), BF16),
        pltpu.VMEM((2, 2, 2 * tok, hcols), BF16),
        pltpu.VMEM((2, 2 * tok, hcols), BF16), pltpu.VMEM((2, 2 * tok, hcols), BF16),
        pltpu.VMEM((2, nx, 2 * tok, hcols), BF16),
        pltpu.VMEM((nt, nx, unit, wide), F32), pltpu.VMEM((C, nx, unit, wide), BF16),
        pltpu.VMEM((nt, nx, unit, wide), BF16), pltpu.VMEM((nt, nx, unit, wide), BF16),
        pltpu.VMEM((nt, nx, unit, wide), BF16), pltpu.VMEM((nt, nt, unit, wide), BF16),
        pltpu.VMEM((nt, unit, tasks * th), BF16), pltpu.VMEM((nt, unit, tasks * th), BF16),
        pltpu.VMEM((tok, wide), BF16),
        pltpu.VMEM((nr, nx, unit, wide), BF16), pltpu.VMEM((nx, unit, wide), BF16),
        pltpu.VMEM((nt, unit, wide), BF16),
        dma((8,)), dma, dma, dma, dma((C,)), dma, dma((C,)),
        dma, dma((C, 2)), dma, dma((C, 2)), dma((2,)), dma((C, 2, 2)),
        dma, dma((nt,)), dma, dma((nt,)), dma, dma((nt,)), dma, dma, dma, dma, dma, dma,
        dma, dma((nx,)), dma((2,)), dma,
    ]
    mixed, scores = pl.pallas_call(
        functools.partial(stay_kernel, dims),
        out_shape=(pltpu.VMEM((feat, tok), BF16), pltpu.VMEM((tasks, unit), F32)),
        in_specs=[hbm] * 8 + [smem],
        out_specs=(vmem, vmem),
        scratch_shapes=scratch,
        compiler_params=pltpu.CompilerParams(
            has_side_effects=True, collective_id=0, vmem_limit_bytes=60 << 20),
        name="stay",
    )(requests.T, expert_ids.T, gate_values.T, w_up, w_down, tower_in, tower_bias, tower_out, out_bias)
    mixed, scores = pl.pallas_call(
        emit_kernel,
        out_shape=(jax.ShapeDtypeStruct(mixed.shape, BF16), jax.ShapeDtypeStruct(scores.shape, F32)),
        in_specs=[vmem, vmem],
        out_specs=(hbm, hbm),
        scratch_shapes=[dma((2,))],
        name="emit",
    )(pltpu.with_memory_space_constraint(mixed, pltpu.VMEM), pltpu.with_memory_space_constraint(scores, pltpu.VMEM))
    return mixed.T, scores


def weights_stay(mesh):
    return mesh.shape["expert"] == 4 and mesh.shape["tensor"] == 4 and mesh.shape["rep"] == 2


def tower_head(pre, tower_bias, tower_out, out_bias):
    active = jax.nn.relu(pre + tower_bias[None, :])
    active = active.reshape(pre.shape[0], tower_out.shape[0], tower_out.shape[1])
    logits = jnp.sum(active * tower_out[None, :, :], axis=2) + out_bias[None, :]
    return jax.nn.sigmoid(logits).T


def per_device(
    requests, expert_ids, gate_values, w_up, w_down, tower_in, tower_bias, tower_out, out_bias
):
    groups = lax.axis_size("expert")
    experts = w_up.shape[0]
    local_experts = experts // groups
    tok_rows = requests.shape[0]
    capacity = 3 * tok_rows // experts
    serve_up, serve_down = (
        lax.all_to_all(w_up, "expert", split_axis=0, concat_axis=1, tiled=True),
        lax.all_to_all(w_down, "expert", split_axis=0, concat_axis=1, tiled=True),
    )
    flat_ids = expert_ids.reshape(-1)
    onehot = (flat_ids[:, None] == jnp.arange(experts, dtype=jnp.int32)[None, :]).astype(jnp.int32)
    before = jnp.cumsum(onehot, axis=0) - onehot
    slot_rank = jnp.sum(before * onehot, axis=1)
    slots = (flat_ids * capacity + slot_rank).reshape(tok_rows, 2)
    slot_index = jnp.arange(experts * capacity, dtype=jnp.int32)
    spread = (
        (slot_index[:, None] == slots[None, :, 0]) | (slot_index[:, None] == slots[None, :, 1])
    ).astype(jnp.bfloat16)
    full_rows = lax.all_gather(requests, ("tensor", "rep"), axis=1, tiled=True)
    outgoing = jnp.dot(spread, full_rows, preferred_element_type=jnp.float32).astype(jnp.bfloat16)
    incoming = lax.all_to_all(outgoing, "expert", split_axis=0, concat_axis=0, tiled=True)
    shaped = incoming.reshape(groups, local_experts, capacity, incoming.shape[1])
    hidden_pre = jnp.einsum("secd,edh->sech", shaped, serve_up, preferred_element_type=jnp.float32)
    hidden = jax.nn.relu(hidden_pre).astype(jnp.bfloat16)
    partial_value = jnp.einsum(
        "sech,edh->secd", hidden, serve_down, preferred_element_type=jnp.float32
    )
    summed = lax.psum_scatter(
        partial_value.astype(jnp.bfloat16), ("tensor", "rep"), scatter_dimension=3, tiled=True
    ).astype(jnp.float32)
    expert_out = summed.astype(jnp.bfloat16).reshape(
        groups * local_experts * capacity, summed.shape[3]
    )
    returned = lax.all_to_all(expert_out, "expert", split_axis=0, concat_axis=0, tiled=True)
    pick_first = (slots[:, 0:1] == slot_index[None, :]).astype(jnp.bfloat16)
    pick_second = (slots[:, 1:2] == slot_index[None, :]).astype(jnp.bfloat16)
    first = jnp.dot(pick_first, returned, preferred_element_type=jnp.float32)
    second = jnp.dot(pick_second, returned, preferred_element_type=jnp.float32)
    mixed = (gate_values[:, 0:1] * first + gate_values[:, 1:2] * second).astype(jnp.bfloat16)
    pre = lax.psum_scatter(
        jnp.dot(mixed, tower_in, preferred_element_type=jnp.float32).astype(jnp.bfloat16),
        ("tensor", "rep"),
        scatter_dimension=0,
        tiled=True,
    ).astype(jnp.float32)
    scores = tower_head(pre, tower_bias, tower_out, out_bias)
    return (mixed, scores)


def solution(mesh):
    in_specs = (
        P("expert", ("tensor", "rep")),
        P("expert", None),
        P("expert", None),
        P(None, "expert", ("tensor", "rep")),
        P(None, "expert", ("tensor", "rep")),
        P(("tensor", "rep"), None),
        P(),
        P(),
        P(),
    )
    out_specs = (P("expert", ("tensor", "rep")), P(None, ("expert", "tensor", "rep")))
    body = stay_device if weights_stay(mesh) else per_device
    return jax.shard_map(
        body, mesh=mesh, in_specs=in_specs, out_specs=out_specs, check_vma=False
    )
```

```python
import functools
import jax
import jax.numpy as jnp
from jax import lax
from jax.experimental import pallas as pl
from jax.experimental.pallas import tpu as pltpu
from jax.sharding import PartitionSpec as P

MESH = pl.DeviceIdType.MESH
F32 = jnp.float32
BF16 = jnp.bfloat16


def stay_kernel(
    dims, req_hbm, ids_hbm, gates_hbm, up_hbm, down_hbm, tin_hbm, bias_hbm, tout_hbm, ob_ref,
    mixed_ref, scores_ref,
    req_ref, ids_ref, gates_ref, bias_ref, tout_ref, up, down, tin, meta_ref, meta, rt, xs,
    hp, r1, s2, r2, hid, mine, dsend0, drecv0, dsend, gat, zrec, fsend, frecv, rows_out, lrec, lsum, zl, ow, owt, pre_ref,
    lsem, me_s, me_r, x_s, x_r, q_s, q_r, s1_s, s1_r, s2_s, s2_r, h_s, h_r,
    p_s, p_r, g_s, g_r, z_s, z_r, m_s, m_r, t_s, t_r, f_s, f_r, l_s, l_r, zl_s, zl_r, o_s, o_r, w_s, w_r, v_s, v_r,
):
    nx, nt, nr, experts, tok, feat, hcols, tasks, th, unit, sizes = dims
    xe, t, r = lax.axis_index("expert"), lax.axis_index("tensor"), lax.axis_index("rep")
    chunks = len(sizes)
    offs = [sum(sizes[:c]) * unit for c in range(chunks)]
    subs = [n * unit for n in sizes]

    def remote(src, dst, ssem, rsem, dev):
        return pltpu.make_async_remote_copy(
            src_ref=src, dst_ref=dst, send_sem=ssem, recv_sem=rsem, device_id=dev,
            device_id_type=MESH)

    def send(src, dst, ssem, rsem, dev):
        remote(src, dst, ssem, rsem, dev).start()

    def got(ref, rsem):
        remote(ref, ref, lsem.at[0], rsem, (xe, t, r)).wait_recv()

    def sent(ref, ssem):
        remote(ref, ref, ssem, lsem.at[0], (xe, t, r)).wait_send()

    first = [
        pltpu.make_async_copy(req_hbm, req_ref, lsem.at[3]),
        pltpu.make_async_copy(ids_hbm, ids_ref, lsem.at[4]),
        pltpu.make_async_copy(gates_hbm, gates_ref, lsem.at[5]),
    ]

    def own_rows(ref, k):
        return ref.at[pl.ds(pl.multiple_of(k * feat, feat), feat)]

    loads = [
        pltpu.make_async_copy(up_hbm, up, lsem.at[0]),
        pltpu.make_async_copy(down_hbm, down, lsem.at[1]),
        pltpu.make_async_copy(tin_hbm, own_rows(tin, r), lsem.at[2]),
        pltpu.make_async_copy(bias_hbm, bias_ref, lsem.at[6]),
        pltpu.make_async_copy(tout_hbm, tout_ref, lsem.at[7]),
    ]
    first[0].start()
    here = t == xe
    away = jnp.logical_not(here)
    partner = (xe, t, 1 - r)
    barrier = pltpu.get_barrier_semaphore()

    def greet(dev):
        pl.semaphore_signal(barrier, inc=1, device_id=dev, device_id_type=MESH)

    me = t * nr + r
    for d in reversed(range(1, nt * nr)):
        other = me ^ d
        greet((xe, lax.div(other, nr), lax.rem(other, nr)))
    for d in range(1, nx):
        for k in range(nr):
            greet((xe ^ d, t, k))
    for b in range(nx):
        @pl.when(jnp.logical_not(jnp.logical_and(here, xe == b)))
        def _():
            greet((b, xe, r))
    for load in first[1:] + loads:
        load.start()
    first[0].wait()
    rt[...] = req_ref[...].T
    greeted = (nt * nr - 1) + (nx - 1) * nr + nt

    with jax.named_scope("barr"):
        @pl.when(here)
        def _():
            pl.semaphore_wait(barrier, greeted - 1)

        @pl.when(away)
        def _():
            pl.semaphore_wait(barrier, greeted)

    def span(c):
        return pl.ds(offs[c], subs[c])

    for c in range(chunks):
        for tt in reversed(range(nt)):
            @pl.when(jnp.logical_not(jnp.logical_and(here, t == tt)))
            def _():
                send(rt.at[span(c)], xs.at[r, xe, span(c)], x_s, x_r.at[c], (t, tt, r))
        if c == 0:
            for load in first[1:]:
                load.wait()
            meta_ref[...] = jnp.concatenate(
                [ids_ref[...].astype(F32), gates_ref[...], jnp.zeros((4, tok), F32)], axis=0)
            for d in range(1, nx):
                send(meta_ref, meta.at[xe], me_s, me_r, (xe ^ d, t, r))
    send(tin_hbm, own_rows(tin, r), t_s, t_r, partner)
    meta[xe] = meta_ref[...]

    @pl.when(here)
    def _():
        xs[r, xe] = rt[...]

    def take(c):
        @pl.when(here)
        def _():
            got(xs.at[r, pl.ds(0, nx - 1), span(c)], x_r.at[c])

        @pl.when(away)
        def _():
            got(xs.at[r, :, span(c)], x_r.at[c])
        send(xs.at[r, :, span(c)], xs.at[r, :, span(c)], q_s, q_r.at[c], partner)

    with jax.named_scope("take0"):
        take(0)
    with jax.named_scope("meta"):
        got(meta.at[pl.ds(0, nx - 1)], me_r)
        info = [meta[b].T for b in range(nx)]

    def column(c, j):
        return jnp.concatenate(
            [info[b][offs[c]:offs[c] + subs[c], j:j + 1] for b in range(nx)], axis=0)

    near = (1, 2)

    def picks(c, k=None):
        if k is None:
            return pl.ds(2 * offs[c], 2 * subs[c])
        return pl.ds(2 * offs[c] + k * subs[c], subs[c])

    def up_chunk(c):
        sub = subs[c]
        got(xs.at[1 - r, :, span(c)], q_r.at[c])
        if c == 0:
            loads[0].wait()
        rows = [xs[k, :, offs[c]:offs[c] + sub, :].reshape(nx * sub, feat) for k in range(nr)]
        ids = (column(c, 0), column(c, 1))
        for h in range(2):
            picked = [jnp.zeros((nx * sub, hcols), F32)] * 2
            for e in range(experts):
                part = None
                for k in range(nr):
                    one = jnp.dot(rows[k], up[e, k * feat:(k + 1) * feat, h * hcols:(h + 1) * hcols],
                                  preferred_element_type=F32)
                    part = one if part is None else part + one
                picked = [jnp.where(ids[k] == float(e), part, picked[k]) for k in range(2)]
            for k in range(2):
                hp[h, :, picks(c, k), :] = picked[k].astype(BF16).reshape(nx, sub, hcols)
            fa, fb = near[h], near[1 - h]
            for i, q, sem in ((0, xe ^ fa ^ fb, s1_r), (1, xe ^ fa, s2_r)):
                send(hp.at[h, q, picks(c)], r1.at[h, i, picks(c)], s1_s, sem.at[c, h],
                     (xe ^ fa, t, r))
        if c + 1 < chunks:
            take(c + 1)

    def reduce_first(c, h):
        fa, fb = near[h], near[1 - h]
        got(r1.at[h, 0, picks(c)], s1_r.at[c, h])
        s2[h, picks(c)] = (hp[h, xe ^ fb, picks(c)].astype(F32)
                           + r1[h, 0, picks(c)].astype(F32)).astype(BF16)
        send(s2.at[h, picks(c)], r2.at[h, picks(c)], s2_s, s2_r.at[c, h], (xe ^ fb, t, r))

    def reduce_second(c, h):
        fa, fb = near[h], near[1 - h]
        got(r1.at[h, :, picks(c)], s2_r.at[c, h])
        total = (hp[h, xe, picks(c)].astype(F32) + r1[h, 1, picks(c)].astype(F32)
                 + r2[h, picks(c)].astype(F32))
        hid[h, xe, picks(c)] = jnp.maximum(total, 0.0).astype(BF16)
        mine_ref = hid.at[h, xe, picks(c)]
        send(mine_ref, mine_ref, h_s.at[0], h_r.at[c, h, 0], (xe ^ fb, t, r))
        send(mine_ref, mine_ref, h_s.at[0], h_r.at[c, h, 1], (xe ^ fa, t, r))

    def forward(c, h):
        fa, fb = near[h], near[1 - h]
        ref = hid.at[h, xe ^ fb, picks(c)]
        got(ref, h_r.at[c, h, 0])
        send(ref, ref, h_s.at[1], h_r.at[c, h, 1], (xe ^ fa, t, r))

    def collect(c, h):
        got(hid.at[h, pl.ds(0, 2), picks(c)], h_r.at[c, h, 1])

    last = chunks - 1
    own_t = nt - 1

    def to_owner(source):
        for q in range(own_t):
            @pl.when(t != own_t)
            def _():
                send(source(q), ow.at[q, t], o_s, o_r, (xe, own_t, r))

            @pl.when(t == own_t)
            def _():
                ow[q, own_t] = source(q)[...]

    def tower_rows(c):
        loads[2].wait()
        got(own_rows(tin, 1 - r), t_r)

        @pl.when(jnp.logical_and(r == end_core, t != own_t))
        def _():
            send(tin, owt.at[t], w_s, w_r, (xe, own_t, r))

    def share_rows(c):
        @pl.when(jnp.logical_and(r == end_core, t == own_t))
        def _():
            got(owt, w_r)
            send(owt, owt, v_s, v_r, partner)

    end_core = (sum(sizes) - 1) % nr
    final_rows = pl.ds((sum(sizes) - 1) * unit, unit)

    def parity(c):
        return sum(sizes[:c]) % nr if sizes[c] == 1 else None

    def slot(c, core):
        start = sum(sizes[:c])
        if sizes[c] == 1 or start % nr == 0:
            return start // nr
        return start // nr + 1 - core

    def if_core(c, other, body, only=None):
        p = parity(c)
        if p is None:
            if only is None:
                body()
            else:
                pl.when(r == only)(body)
        elif only is None or only == p:
            pl.when(r == (1 - p if other else p))(body)

    def down_chunk(c):
        sub = subs[c]
        ids = (column(c, 0), column(c, 1))
        gates = (column(c, 2), column(c, 3))
        total = jnp.zeros((nx * sub, nr * feat), F32)
        for e in range(experts):
            hit = (ids[0] == float(e), ids[1] == float(e))
            weight = jnp.where(hit[0], gates[0], 0.0) + jnp.where(hit[1], gates[1], 0.0)
            part = None
            for h in range(2):
                values = [hid[h, :, picks(c, k), :].reshape(nx * sub, hcols) for k in range(2)]
                chosen = jnp.where(hit[0], values[0], jnp.where(hit[1], values[1], jnp.zeros_like(values[1])))
                one = lax.dot_general(chosen, down[e, :, h * hcols:(h + 1) * hcols],
                                      (((1,), (1,)), ((), ())), preferred_element_type=F32)
                part = one if part is None else part + one
            total = total + weight * part
        total = total.reshape(nx, sub, nr * feat)
        if c == last:
            dsend0[c] = total.astype(BF16)
            for d in (3, 1, 2):
                send(dsend0.at[c, xe ^ d], lrec.at[r, xe], l_s, l_r.at[d], (xe ^ d, t, end_core))

            @pl.when(r == end_core)
            def _():
                lrec[r, xe] = dsend0[c, xe]

            @pl.when(r != end_core)
            def _():
                send(dsend0.at[c, xe], lrec.at[r, xe], l_s, l_r.at[0], partner)
            return
        if sizes[c] == 1:
            keep = give = total
        else:
            lead = sum(sizes[:c]) % nr
            keep = jnp.where(r == lead, total[:, :unit], total[:, unit:])
            give = jnp.where(r == lead, total[:, unit:], total[:, :unit])

        def store():
            mine[slot(c, r)] = keep

        def give_away():
            at = slot(c, 1 - r)
            dsend0[c] = give.astype(BF16)
            send(dsend0.at[c], drecv0.at[at], p_s, p_r.at[at], partner)
        if_core(c, True, give_away)
        if_core(c, False, store)

    def last_sum(q):
        lsum[q] = (lrec[0, q].astype(F32) + lrec[1, q].astype(F32)).astype(BF16)
        send(lsum.at[q], zl.at[t], zl_s.at[0], zl_r, (xe, q, 1 - r))

        @pl.when(q != t)
        def _():
            send(lsum.at[q], zl.at[t], zl_s.at[1], zl_r, (xe, q, r))

        @pl.when(q == t)
        def _():
            zl[t] = lsum[q]

    def last_own(c):
        @pl.when(r == end_core)
        def _():
            got(lrec.at[1 - r, xe], l_r.at[0])
            last_sum(xe)

    def last_pass():
        for k in reversed(range(nt)):
            q = t ^ k

            @pl.when(q != xe)
            def _():
                got(lrec.at[:, q], l_r.at[q ^ xe])
                last_sum(q)
        to_owner(lambda q: lsum.at[q])

    def last_mixed():
        @pl.when(r == end_core)
        def _():
            got(zl.at[pl.ds(0, nt - 1)], zl_r)

        @pl.when(r != end_core)
        def _():
            got(zl, zl_r)
        total = zl[0].astype(F32)
        for src in range(1, nt):
            total = total + zl[src].astype(F32)
        value = total.astype(BF16)
        rows_out[final_rows, :] = value

    def pair_chunk(c, only=None):
        if c == last:
            return

        def body():
            s = slot(c, r)
            got(drecv0.at[s], p_r.at[s])
            dsend[s] = (mine[s] + drecv0[s].astype(F32)).astype(BF16)
            for d in (3, 1, 2):
                send(dsend.at[s, xe ^ d], gat.at[s, xe], g_s, g_r.at[s], (xe ^ d, t, r))
            gat[s, xe] = dsend[s, xe]

            @pl.when(away)
            def _():
                send(dsend.at[s, xe], zrec.at[s, t], z_s, z_r.at[s], (xe, xe, r))
        if_core(c, False, body, only)

    def pass_chunk(c, only=None):
        if c == last:
            pl.when(r == end_core)(last_pass)
            return

        def body():
            s = slot(c, r)
            got(gat.at[s, pl.ds(0, nx - 1)], g_r.at[s])
            for d in (1, 2, 3):
                q = xe ^ d

                @pl.when(q != t)
                def _():
                    send(gat.at[s, q], zrec.at[s, t], z_s, z_r.at[s], (xe, q, r))
            if c == last - 1:
                to_owner(lambda q: gat.at[s, q])
        if_core(c, False, body, only)

    def mixed_chunk(c, only=None):
        if c == last:
            return last_mixed()

        def body():
            s = slot(c, r)
            got(zrec.at[s, pl.ds(0, nt - 1)], z_r.at[s])
            total = gat[s, t].astype(F32)
            for d in range(1, nt):
                total = total + zrec[s, t ^ d].astype(F32)
            value = total.astype(BF16)
            at = pl.ds(pl.multiple_of((s * nr + r) * unit, unit), unit)
            rows_out[at, :] = value
            send(rows_out.at[at], rows_out.at[at], m_s, m_r, partner)
            if c == last - 1:
                return
            fsend[s] = jnp.dot(value, tin[...], preferred_element_type=F32).astype(BF16)

            @pl.when(t != s)
            def _():
                send(fsend.at[s], frecv.at[t], f_s, f_r, (xe, s, r))
        if_core(c, False, body, only)

    def drain(c):
        sent(r1, s1_s)
        sent(r2, s2_s)
        sent(r1, h_s.at[0])
        sent(r2, h_s.at[1])
        sent(meta.at[pl.ds(0, nx - 1)], me_s)
        sent(own_rows(tin, r), t_s)
        sent(xs.at[r], q_s)

        @pl.when(r == end_core)
        def _():
            sent(lrec.at[0, pl.ds(0, nx - 1)], l_s)
            sent(drecv0, p_s)
            sent(gat.at[pl.ds(0, nt - 1), pl.ds(0, nx - 1)], g_s)
            sent(zrec.at[pl.ds(0, nt - 1), pl.ds(0, nt - 1)], z_s)

        @pl.when(r != end_core)
        def _():
            sent(lrec.at[0], l_s)
            sent(drecv0.at[pl.ds(0, nt - 1)], p_s)
            sent(gat.at[:, pl.ds(0, nx - 1)], g_s)
            sent(zrec.at[:, pl.ds(0, nt - 1)], z_s)

        @pl.when(here)
        def _():
            sent(xs.at[r, pl.ds(0, nx - 1)], x_s)

        @pl.when(away)
        def _():
            sent(xs.at[r], x_s)

    stages = {
        "fw": forward, "rb": reduce_second, "ra": reduce_first, "up": up_chunk, "co": collect,
        "dn": down_chunk, "pr": pair_chunk, "ps": pass_chunk, "mx": mixed_chunk, "drain": drain,
        "pe": last_own, "tw": tower_rows, "tf": share_rows,
    }
    for core in range(nr):
        for name in ("pr", "ps", "mx"):
            stages[f"{name}{core}"] = functools.partial(stages[name], only=core)
    order = []
    for i in range(chunks + 4):
        order += [("up", i), ("ra", i - 1), ("rb", i - 2), ("fw", i - 3), ("co", i - 4), ("dn", i - 4)]
        if i < chunks + 3:
            order += [("pr0", i - 4), ("pr1", i - 5)]
            if i < chunks + 2:
                order += [("ps0", i - 5)]
            order += [("ps1", i - 6), ("mx0", i - 7), ("mx1", i - 7)]
    n = last
    order += [("pr1", n - 1), ("ps0", n - 2), ("ps1", n - 2), ("mx0", n - 3), ("ps0", n - 1), ("mx0", n - 2), ("mx1", n - 3),
              ("ps1", n - 1), ("pe", n), ("mx1", n - 2), ("ps", n), ("mx0", n - 1), ("mx1", n - 1), ("drain", n), ("mx", n)]
    order.insert(order.index(("up", 2)) + 1, ("tw", last))
    order.insert(order.index(("dn", last)) + 1, ("tf", last))
    for name, c in order:
        if not 0 <= c < chunks or (c == last and name[-1].isdigit()):
            continue
        if name == "dn" and c == 0:
            for load in loads[1:2] + loads[3:]:
                load.wait()
        with jax.named_scope(f"{name}_{c}"):
            if name in ("fw", "rb", "ra", "co"):
                for h in range(2):
                    stages[name](c, h)
            else:
                stages[name](c)
    half = tok // nr
    fewer = half - unit
    with jax.named_scope("mout"):
        @pl.when(r == end_core)
        def _():
            got(rows_out.at[pl.ds(0, half)], m_r)

        @pl.when(r != end_core)
        def _():
            got(rows_out.at[pl.ds(0, fewer)], m_r)
    out = rows_out[...].T
    mixed_ref[...] = jnp.where(r == 0, out[:feat], out[feat:])
    with jax.named_scope("fin"):
        @pl.when(t == own_t)
        def _():
            at = pl.ds(pl.multiple_of((own_t * nr + r) * unit, unit), unit)
            got(ow.at[:, pl.ds(0, nt - 1)], o_r)

            @pl.when(r != end_core)
            def _():
                got(owt, v_r)
            pre = jnp.dot(rows_out[at, :], tin[...], preferred_element_type=F32)
            for q in range(own_t):
                total = ow[q, 0].astype(F32)
                for src in range(1, nt):
                    total = total + ow[q, src].astype(F32)
                pre = pre + jnp.dot(total.astype(BF16), owt[q], preferred_element_type=F32)
            pre_ref[...] = pre

        @pl.when(t != own_t)
        def _():
            got(frecv.at[pl.ds(0, nt - 1)], f_r)
            pre = fsend[t].astype(F32)
            for d in range(1, nt):
                pre = pre + frecv[t ^ d].astype(F32)
            pre_ref[...] = pre
        pre = pre_ref[...]
    active = jnp.maximum(pre + bias_ref[...].reshape(1, tasks * th), 0.0)
    outs = []
    for j in range(tasks):
        outs.append(jnp.sum(active[:, j * th:(j + 1) * th] * tout_ref[j:j + 1, :], axis=1, keepdims=True))
    lane = lax.broadcasted_iota(jnp.int32, (unit, 128), 1)
    logits = jnp.zeros((unit, 128), F32)
    for j in range(tasks):
        logits = jnp.where(lane == j, outs[j] + ob_ref[j], logits)
    scores_ref[...] = jax.nn.sigmoid(logits.T[:tasks, :])
    with jax.named_scope("end"):
        @pl.when(r == end_core)
        def _():
            sent(zrec.at[0], zl_s.at[0])
            sent(zrec.at[1, pl.ds(0, nt - 1)], zl_s.at[1])
            sent(rows_out.at[pl.ds(0, fewer)], m_s)

        @pl.when(r != end_core)
        def _():
            sent(rows_out.at[pl.ds(0, half)], m_s)
        @pl.when(t == own_t)
        def _():
            sent(frecv.at[pl.ds(0, nt - 1)], f_s)

        @pl.when(t != own_t)
        def _():
            sent(frecv.at[pl.ds(0, nt - 2)], f_s)
            sent(ow.at[0, pl.ds(0, nt - 1)], o_s)

        @pl.when(jnp.logical_and(r == end_core, t == own_t))
        def _():
            sent(owt, v_s)

        @pl.when(jnp.logical_and(r == end_core, t != own_t))
        def _():
            sent(tin, w_s)


def emit_kernel(mixed_in, scores_in, mixed_out, scores_out, sem):
    copies = [
        pltpu.make_async_copy(mixed_in, mixed_out, sem.at[0]),
        pltpu.make_async_copy(scores_in, scores_out, sem.at[1]),
    ]
    for copy in copies:
        copy.start()
    for copy in copies:
        copy.wait()


def stay_device(requests, expert_ids, gate_values, w_up, w_down, tower_in, tower_bias, tower_out,
                out_bias):
    nx, nt, nr = lax.axis_size("expert"), lax.axis_size("tensor"), lax.axis_size("rep")
    experts, _, hid_cols = w_up.shape
    tok, feat = requests.shape
    tasks, th = tower_out.shape
    hcols = hid_cols // 2
    unit = tok // (nt * nr)
    sizes = (nr,) * (nt - 1) + (1,) * nr
    C = len(sizes)
    dims = (nx, nt, nr, experts, tok, feat, hcols, tasks, th, unit, sizes)
    vmem = pl.BlockSpec(memory_space=pltpu.VMEM)
    hbm = pl.BlockSpec(memory_space=pltpu.HBM)
    smem = pl.BlockSpec(memory_space=pltpu.SMEM)
    dma = pltpu.SemaphoreType.DMA
    wide = nr * feat
    scratch = [
        pltpu.VMEM((feat, tok), BF16), pltpu.VMEM((2, tok), jnp.int32), pltpu.VMEM((2, tok), F32),
        pltpu.VMEM(tower_bias.shape, F32), pltpu.VMEM(tower_out.shape, F32),
        pltpu.VMEM(w_up.shape, BF16), pltpu.VMEM(w_down.shape, BF16),
        pltpu.VMEM((wide, tower_in.shape[1]), BF16),
        pltpu.VMEM((8, tok), F32), pltpu.VMEM((nx, 8, tok), F32),
        pltpu.VMEM((tok, feat), BF16), pltpu.VMEM((nr, nx, tok, feat), BF16),
        pltpu.VMEM((2, nx, 2 * tok, hcols), BF16),
        pltpu.VMEM((2, 2, 2 * tok, hcols), BF16),
        pltpu.VMEM((2, 2 * tok, hcols), BF16), pltpu.VMEM((2, 2 * tok, hcols), BF16),
        pltpu.VMEM((2, nx, 2 * tok, hcols), BF16),
        pltpu.VMEM((nt, nx, unit, wide), F32), pltpu.VMEM((C, nx, unit, wide), BF16),
        pltpu.VMEM((nt, nx, unit, wide), BF16), pltpu.VMEM((nt, nx, unit, wide), BF16),
        pltpu.VMEM((nt, nx, unit, wide), BF16), pltpu.VMEM((nt, nt, unit, wide), BF16),
        pltpu.VMEM((nt, unit, tasks * th), BF16), pltpu.VMEM((nt, unit, tasks * th), BF16),
        pltpu.VMEM((tok, wide), BF16),
        pltpu.VMEM((nr, nx, unit, wide), BF16), pltpu.VMEM((nx, unit, wide), BF16),
        pltpu.VMEM((nt, unit, wide), BF16),
        pltpu.VMEM((nt - 1, nt, unit, wide), BF16),
        pltpu.VMEM((nt - 1, wide, tower_in.shape[1]), BF16),
        pltpu.VMEM((unit, tower_in.shape[1]), F32),
        dma((8,)), dma, dma, dma, dma((C,)), dma, dma((C,)),
        dma, dma((C, 2)), dma, dma((C, 2)), dma((2,)), dma((C, 2, 2)),
        dma, dma((nt,)), dma, dma((nt,)), dma, dma((nt,)), dma, dma, dma, dma, dma, dma,
        dma, dma((nx,)), dma((2,)), dma, dma, dma, dma, dma, dma, dma,
    ]
    mixed, scores = pl.pallas_call(
        functools.partial(stay_kernel, dims),
        out_shape=(pltpu.VMEM((feat, tok), BF16), pltpu.VMEM((tasks, unit), F32)),
        in_specs=[hbm] * 8 + [smem],
        out_specs=(vmem, vmem),
        scratch_shapes=scratch,
        compiler_params=pltpu.CompilerParams(
            has_side_effects=True, collective_id=0, vmem_limit_bytes=60 << 20),
        name="stay",
    )(requests.T, expert_ids.T, gate_values.T, w_up, w_down, tower_in, tower_bias, tower_out, out_bias)
    mixed, scores = pl.pallas_call(
        emit_kernel,
        out_shape=(jax.ShapeDtypeStruct(mixed.shape, BF16), jax.ShapeDtypeStruct(scores.shape, F32)),
        in_specs=[vmem, vmem],
        out_specs=(hbm, hbm),
        scratch_shapes=[dma((2,))],
        name="emit",
    )(pltpu.with_memory_space_constraint(mixed, pltpu.VMEM), pltpu.with_memory_space_constraint(scores, pltpu.VMEM))
    return mixed.T, scores


def weights_stay(mesh):
    return mesh.shape["expert"] == 4 and mesh.shape["tensor"] == 4 and mesh.shape["rep"] == 2


def tower_head(pre, tower_bias, tower_out, out_bias):
    active = jax.nn.relu(pre + tower_bias[None, :])
    active = active.reshape(pre.shape[0], tower_out.shape[0], tower_out.shape[1])
    logits = jnp.sum(active * tower_out[None, :, :], axis=2) + out_bias[None, :]
    return jax.nn.sigmoid(logits).T


def per_device(
    requests, expert_ids, gate_values, w_up, w_down, tower_in, tower_bias, tower_out, out_bias
):
    groups = lax.axis_size("expert")
    experts = w_up.shape[0]
    local_experts = experts // groups
    tok_rows = requests.shape[0]
    capacity = 3 * tok_rows // experts
    serve_up, serve_down = (
        lax.all_to_all(w_up, "expert", split_axis=0, concat_axis=1, tiled=True),
        lax.all_to_all(w_down, "expert", split_axis=0, concat_axis=1, tiled=True),
    )
    flat_ids = expert_ids.reshape(-1)
    onehot = (flat_ids[:, None] == jnp.arange(experts, dtype=jnp.int32)[None, :]).astype(jnp.int32)
    before = jnp.cumsum(onehot, axis=0) - onehot
    slot_rank = jnp.sum(before * onehot, axis=1)
    slots = (flat_ids * capacity + slot_rank).reshape(tok_rows, 2)
    slot_index = jnp.arange(experts * capacity, dtype=jnp.int32)
    spread = (
        (slot_index[:, None] == slots[None, :, 0]) | (slot_index[:, None] == slots[None, :, 1])
    ).astype(jnp.bfloat16)
    full_rows = lax.all_gather(requests, ("tensor", "rep"), axis=1, tiled=True)
    outgoing = jnp.dot(spread, full_rows, preferred_element_type=jnp.float32).astype(jnp.bfloat16)
    incoming = lax.all_to_all(outgoing, "expert", split_axis=0, concat_axis=0, tiled=True)
    shaped = incoming.reshape(groups, local_experts, capacity, incoming.shape[1])
    hidden_pre = jnp.einsum("secd,edh->sech", shaped, serve_up, preferred_element_type=jnp.float32)
    hidden = jax.nn.relu(hidden_pre).astype(jnp.bfloat16)
    partial_value = jnp.einsum(
        "sech,edh->secd", hidden, serve_down, preferred_element_type=jnp.float32
    )
    summed = lax.psum_scatter(
        partial_value.astype(jnp.bfloat16), ("tensor", "rep"), scatter_dimension=3, tiled=True
    ).astype(jnp.float32)
    expert_out = summed.astype(jnp.bfloat16).reshape(
        groups * local_experts * capacity, summed.shape[3]
    )
    returned = lax.all_to_all(expert_out, "expert", split_axis=0, concat_axis=0, tiled=True)
    pick_first = (slots[:, 0:1] == slot_index[None, :]).astype(jnp.bfloat16)
    pick_second = (slots[:, 1:2] == slot_index[None, :]).astype(jnp.bfloat16)
    first = jnp.dot(pick_first, returned, preferred_element_type=jnp.float32)
    second = jnp.dot(pick_second, returned, preferred_element_type=jnp.float32)
    mixed = (gate_values[:, 0:1] * first + gate_values[:, 1:2] * second).astype(jnp.bfloat16)
    pre = lax.psum_scatter(
        jnp.dot(mixed, tower_in, preferred_element_type=jnp.float32).astype(jnp.bfloat16),
        ("tensor", "rep"),
        scatter_dimension=0,
        tiled=True,
    ).astype(jnp.float32)
    scores = tower_head(pre, tower_bias, tower_out, out_bias)
    return (mixed, scores)


def solution(mesh):
    in_specs = (
        P("expert", ("tensor", "rep")),
        P("expert", None),
        P("expert", None),
        P(None, "expert", ("tensor", "rep")),
        P(None, "expert", ("tensor", "rep")),
        P(("tensor", "rep"), None),
        P(),
        P(),
        P(),
    )
    out_specs = (P("expert", ("tensor", "rep")), P(None, ("expert", "tensor", "rep")))
    body = stay_device if weights_stay(mesh) else per_device
    return jax.shard_map(
        body, mesh=mesh, in_specs=in_specs, out_specs=out_specs, check_vma=False
    )
```

```python
import functools
import jax
import jax.numpy as jnp
from jax import lax
from jax.experimental import pallas as pl
from jax.experimental.pallas import tpu as pltpu
from jax.sharding import PartitionSpec as P

MESH = pl.DeviceIdType.MESH
F32 = jnp.float32
BF16 = jnp.bfloat16


def stay_kernel(
    dims, req_hbm, ids_hbm, gates_hbm, up_hbm, down_hbm, tin_hbm, bias_hbm, tout_hbm, ob_ref,
    mixed_ref, scores_ref,
    req_ref, ids_ref, gates_ref, bias_ref, tout_ref, up, down, tin, meta_ref, meta, rt, xs,
    hp, r1, s2, r2, hid, mine, dsend0, drecv0, dsend, gat, zrec, fsend, frecv, rows_out, lrec, lsum, zl, ow, owt, pre_ref,
    lsem, me_s, me_r, x_s, x_r, q_s, q_r, s1_s, s1_r, s2_s, s2_r, h_s, h_r,
    p_s, p_r, g_s, g_r, z_s, z_r, m_s, m_r, t_s, t_r, f_s, f_r, l_s, l_r, zl_s, zl_r, o_s, o_r, w_s, w_r, v_s, v_r,
):
    nx, nt, nr, experts, tok, feat, hcols, tasks, th, unit, sizes = dims
    xe, t, r = lax.axis_index("expert"), lax.axis_index("tensor"), lax.axis_index("rep")
    chunks = len(sizes)
    offs = [sum(sizes[:c]) * unit for c in range(chunks)]
    low = feat // 128 * 128
    rem = feat - low
    starts = [sum(sizes[:c]) for c in range(chunks)]
    extra = [unit if n > 1 or start % nr == 0 else 0 for n, start in zip(sizes, starts)]
    plan = [n * unit + e for n, e in zip(sizes, extra)]
    base = [sum(plan[:c]) for c in range(chunks)]
    subs = [n * unit for n in sizes]

    def remote(src, dst, ssem, rsem, dev):
        return pltpu.make_async_remote_copy(
            src_ref=src, dst_ref=dst, send_sem=ssem, recv_sem=rsem, device_id=dev,
            device_id_type=MESH)

    def send(src, dst, ssem, rsem, dev):
        remote(src, dst, ssem, rsem, dev).start()

    def got(ref, rsem):
        remote(ref, ref, lsem.at[0], rsem, (xe, t, r)).wait_recv()

    def sent(ref, ssem):
        remote(ref, ref, ssem, lsem.at[0], (xe, t, r)).wait_send()

    first = [
        pltpu.make_async_copy(req_hbm, req_ref, lsem.at[3]),
        pltpu.make_async_copy(ids_hbm, ids_ref, lsem.at[4]),
        pltpu.make_async_copy(gates_hbm, gates_ref, lsem.at[5]),
    ]

    def own_rows(ref, k):
        return ref.at[pl.ds(pl.multiple_of(k * feat, feat), feat)]

    loads = [
        pltpu.make_async_copy(up_hbm, up, lsem.at[0]),
        pltpu.make_async_copy(down_hbm, down, lsem.at[1]),
        pltpu.make_async_copy(tin_hbm, own_rows(tin, r), lsem.at[2]),
        pltpu.make_async_copy(bias_hbm, bias_ref, lsem.at[6]),
        pltpu.make_async_copy(tout_hbm, tout_ref, lsem.at[7]),
    ]
    first[0].start()
    here = t == xe
    away = jnp.logical_not(here)
    partner = (xe, t, 1 - r)
    barrier = pltpu.get_barrier_semaphore()

    def greet(dev):
        pl.semaphore_signal(barrier, inc=1, device_id=dev, device_id_type=MESH)

    me = t * nr + r
    for d in reversed(range(1, nt * nr)):
        other = me ^ d
        greet((xe, lax.div(other, nr), lax.rem(other, nr)))
    for d in range(1, nx):
        for k in range(nr):
            greet((xe ^ d, t, k))
    hub = nr - 1

    @pl.when(r == hub)
    def _():
        for b in range(nx):
            for k in range(hub):
                greet((b, xe, k))

            @pl.when(jnp.logical_not(jnp.logical_and(here, xe == b)))
            def _():
                greet((b, xe, hub))
    for load in first[1:] + loads:
        load.start()
    first[0].wait()
    full = req_ref[...].T
    for c in range(chunks):
        rt[base[c]:base[c] + subs[c], :] = full[offs[c]:offs[c] + subs[c], :low]
        if extra[c]:
            rt[base[c] + subs[c]:base[c] + plan[c], :] = jnp.concatenate(
                [full[offs[c] + k * unit:offs[c] + (k + 1) * unit, low:] for k in range(nr)], axis=1)
    greeted = (nt * nr - 1) + (nx - 1) * nr + nt

    with jax.named_scope("barr"):
        @pl.when(jnp.logical_and(here, r == hub))
        def _():
            pl.semaphore_wait(barrier, greeted - 1)

        @pl.when(jnp.logical_or(away, r != hub))
        def _():
            pl.semaphore_wait(barrier, greeted)

    def span(c):
        return pl.ds(base[c], plan[c])

    for c in range(chunks):
        for tt in reversed(range(nt)):
            @pl.when(jnp.logical_not(jnp.logical_and(jnp.logical_and(here, t == tt), r == hub)))
            def _():
                send(rt.at[span(c)], xs.at[r, xe, span(c)], x_s, x_r.at[r, c], (t, tt, hub))
        if c == 0:
            for load in first[1:]:
                load.wait()
            meta_ref[...] = jnp.concatenate(
                [ids_ref[...].astype(F32), gates_ref[...], jnp.zeros((4, tok), F32)], axis=0)
            for d in range(1, nx):
                send(meta_ref, meta.at[xe], me_s, me_r, (xe ^ d, t, r))
    send(tin_hbm, own_rows(tin, r), t_s, t_r, partner)
    meta[xe] = meta_ref[...]

    @pl.when(jnp.logical_and(here, r == hub))
    def _():
        xs[hub, xe] = rt[...]

    def take(c):
        @pl.when(r == hub)
        def _():
            for k in range(hub):
                got(xs.at[k, :, span(c)], x_r.at[k, c])

            @pl.when(here)
            def _():
                got(xs.at[hub, pl.ds(0, nx - 1), span(c)], x_r.at[hub, c])

            @pl.when(away)
            def _():
                got(xs.at[hub, :, span(c)], x_r.at[hub, c])
            send(xs.at[:, :, span(c)], xs.at[:, :, span(c)], q_s, q_r.at[c], partner)

    with jax.named_scope("take0"):
        take(0)
    with jax.named_scope("meta"):
        got(meta.at[pl.ds(0, nx - 1)], me_r)
        info = [meta[b].T for b in range(nx)]

    def column(c, j):
        return jnp.concatenate(
            [info[b][offs[c]:offs[c] + subs[c], j:j + 1] for b in range(nx)], axis=0)

    near = (1, 2)

    def picks(c, k=None):
        if k is None:
            return pl.ds(2 * offs[c], 2 * subs[c])
        return pl.ds(2 * offs[c] + k * subs[c], subs[c])

    def up_chunk(c):
        sub = subs[c]
        @pl.when(r != hub)
        def _():
            got(xs.at[:, :, span(c)], q_r.at[c])
        if c == 0:
            loads[0].wait()
        from_chunk = c if extra[c] else c - 1
        tail_at = base[from_chunk] + subs[from_chunk]
        first_unit = starts[c] % nr
        rows = []
        for k in range(nr):
            parts = []
            for b in range(nx):
                main = xs[k, b, base[c]:base[c] + sub, :]
                side = xs[k, b, tail_at:tail_at + unit, :]
                side = [side[:, u * rem:(u + 1) * rem] for u in range(first_unit, first_unit + sizes[c])]
                side = side[0] if len(side) == 1 else jnp.concatenate(side, axis=0)
                parts.append(jnp.concatenate([main, side], axis=1))
            rows.append(jnp.concatenate(parts, axis=0))
        ids = (column(c, 0), column(c, 1))
        for h in range(2):
            picked = [jnp.zeros((nx * sub, hcols), F32)] * 2
            for e in range(experts):
                part = None
                for k in range(nr):
                    one = jnp.dot(rows[k], up[e, k * feat:(k + 1) * feat, h * hcols:(h + 1) * hcols],
                                  preferred_element_type=F32)
                    part = one if part is None else part + one
                picked = [jnp.where(ids[k] == float(e), part, picked[k]) for k in range(2)]
            for k in range(2):
                hp[h, :, picks(c, k), :] = picked[k].astype(BF16).reshape(nx, sub, hcols)
            fa, fb = near[h], near[1 - h]
            for i, q, sem in ((0, xe ^ fa ^ fb, s1_r), (1, xe ^ fa, s2_r)):
                send(hp.at[h, q, picks(c)], r1.at[h, i, picks(c)], s1_s, sem.at[c],
                     (xe ^ fa, t, r))
        if c + 1 < chunks:
            take(c + 1)

    def reduce_first(c, h):
        fa, fb = near[h], near[1 - h]
        if h == 0:
            got(r1.at[:, 0, picks(c)], s1_r.at[c])
        s2[h, picks(c)] = (hp[h, xe ^ fb, picks(c)].astype(F32)
                           + r1[h, 0, picks(c)].astype(F32)).astype(BF16)
        send(s2.at[h, picks(c)], r2.at[h, picks(c)], s2_s, s2_r.at[c], (xe ^ fb, t, r))

    def reduce_second(c, h):
        fa, fb = near[h], near[1 - h]
        if h == 0:
            got(r1.at[:, :, picks(c)], s2_r.at[c])
        total = (hp[h, xe, picks(c)].astype(F32) + r1[h, 1, picks(c)].astype(F32)
                 + r2[h, picks(c)].astype(F32))
        hid[h, xe, picks(c)] = jnp.maximum(total, 0.0).astype(BF16)
        mine_ref = hid.at[h, xe, picks(c)]
        send(mine_ref, mine_ref, h_s.at[0], h_r.at[c, 0], (xe ^ fb, t, r))
        send(mine_ref, mine_ref, h_s.at[0], h_r.at[c, 1], (xe ^ fa, t, r))

    def forward(c, h):
        fa, fb = near[h], near[1 - h]
        ref = hid.at[h, xe ^ fb, picks(c)]
        if h == 0:
            got(hid.at[:, 0, picks(c)], h_r.at[c, 0])
        send(ref, ref, h_s.at[1], h_r.at[c, 1], (xe ^ fa, t, r))

    def collect(c, h):
        if h == 0:
            got(hid.at[:, pl.ds(0, 2), picks(c)], h_r.at[c, 1])

    last = chunks - 1
    own_t = nt - 1

    def to_owner(source):
        for q in range(own_t):
            @pl.when(t != own_t)
            def _():
                send(source(q), ow.at[q, t], o_s, o_r, (xe, own_t, r))

            @pl.when(t == own_t)
            def _():
                ow[q, own_t] = source(q)[...]

    def tower_rows(c):
        loads[2].wait()
        got(own_rows(tin, 1 - r), t_r)

        @pl.when(jnp.logical_and(r == end_core, t != own_t))
        def _():
            send(tin, owt.at[t], w_s, w_r, (xe, own_t, r))

    def share_rows(c):
        @pl.when(jnp.logical_and(r == end_core, t == own_t))
        def _():
            got(owt, w_r)
            send(owt, owt, v_s, v_r, partner)

    end_core = (sum(sizes) - 1) % nr
    final_rows = pl.ds((sum(sizes) - 1) * unit, unit)

    def parity(c):
        return sum(sizes[:c]) % nr if sizes[c] == 1 else None

    def slot(c, core):
        start = sum(sizes[:c])
        if sizes[c] == 1 or start % nr == 0:
            return start // nr
        return start // nr + 1 - core

    def if_core(c, other, body, only=None):
        p = parity(c)
        if p is None:
            if only is None:
                body()
            else:
                pl.when(r == only)(body)
        elif only is None or only == p:
            pl.when(r == (1 - p if other else p))(body)

    def down_chunk(c):
        sub = subs[c]
        ids = (column(c, 0), column(c, 1))
        gates = (column(c, 2), column(c, 3))
        total = jnp.zeros((nx * sub, nr * feat), F32)
        for e in range(experts):
            hit = (ids[0] == float(e), ids[1] == float(e))
            weight = jnp.where(hit[0], gates[0], 0.0) + jnp.where(hit[1], gates[1], 0.0)
            part = None
            for h in range(2):
                values = [hid[h, :, picks(c, k), :].reshape(nx * sub, hcols) for k in range(2)]
                chosen = jnp.where(hit[0], values[0], jnp.where(hit[1], values[1], jnp.zeros_like(values[1])))
                one = lax.dot_general(chosen, down[e, :, h * hcols:(h + 1) * hcols],
                                      (((1,), (1,)), ((), ())), preferred_element_type=F32)
                part = one if part is None else part + one
            total = total + weight * part
        total = total.reshape(nx, sub, nr * feat)
        if c == last:
            dsend0[c] = total.astype(BF16)
            for d in (3, 1, 2):
                send(dsend0.at[c, xe ^ d], lrec.at[r, xe], l_s, l_r.at[d], (xe ^ d, t, end_core))

            @pl.when(r == end_core)
            def _():
                lrec[r, xe] = dsend0[c, xe]

            @pl.when(r != end_core)
            def _():
                send(dsend0.at[c, xe], lrec.at[r, xe], l_s, l_r.at[0], partner)
            return
        if sizes[c] == 1:
            keep = give = total
        else:
            lead = sum(sizes[:c]) % nr
            keep = jnp.where(r == lead, total[:, :unit], total[:, unit:])
            give = jnp.where(r == lead, total[:, unit:], total[:, :unit])

        def store():
            mine[slot(c, r)] = keep

        def give_away():
            at = slot(c, 1 - r)
            dsend0[c] = give.astype(BF16)
            send(dsend0.at[c], drecv0.at[at], p_s, p_r.at[at], partner)
        if_core(c, True, give_away)
        if_core(c, False, store)

    def last_sum(q):
        lsum[q] = (lrec[0, q].astype(F32) + lrec[1, q].astype(F32)).astype(BF16)
        send(lsum.at[q], zl.at[t], zl_s.at[0], zl_r, (xe, q, 1 - r))

        @pl.when(q != t)
        def _():
            send(lsum.at[q], zl.at[t], zl_s.at[1], zl_r, (xe, q, r))

        @pl.when(q == t)
        def _():
            zl[t] = lsum[q]

    def last_own(c):
        @pl.when(r == end_core)
        def _():
            got(lrec.at[1 - r, xe], l_r.at[0])
            last_sum(xe)

    def last_pass():
        for k in reversed(range(nt)):
            q = t ^ k

            @pl.when(q != xe)
            def _():
                got(lrec.at[:, q], l_r.at[q ^ xe])
                last_sum(q)
        to_owner(lambda q: lsum.at[q])

    def last_mixed():
        @pl.when(r == end_core)
        def _():
            got(zl.at[pl.ds(0, nt - 1)], zl_r)

        @pl.when(r != end_core)
        def _():
            got(zl, zl_r)
        total = zl[0].astype(F32)
        for src in range(1, nt):
            total = total + zl[src].astype(F32)
        value = total.astype(BF16)
        rows_out[final_rows, :] = value

    def pair_chunk(c, only=None):
        if c == last:
            return

        def body():
            s = slot(c, r)
            got(drecv0.at[s], p_r.at[s])
            dsend[s] = (mine[s] + drecv0[s].astype(F32)).astype(BF16)
            for d in (3, 1, 2):
                send(dsend.at[s, xe ^ d], gat.at[s, xe], g_s, g_r.at[s], (xe ^ d, t, r))
            gat[s, xe] = dsend[s, xe]

            @pl.when(away)
            def _():
                send(dsend.at[s, xe], zrec.at[s, t], z_s, z_r.at[s], (xe, xe, r))
        if_core(c, False, body, only)

    def pass_chunk(c, only=None):
        if c == last:
            pl.when(r == end_core)(last_pass)
            return

        def body():
            s = slot(c, r)
            got(gat.at[s, pl.ds(0, nx - 1)], g_r.at[s])
            for d in (1, 2, 3):
                q = xe ^ d

                @pl.when(q != t)
                def _():
                    send(gat.at[s, q], zrec.at[s, t], z_s, z_r.at[s], (xe, q, r))
            if c == last - 1:
                to_owner(lambda q: gat.at[s, q])
        if_core(c, False, body, only)

    def mixed_chunk(c, only=None):
        if c == last:
            return last_mixed()

        def body():
            s = slot(c, r)
            got(zrec.at[s, pl.ds(0, nt - 1)], z_r.at[s])
            total = gat[s, t].astype(F32)
            for d in range(1, nt):
                total = total + zrec[s, t ^ d].astype(F32)
            value = total.astype(BF16)
            at = pl.ds(pl.multiple_of((s * nr + r) * unit, unit), unit)
            rows_out[at, :] = value
            send(rows_out.at[at], rows_out.at[at], m_s, m_r, partner)
            if c == last - 1:
                return
            fsend[s] = jnp.dot(value, tin[...], preferred_element_type=F32).astype(BF16)

            @pl.when(t != s)
            def _():
                send(fsend.at[s], frecv.at[t], f_s, f_r, (xe, s, r))
        if_core(c, False, body, only)

    def drain(c):
        sent(r1, s1_s)
        sent(r2, s2_s)
        sent(r1, h_s.at[0])
        sent(r2, h_s.at[1])
        sent(meta.at[pl.ds(0, nx - 1)], me_s)
        sent(own_rows(tin, r), t_s)

        @pl.when(r == hub)
        def _():
            sent(xs, q_s)


        @pl.when(r == end_core)
        def _():
            sent(lrec.at[0, pl.ds(0, nx - 1)], l_s)
            sent(drecv0, p_s)
            sent(gat.at[pl.ds(0, nt - 1), pl.ds(0, nx - 1)], g_s)
            sent(zrec.at[pl.ds(0, nt - 1), pl.ds(0, nt - 1)], z_s)

        @pl.when(r != end_core)
        def _():
            sent(lrec.at[0], l_s)
            sent(drecv0.at[pl.ds(0, nt - 1)], p_s)
            sent(gat.at[:, pl.ds(0, nx - 1)], g_s)
            sent(zrec.at[:, pl.ds(0, nt - 1)], z_s)

        @pl.when(jnp.logical_and(here, r == hub))
        def _():
            sent(xs.at[r, pl.ds(0, nx - 1)], x_s)

        @pl.when(jnp.logical_or(away, r != hub))
        def _():
            sent(xs.at[r], x_s)

    stages = {
        "fw": forward, "rb": reduce_second, "ra": reduce_first, "up": up_chunk, "co": collect,
        "dn": down_chunk, "pr": pair_chunk, "ps": pass_chunk, "mx": mixed_chunk, "drain": drain,
        "pe": last_own, "tw": tower_rows, "tf": share_rows,
    }
    for core in range(nr):
        for name in ("pr", "ps", "mx"):
            stages[f"{name}{core}"] = functools.partial(stages[name], only=core)
    order = []
    n = last
    for i in range(n):
        order += [("up", i), ("ra", i - 1), ("rb", i - 2), ("fw", i - 3)]
    order += [("up", n), ("ra", n - 1), ("rb", n - 2), ("fw", n - 3), ("ra", n), ("co", n - 4), ("dn", n - 4), ("pr0", n - 4),
              ("rb", n - 1), ("fw", n - 2), ("rb", n), ("co", n - 3), ("dn", n - 3), ("pr0", n - 3), ("pr1", n - 4), ("ps0", n - 4),
              ("fw", n - 1), ("fw", n), ("co", n - 2), ("dn", n - 2), ("pr0", n - 2), ("pr1", n - 3), ("ps0", n - 3), ("ps1", n - 4),
              ("co", n - 1), ("dn", n - 1), ("pr0", n - 1), ("pr1", n - 2), ("ps1", n - 3), ("mx0", n - 4), ("mx1", n - 4),
              ("co", n), ("dn", n)]
    order += [("pr1", n - 1), ("ps0", n - 2), ("ps1", n - 2), ("mx0", n - 3), ("ps0", n - 1), ("mx0", n - 2), ("mx1", n - 3),
              ("ps1", n - 1), ("pe", n), ("mx1", n - 2), ("ps", n), ("mx0", n - 1), ("mx1", n - 1), ("drain", n), ("mx", n)]
    order.insert(order.index(("up", 2)) + 1, ("tw", last))
    order.insert(order.index(("dn", last)) + 1, ("tf", last))
    for name, c in order:
        if not 0 <= c < chunks or (c == last and name[-1].isdigit()):
            continue
        if name == "dn" and c == 0:
            for load in loads[1:2] + loads[3:]:
                load.wait()
        with jax.named_scope(f"{name}_{c}"):
            if name in ("fw", "rb", "ra", "co"):
                for h in range(2):
                    stages[name](c, h)
            else:
                stages[name](c)
    half = tok // nr
    fewer = half - unit
    with jax.named_scope("mout"):
        @pl.when(r == end_core)
        def _():
            got(rows_out.at[pl.ds(0, half)], m_r)

        @pl.when(r != end_core)
        def _():
            got(rows_out.at[pl.ds(0, fewer)], m_r)
    out = rows_out[...].T
    mixed_ref[...] = jnp.where(r == 0, out[:feat], out[feat:])
    with jax.named_scope("fin"):
        @pl.when(t == own_t)
        def _():
            at = pl.ds(pl.multiple_of((own_t * nr + r) * unit, unit), unit)
            got(ow.at[:, pl.ds(0, nt - 1)], o_r)

            @pl.when(r != end_core)
            def _():
                got(owt, v_r)
            pre = jnp.dot(rows_out[at, :], tin[...], preferred_element_type=F32)
            for q in range(own_t):
                total = ow[q, 0].astype(F32)
                for src in range(1, nt):
                    total = total + ow[q, src].astype(F32)
                pre = pre + jnp.dot(total.astype(BF16), owt[q], preferred_element_type=F32)
            pre_ref[...] = pre

        @pl.when(t != own_t)
        def _():
            got(frecv.at[pl.ds(0, nt - 1)], f_r)
            pre = fsend[t].astype(F32)
            for d in range(1, nt):
                pre = pre + frecv[t ^ d].astype(F32)
            pre_ref[...] = pre
        pre = pre_ref[...]
    active = jnp.maximum(pre + bias_ref[...].reshape(1, tasks * th), 0.0)
    outs = []
    for j in range(tasks):
        outs.append(jnp.sum(active[:, j * th:(j + 1) * th] * tout_ref[j:j + 1, :], axis=1, keepdims=True))
    lane = lax.broadcasted_iota(jnp.int32, (unit, 128), 1)
    logits = jnp.zeros((unit, 128), F32)
    for j in range(tasks):
        logits = jnp.where(lane == j, outs[j] + ob_ref[j], logits)
    scores_ref[...] = jax.nn.sigmoid(logits.T[:tasks, :])
    with jax.named_scope("end"):
        @pl.when(r == end_core)
        def _():
            sent(zrec.at[0], zl_s.at[0])
            sent(zrec.at[1, pl.ds(0, nt - 1)], zl_s.at[1])
            sent(rows_out.at[pl.ds(0, fewer)], m_s)

        @pl.when(r != end_core)
        def _():
            sent(rows_out.at[pl.ds(0, half)], m_s)
        @pl.when(t == own_t)
        def _():
            sent(frecv.at[pl.ds(0, nt - 1)], f_s)

        @pl.when(t != own_t)
        def _():
            sent(frecv.at[pl.ds(0, nt - 2)], f_s)
            sent(ow.at[0, pl.ds(0, nt - 1)], o_s)

        @pl.when(jnp.logical_and(r == end_core, t == own_t))
        def _():
            sent(owt, v_s)

        @pl.when(jnp.logical_and(r == end_core, t != own_t))
        def _():
            sent(tin, w_s)


def emit_kernel(mixed_in, scores_in, mixed_out, scores_out, sem):
    copies = [
        pltpu.make_async_copy(mixed_in, mixed_out, sem.at[0]),
        pltpu.make_async_copy(scores_in, scores_out, sem.at[1]),
    ]
    for copy in copies:
        copy.start()
    for copy in copies:
        copy.wait()


def stay_device(requests, expert_ids, gate_values, w_up, w_down, tower_in, tower_bias, tower_out,
                out_bias):
    nx, nt, nr = lax.axis_size("expert"), lax.axis_size("tensor"), lax.axis_size("rep")
    experts, _, hid_cols = w_up.shape
    tok, feat = requests.shape
    tasks, th = tower_out.shape
    hcols = hid_cols // 2
    unit = tok // (nt * nr)
    sizes = (nr,) * (nt - 1) + (1,) * nr
    C = len(sizes)
    dims = (nx, nt, nr, experts, tok, feat, hcols, tasks, th, unit, sizes)
    vmem = pl.BlockSpec(memory_space=pltpu.VMEM)
    hbm = pl.BlockSpec(memory_space=pltpu.HBM)
    smem = pl.BlockSpec(memory_space=pltpu.SMEM)
    dma = pltpu.SemaphoreType.DMA
    wide = nr * feat
    scratch = [
        pltpu.VMEM((feat, tok), BF16), pltpu.VMEM((2, tok), jnp.int32), pltpu.VMEM((2, tok), F32),
        pltpu.VMEM(tower_bias.shape, F32), pltpu.VMEM(tower_out.shape, F32),
        pltpu.VMEM(w_up.shape, BF16), pltpu.VMEM(w_down.shape, BF16),
        pltpu.VMEM((wide, tower_in.shape[1]), BF16),
        pltpu.VMEM((8, tok), F32), pltpu.VMEM((nx, 8, tok), F32),
        pltpu.VMEM((tok * feat // 128, 128), BF16), pltpu.VMEM((nr, nx, tok * feat // 128, 128), BF16),
        pltpu.VMEM((2, nx, 2 * tok, hcols), BF16),
        pltpu.VMEM((2, 2, 2 * tok, hcols), BF16),
        pltpu.VMEM((2, 2 * tok, hcols), BF16), pltpu.VMEM((2, 2 * tok, hcols), BF16),
        pltpu.VMEM((2, nx, 2 * tok, hcols), BF16),
        pltpu.VMEM((nt, nx, unit, wide), F32), pltpu.VMEM((C, nx, unit, wide), BF16),
        pltpu.VMEM((nt, nx, unit, wide), BF16), pltpu.VMEM((nt, nx, unit, wide), BF16),
        pltpu.VMEM((nt, nx, unit, wide), BF16), pltpu.VMEM((nt, nt, unit, wide), BF16),
        pltpu.VMEM((nt, unit, tasks * th), BF16), pltpu.VMEM((nt, unit, tasks * th), BF16),
        pltpu.VMEM((tok, wide), BF16),
        pltpu.VMEM((nr, nx, unit, wide), BF16), pltpu.VMEM((nx, unit, wide), BF16),
        pltpu.VMEM((nt, unit, wide), BF16),
        pltpu.VMEM((nt - 1, nt, unit, wide), BF16),
        pltpu.VMEM((nt - 1, wide, tower_in.shape[1]), BF16),
        pltpu.VMEM((unit, tower_in.shape[1]), F32),
        dma((8,)), dma, dma, dma, dma((nr, C)), dma, dma((C,)),
        dma, dma((C,)), dma, dma((C,)), dma((2,)), dma((C, 2)),
        dma, dma((nt,)), dma, dma((nt,)), dma, dma((nt,)), dma, dma, dma, dma, dma, dma,
        dma, dma((nx,)), dma((2,)), dma, dma, dma, dma, dma, dma, dma,
    ]
    mixed, scores = pl.pallas_call(
        functools.partial(stay_kernel, dims),
        out_shape=(pltpu.VMEM((feat, tok), BF16), pltpu.VMEM((tasks, unit), F32)),
        in_specs=[hbm] * 8 + [smem],
        out_specs=(vmem, vmem),
        scratch_shapes=scratch,
        compiler_params=pltpu.CompilerParams(
            has_side_effects=True, collective_id=0, vmem_limit_bytes=60 << 20),
        name="stay",
    )(requests.T, expert_ids.T, gate_values.T, w_up, w_down, tower_in, tower_bias, tower_out, out_bias)
    mixed, scores = pl.pallas_call(
        emit_kernel,
        out_shape=(jax.ShapeDtypeStruct(mixed.shape, BF16), jax.ShapeDtypeStruct(scores.shape, F32)),
        in_specs=[vmem, vmem],
        out_specs=(hbm, hbm),
        scratch_shapes=[dma((2,))],
        name="emit",
    )(pltpu.with_memory_space_constraint(mixed, pltpu.VMEM), pltpu.with_memory_space_constraint(scores, pltpu.VMEM))
    return mixed.T, scores


def weights_stay(mesh):
    return mesh.shape["expert"] == 4 and mesh.shape["tensor"] == 4 and mesh.shape["rep"] == 2


def tower_head(pre, tower_bias, tower_out, out_bias):
    active = jax.nn.relu(pre + tower_bias[None, :])
    active = active.reshape(pre.shape[0], tower_out.shape[0], tower_out.shape[1])
    logits = jnp.sum(active * tower_out[None, :, :], axis=2) + out_bias[None, :]
    return jax.nn.sigmoid(logits).T


def per_device(
    requests, expert_ids, gate_values, w_up, w_down, tower_in, tower_bias, tower_out, out_bias
):
    groups = lax.axis_size("expert")
    experts = w_up.shape[0]
    local_experts = experts // groups
    tok_rows = requests.shape[0]
    capacity = 3 * tok_rows // experts
    serve_up, serve_down = (
        lax.all_to_all(w_up, "expert", split_axis=0, concat_axis=1, tiled=True),
        lax.all_to_all(w_down, "expert", split_axis=0, concat_axis=1, tiled=True),
    )
    flat_ids = expert_ids.reshape(-1)
    onehot = (flat_ids[:, None] == jnp.arange(experts, dtype=jnp.int32)[None, :]).astype(jnp.int32)
    before = jnp.cumsum(onehot, axis=0) - onehot
    slot_rank = jnp.sum(before * onehot, axis=1)
    slots = (flat_ids * capacity + slot_rank).reshape(tok_rows, 2)
    slot_index = jnp.arange(experts * capacity, dtype=jnp.int32)
    spread = (
        (slot_index[:, None] == slots[None, :, 0]) | (slot_index[:, None] == slots[None, :, 1])
    ).astype(jnp.bfloat16)
    full_rows = lax.all_gather(requests, ("tensor", "rep"), axis=1, tiled=True)
    outgoing = jnp.dot(spread, full_rows, preferred_element_type=jnp.float32).astype(jnp.bfloat16)
    incoming = lax.all_to_all(outgoing, "expert", split_axis=0, concat_axis=0, tiled=True)
    shaped = incoming.reshape(groups, local_experts, capacity, incoming.shape[1])
    hidden_pre = jnp.einsum("secd,edh->sech", shaped, serve_up, preferred_element_type=jnp.float32)
    hidden = jax.nn.relu(hidden_pre).astype(jnp.bfloat16)
    partial_value = jnp.einsum(
        "sech,edh->secd", hidden, serve_down, preferred_element_type=jnp.float32
    )
    summed = lax.psum_scatter(
        partial_value.astype(jnp.bfloat16), ("tensor", "rep"), scatter_dimension=3, tiled=True
    ).astype(jnp.float32)
    expert_out = summed.astype(jnp.bfloat16).reshape(
        groups * local_experts * capacity, summed.shape[3]
    )
    returned = lax.all_to_all(expert_out, "expert", split_axis=0, concat_axis=0, tiled=True)
    pick_first = (slots[:, 0:1] == slot_index[None, :]).astype(jnp.bfloat16)
    pick_second = (slots[:, 1:2] == slot_index[None, :]).astype(jnp.bfloat16)
    first = jnp.dot(pick_first, returned, preferred_element_type=jnp.float32)
    second = jnp.dot(pick_second, returned, preferred_element_type=jnp.float32)
    mixed = (gate_values[:, 0:1] * first + gate_values[:, 1:2] * second).astype(jnp.bfloat16)
    pre = lax.psum_scatter(
        jnp.dot(mixed, tower_in, preferred_element_type=jnp.float32).astype(jnp.bfloat16),
        ("tensor", "rep"),
        scatter_dimension=0,
        tiled=True,
    ).astype(jnp.float32)
    scores = tower_head(pre, tower_bias, tower_out, out_bias)
    return (mixed, scores)


def solution(mesh):
    in_specs = (
        P("expert", ("tensor", "rep")),
        P("expert", None),
        P("expert", None),
        P(None, "expert", ("tensor", "rep")),
        P(None, "expert", ("tensor", "rep")),
        P(("tensor", "rep"), None),
        P(),
        P(),
        P(),
    )
    out_specs = (P("expert", ("tensor", "rep")), P(None, ("expert", "tensor", "rep")))
    body = stay_device if weights_stay(mesh) else per_device
    return jax.shard_map(
        body, mesh=mesh, in_specs=in_specs, out_specs=out_specs, check_vma=False
    )
```

```python
import functools
import jax
import jax.numpy as jnp
from jax import lax
from jax.experimental import pallas as pl
from jax.experimental.pallas import tpu as pltpu
from jax.sharding import PartitionSpec as P

MESH = pl.DeviceIdType.MESH
F32 = jnp.float32
BF16 = jnp.bfloat16


def stay_kernel(
    dims, req_hbm, ids_hbm, gates_hbm, up_hbm, down_hbm, tin_hbm, bias_hbm, tout_hbm, ob_ref,
    mixed_ref, scores_ref,
    req_ref, ids_ref, gates_ref, bias_ref, tout_ref, up, down, tin, meta_ref, meta, rt, xs,
    hp, r1, s2, r2, hid, mine, dsend0, drecv0, dsend, gat, zrec, fsend, frecv, rows_out, lrec, lsum, zl, ow, owt, pre_ref,
    lsem, me_s, me_r, x_s, x_r, q_s, q_r, s1_s, s1_r, s2_s, s2_r, h_s, h_r,
    p_s, p_r, g_s, g_r, z_s, z_r, m_s, m_r, t_s, t_r, f_s, f_r, l_s, l_r, zl_s, zl_r, o_s, o_r, w_s, w_r, v_s, v_r,
):
    nx, nt, nr, experts, tok, feat, hcols, tasks, th, unit, sizes = dims
    xe, t, r = lax.axis_index("expert"), lax.axis_index("tensor"), lax.axis_index("rep")
    chunks = len(sizes)
    offs = [sum(sizes[:c]) * unit for c in range(chunks)]
    low = feat // 128 * 128
    rem = feat - low
    starts = [sum(sizes[:c]) for c in range(chunks)]
    extra = [unit if n > 1 or start % nr == 0 else 0 for n, start in zip(sizes, starts)]
    plan = [n * unit + e for n, e in zip(sizes, extra)]
    base = [sum(plan[:c]) for c in range(chunks)]
    subs = [n * unit for n in sizes]

    def remote(src, dst, ssem, rsem, dev):
        return pltpu.make_async_remote_copy(
            src_ref=src, dst_ref=dst, send_sem=ssem, recv_sem=rsem, device_id=dev,
            device_id_type=MESH)

    def send(src, dst, ssem, rsem, dev):
        remote(src, dst, ssem, rsem, dev).start()

    def got(ref, rsem):
        remote(ref, ref, lsem.at[0], rsem, (xe, t, r)).wait_recv()

    def sent(ref, ssem):
        remote(ref, ref, ssem, lsem.at[0], (xe, t, r)).wait_send()

    first = [
        pltpu.make_async_copy(req_hbm, req_ref, lsem.at[3]),
        pltpu.make_async_copy(ids_hbm, ids_ref, lsem.at[4]),
        pltpu.make_async_copy(gates_hbm, gates_ref, lsem.at[5]),
    ]

    def own_rows(ref, k):
        return ref.at[pl.ds(pl.multiple_of(k * feat, feat), feat)]

    loads = [
        pltpu.make_async_copy(up_hbm, up, lsem.at[0]),
        pltpu.make_async_copy(down_hbm, down, lsem.at[1]),
        pltpu.make_async_copy(tin_hbm, own_rows(tin, r), lsem.at[2]),
        pltpu.make_async_copy(bias_hbm, bias_ref, lsem.at[6]),
        pltpu.make_async_copy(tout_hbm, tout_ref, lsem.at[7]),
    ]
    first[0].start()
    here = t == xe
    away = jnp.logical_not(here)
    partner = (xe, t, 1 - r)
    barrier = pltpu.get_barrier_semaphore()

    def greet(dev):
        pl.semaphore_signal(barrier, inc=1, device_id=dev, device_id_type=MESH)

    me = t * nr + r
    for d in reversed(range(1, nt * nr)):
        other = me ^ d
        greet((xe, lax.div(other, nr), lax.rem(other, nr)))
    for d in range(1, nx):
        for k in range(nr):
            greet((xe ^ d, t, k))
    hub = nr - 1

    @pl.when(r == hub)
    def _():
        for b in range(nx):
            for k in range(hub):
                greet((b, xe, k))

            @pl.when(jnp.logical_not(jnp.logical_and(here, xe == b)))
            def _():
                greet((b, xe, hub))
    for load in first[1:] + loads:
        load.start()
    first[0].wait()
    full = req_ref[...].T
    for c in range(chunks):
        rt[base[c]:base[c] + subs[c], :] = full[offs[c]:offs[c] + subs[c], :low]
        if extra[c]:
            rt[base[c] + subs[c]:base[c] + plan[c], :] = jnp.concatenate(
                [full[offs[c] + k * unit:offs[c] + (k + 1) * unit, low:] for k in range(nr)], axis=1)
    greeted = (nt * nr - 1) + (nx - 1) * nr + nt

    with jax.named_scope("barr"):
        @pl.when(jnp.logical_and(here, r == hub))
        def _():
            pl.semaphore_wait(barrier, greeted - 1)

        @pl.when(jnp.logical_or(away, r != hub))
        def _():
            pl.semaphore_wait(barrier, greeted)

    def span(c):
        return pl.ds(base[c], plan[c])

    for c in range(chunks):
        for tt in reversed(range(nt)):
            @pl.when(jnp.logical_not(jnp.logical_and(jnp.logical_and(here, t == tt), r == hub)))
            def _():
                send(rt.at[span(c)], xs.at[r, xe, span(c)], x_s, x_r.at[r, c], (t, tt, hub))
        if c == 0:
            for load in first[1:]:
                load.wait()
            meta_ref[...] = jnp.concatenate(
                [ids_ref[...].astype(F32), gates_ref[...], jnp.zeros((4, tok), F32)], axis=0)
            for d in range(1, nx):
                send(meta_ref, meta.at[xe], me_s, me_r, (xe ^ d, t, r))
    send(tin_hbm, own_rows(tin, r), t_s, t_r, partner)
    meta[xe] = meta_ref[...]

    @pl.when(jnp.logical_and(here, r == hub))
    def _():
        xs[hub, xe] = rt[...]

    def take(c):
        @pl.when(r == hub)
        def _():
            for k in range(hub):
                got(xs.at[k, :, span(c)], x_r.at[k, c])

            @pl.when(here)
            def _():
                got(xs.at[hub, pl.ds(0, nx - 1), span(c)], x_r.at[hub, c])

            @pl.when(away)
            def _():
                got(xs.at[hub, :, span(c)], x_r.at[hub, c])
            send(xs.at[:, :, span(c)], xs.at[:, :, span(c)], q_s, q_r.at[c], partner)

    with jax.named_scope("take0"):
        take(0)
    with jax.named_scope("meta"):
        got(meta.at[pl.ds(0, nx - 1)], me_r)
        info = [meta[b].T for b in range(nx)]

    def column(c, j):
        return jnp.concatenate(
            [info[b][offs[c]:offs[c] + subs[c], j:j + 1] for b in range(nx)], axis=0)

    near = (1, 2)

    def picks(c, k=None):
        if k is None:
            return pl.ds(2 * offs[c], 2 * subs[c])
        return pl.ds(2 * offs[c] + k * subs[c], subs[c])

    def up_chunk(c):
        sub = subs[c]
        @pl.when(r != hub)
        def _():
            got(xs.at[:, :, span(c)], q_r.at[c])
        if c == 0:
            loads[0].wait()
        from_chunk = c if extra[c] else c - 1
        tail_at = base[from_chunk] + subs[from_chunk]
        first_unit = starts[c] % nr
        rows = []
        for k in range(nr):
            parts = []
            for b in range(nx):
                main = xs[k, b, base[c]:base[c] + sub, :]
                side = xs[k, b, tail_at:tail_at + unit, :]
                side = [side[:, u * rem:(u + 1) * rem] for u in range(first_unit, first_unit + sizes[c])]
                side = side[0] if len(side) == 1 else jnp.concatenate(side, axis=0)
                parts.append(jnp.concatenate([main, side], axis=1))
            rows.append(jnp.concatenate(parts, axis=0))
        ids = (column(c, 0), column(c, 1))
        for h in range(2):
            picked = [jnp.zeros((nx * sub, hcols), F32)] * 2
            for e in range(experts):
                part = None
                for k in range(nr):
                    one = jnp.dot(rows[k], up[e, k * feat:(k + 1) * feat, h * hcols:(h + 1) * hcols],
                                  preferred_element_type=F32)
                    part = one if part is None else part + one
                picked = [jnp.where(ids[k] == float(e), part, picked[k]) for k in range(2)]
            for k in range(2):
                hp[h, :, picks(c, k), :] = picked[k].astype(BF16).reshape(nx, sub, hcols)
            fa, fb = near[h], near[1 - h]
            for i, q, sem in ((0, xe ^ fa ^ fb, s1_r), (1, xe ^ fa, s2_r)):
                send(hp.at[h, q, picks(c)], r1.at[h, i, picks(c)], s1_s, sem.at[c],
                     (xe ^ fa, t, r))
        if c + 1 < chunks:
            take(c + 1)

    def reduce_first(c, h):
        fa, fb = near[h], near[1 - h]
        if h == 0:
            got(r1.at[:, 0, picks(c)], s1_r.at[c])
        s2[h, picks(c)] = (hp[h, xe ^ fb, picks(c)].astype(F32)
                           + r1[h, 0, picks(c)].astype(F32)).astype(BF16)
        send(s2.at[h, picks(c)], r2.at[h, picks(c)], s2_s, s2_r.at[c], (xe ^ fb, t, r))

    def reduce_second(c, h):
        fa, fb = near[h], near[1 - h]
        if h == 0:
            got(r1.at[:, :, picks(c)], s2_r.at[c])
        total = (hp[h, xe, picks(c)].astype(F32) + r1[h, 1, picks(c)].astype(F32)
                 + r2[h, picks(c)].astype(F32))
        hid[h, xe, picks(c)] = jnp.maximum(total, 0.0).astype(BF16)
        mine_ref = hid.at[h, xe, picks(c)]
        send(mine_ref, mine_ref, h_s.at[0], h_r.at[c, 0], (xe ^ fb, t, r))
        send(mine_ref, mine_ref, h_s.at[0], h_r.at[c, 1], (xe ^ fa, t, r))

    def forward(c, h):
        fa, fb = near[h], near[1 - h]
        ref = hid.at[h, xe ^ fb, picks(c)]
        if h == 0:
            got(hid.at[:, 0, picks(c)], h_r.at[c, 0])
        send(ref, ref, h_s.at[1], h_r.at[c, 1], (xe ^ fa, t, r))

    def collect(c, h):
        if h == 0:
            got(hid.at[:, pl.ds(0, 2), picks(c)], h_r.at[c, 1])

    last = chunks - 1
    own_t = nt - 1

    def to_owner(source):
        for q in range(own_t):
            @pl.when(t != own_t)
            def _():
                send(source(q), ow.at[q, t], o_s, o_r, (xe, own_t, r))

            @pl.when(t == own_t)
            def _():
                ow[q, own_t] = source(q)[...]

    def tower_rows(c):
        loads[2].wait()
        got(own_rows(tin, 1 - r), t_r)

        @pl.when(jnp.logical_and(r == end_core, t != own_t))
        def _():
            send(tin, owt.at[t], w_s, w_r, (xe, own_t, r))

    def share_rows(c):
        @pl.when(jnp.logical_and(r == end_core, t == own_t))
        def _():
            got(owt, w_r)
            send(owt, owt, v_s, v_r, partner)

    end_core = (sum(sizes) - 1) % nr
    final_rows = pl.ds((sum(sizes) - 1) * unit, unit)

    def parity(c):
        return sum(sizes[:c]) % nr if sizes[c] == 1 else None

    def slot(c, core):
        start = sum(sizes[:c])
        if sizes[c] == 1 or start % nr == 0:
            return start // nr
        return start // nr + 1 - core

    def if_core(c, other, body, only=None):
        p = parity(c)
        if p is None:
            if only is None:
                body()
            else:
                pl.when(r == only)(body)
        elif only is None or only == p:
            pl.when(r == (1 - p if other else p))(body)

    def down_chunk(c):
        sub = subs[c]
        ids = (column(c, 0), column(c, 1))
        gates = (column(c, 2), column(c, 3))
        total = jnp.zeros((nx * sub, nr * feat), F32)
        for e in range(experts):
            hit = (ids[0] == float(e), ids[1] == float(e))
            weight = jnp.where(hit[0], gates[0], 0.0) + jnp.where(hit[1], gates[1], 0.0)
            part = None
            for h in range(2):
                values = [hid[h, :, picks(c, k), :].reshape(nx * sub, hcols) for k in range(2)]
                chosen = jnp.where(hit[0], values[0], jnp.where(hit[1], values[1], jnp.zeros_like(values[1])))
                one = lax.dot_general(chosen, down[e, :, h * hcols:(h + 1) * hcols],
                                      (((1,), (1,)), ((), ())), preferred_element_type=F32)
                part = one if part is None else part + one
            total = total + weight * part
        total = total.reshape(nx, sub, nr * feat)
        if c == last:
            dsend0[c] = total.astype(BF16)

            @pl.when(r != end_core)
            def _():
                send(dsend0.at[c, xe], lrec.at[r, xe], l_s, l_r.at[0], partner)
            for d in (3, 1, 2):
                send(dsend0.at[c, xe ^ d], lrec.at[r, xe], l_s, l_r.at[d], (xe ^ d, t, end_core))

            @pl.when(r == end_core)
            def _():
                lrec[r, xe] = dsend0[c, xe]
            return
        if sizes[c] == 1:
            keep = give = total
        else:
            lead = sum(sizes[:c]) % nr
            keep = jnp.where(r == lead, total[:, :unit], total[:, unit:])
            give = jnp.where(r == lead, total[:, unit:], total[:, :unit])

        def store():
            mine[slot(c, r)] = keep

        def give_away():
            at = slot(c, 1 - r)
            dsend0[c] = give.astype(BF16)
            send(dsend0.at[c], drecv0.at[at], p_s, p_r.at[at], partner)
        if_core(c, True, give_away)
        if_core(c, False, store)

    def last_sum(q):
        lsum[q] = (lrec[0, q].astype(F32) + lrec[1, q].astype(F32)).astype(BF16)
        send(lsum.at[q], zl.at[t], zl_s.at[0], zl_r, (xe, q, 1 - r))

        @pl.when(q != t)
        def _():
            send(lsum.at[q], zl.at[t], zl_s.at[1], zl_r, (xe, q, r))

        @pl.when(q == t)
        def _():
            zl[t] = lsum[q]

    def last_own(c):
        @pl.when(r == end_core)
        def _():
            got(lrec.at[1 - r, xe], l_r.at[0])
            last_sum(xe)

    def last_pass():
        for k in reversed(range(nt)):
            q = t ^ k

            @pl.when(q != xe)
            def _():
                got(lrec.at[:, q], l_r.at[q ^ xe])
                last_sum(q)
        to_owner(lambda q: lsum.at[q])

    def last_mixed():
        @pl.when(r == end_core)
        def _():
            got(zl.at[pl.ds(0, nt - 1)], zl_r)

        @pl.when(r != end_core)
        def _():
            got(zl, zl_r)
        total = zl[0].astype(F32)
        for src in range(1, nt):
            total = total + zl[src].astype(F32)
        value = total.astype(BF16)
        rows_out[final_rows, :] = value

    def pair_chunk(c, only=None):
        if c == last:
            return

        def body():
            s = slot(c, r)
            got(drecv0.at[s], p_r.at[s])
            dsend[s] = (mine[s] + drecv0[s].astype(F32)).astype(BF16)
            for d in (3, 1, 2):
                send(dsend.at[s, xe ^ d], gat.at[s, xe], g_s, g_r.at[s], (xe ^ d, t, r))
            gat[s, xe] = dsend[s, xe]

            @pl.when(away)
            def _():
                send(dsend.at[s, xe], zrec.at[s, t], z_s, z_r.at[s], (xe, xe, r))
        if_core(c, False, body, only)

    def pass_chunk(c, only=None):
        if c == last:
            pl.when(r == end_core)(last_pass)
            return

        def body():
            s = slot(c, r)
            got(gat.at[s, pl.ds(0, nx - 1)], g_r.at[s])
            for d in (1, 2, 3):
                q = xe ^ d

                @pl.when(q != t)
                def _():
                    send(gat.at[s, q], zrec.at[s, t], z_s, z_r.at[s], (xe, q, r))
            if c == last - 1:
                to_owner(lambda q: gat.at[s, q])
        if_core(c, False, body, only)

    def mixed_chunk(c, only=None):
        if c == last:
            return last_mixed()

        def body():
            s = slot(c, r)
            got(zrec.at[s, pl.ds(0, nt - 1)], z_r.at[s])
            total = gat[s, t].astype(F32)
            for d in range(1, nt):
                total = total + zrec[s, t ^ d].astype(F32)
            value = total.astype(BF16)
            at = pl.ds(pl.multiple_of((s * nr + r) * unit, unit), unit)
            rows_out[at, :] = value
            send(rows_out.at[at], rows_out.at[at], m_s, m_r, partner)
            if c == last - 1:
                return
            fsend[s] = jnp.dot(value, tin[...], preferred_element_type=F32).astype(BF16)

            @pl.when(t != s)
            def _():
                send(fsend.at[s], frecv.at[t], f_s, f_r, (xe, s, r))
        if_core(c, False, body, only)

    def drain(c):
        sent(r1, s1_s)
        sent(r2, s2_s)
        sent(r1, h_s.at[0])
        sent(r2, h_s.at[1])
        sent(meta.at[pl.ds(0, nx - 1)], me_s)
        sent(own_rows(tin, r), t_s)

        @pl.when(r == hub)
        def _():
            sent(xs, q_s)


        @pl.when(r == end_core)
        def _():
            sent(lrec.at[0, pl.ds(0, nx - 1)], l_s)
            sent(drecv0, p_s)
            sent(gat.at[pl.ds(0, nt - 1), pl.ds(0, nx - 1)], g_s)
            sent(zrec.at[pl.ds(0, nt - 1), pl.ds(0, nt - 1)], z_s)

        @pl.when(r != end_core)
        def _():
            sent(lrec.at[0], l_s)
            sent(drecv0.at[pl.ds(0, nt - 1)], p_s)
            sent(gat.at[:, pl.ds(0, nx - 1)], g_s)
            sent(zrec.at[:, pl.ds(0, nt - 1)], z_s)

        @pl.when(jnp.logical_and(here, r == hub))
        def _():
            sent(xs.at[r, pl.ds(0, nx - 1)], x_s)

        @pl.when(jnp.logical_or(away, r != hub))
        def _():
            sent(xs.at[r], x_s)

    stages = {
        "fw": forward, "rb": reduce_second, "ra": reduce_first, "up": up_chunk, "co": collect,
        "dn": down_chunk, "pr": pair_chunk, "ps": pass_chunk, "mx": mixed_chunk, "drain": drain,
        "pe": last_own, "tw": tower_rows, "tf": share_rows,
    }
    for core in range(nr):
        for name in ("pr", "ps", "mx"):
            stages[f"{name}{core}"] = functools.partial(stages[name], only=core)
    order = []
    n = last
    for i in range(n):
        order += [("up", i), ("ra", i - 1), ("rb", i - 2), ("fw", i - 3)]
    order += [("up", n), ("ra", n - 1), ("rb", n - 2), ("fw", n - 3), ("ra", n), ("co", n - 4), ("dn", n - 4), ("pr0", n - 4),
              ("rb", n - 1), ("fw", n - 2), ("rb", n), ("co", n - 3), ("dn", n - 3), ("pr0", n - 3), ("pr1", n - 4), ("ps0", n - 4),
              ("fw", n - 1), ("fw", n), ("co", n - 2), ("dn", n - 2), ("pr0", n - 2), ("pr1", n - 3), ("ps0", n - 3), ("ps1", n - 4),
              ("co", n - 1), ("dn", n - 1), ("pr0", n - 1), ("pr1", n - 2), ("ps1", n - 3), ("mx0", n - 4), ("mx1", n - 4),
              ("co", n), ("dn", n)]
    order += [("pr1", n - 1), ("ps0", n - 2), ("mx0", n - 3), ("ps0", n - 1), ("mx0", n - 2),
              ("ps1", n - 2), ("pe", n), ("mx1", n - 3), ("ps1", n - 1), ("ps", n),
              ("mx1", n - 2), ("mx0", n - 1), ("mx1", n - 1), ("drain", n), ("mx", n)]
    order.insert(order.index(("up", 2)) + 1, ("tw", last))
    order.insert(order.index(("dn", last)) + 1, ("tf", last))
    for name, c in order:
        if not 0 <= c < chunks or (c == last and name[-1].isdigit()):
            continue
        if name == "dn" and c == 0:
            for load in loads[1:2] + loads[3:]:
                load.wait()
        with jax.named_scope(f"{name}_{c}"):
            if name in ("fw", "rb", "ra", "co"):
                for h in range(2):
                    stages[name](c, h)
            else:
                stages[name](c)
    half = tok // nr
    fewer = half - unit
    with jax.named_scope("mout"):
        @pl.when(r == end_core)
        def _():
            got(rows_out.at[pl.ds(0, half)], m_r)

        @pl.when(r != end_core)
        def _():
            got(rows_out.at[pl.ds(0, fewer)], m_r)
    out = rows_out[...].T
    mixed_ref[...] = jnp.where(r == 0, out[:feat], out[feat:])
    with jax.named_scope("fin"):
        @pl.when(t == own_t)
        def _():
            at = pl.ds(pl.multiple_of((own_t * nr + r) * unit, unit), unit)
            got(ow.at[:, pl.ds(0, nt - 1)], o_r)

            @pl.when(r != end_core)
            def _():
                got(owt, v_r)
            pre = jnp.dot(rows_out[at, :], tin[...], preferred_element_type=F32)
            for q in range(own_t):
                total = ow[q, 0].astype(F32)
                for src in range(1, nt):
                    total = total + ow[q, src].astype(F32)
                pre = pre + jnp.dot(total.astype(BF16), owt[q], preferred_element_type=F32)
            pre_ref[...] = pre

        @pl.when(t != own_t)
        def _():
            got(frecv.at[pl.ds(0, nt - 1)], f_r)
            pre = fsend[t].astype(F32)
            for d in range(1, nt):
                pre = pre + frecv[t ^ d].astype(F32)
            pre_ref[...] = pre
        pre = pre_ref[...]
    active = jnp.maximum(pre + bias_ref[...].reshape(1, tasks * th), 0.0)
    outs = []
    for j in range(tasks):
        outs.append(jnp.sum(active[:, j * th:(j + 1) * th] * tout_ref[j:j + 1, :], axis=1, keepdims=True))
    lane = lax.broadcasted_iota(jnp.int32, (unit, 128), 1)
    logits = jnp.zeros((unit, 128), F32)
    for j in range(tasks):
        logits = jnp.where(lane == j, outs[j] + ob_ref[j], logits)
    scores_ref[...] = jax.nn.sigmoid(logits.T[:tasks, :])
    with jax.named_scope("end"):
        @pl.when(r == end_core)
        def _():
            sent(zrec.at[0], zl_s.at[0])
            sent(zrec.at[1, pl.ds(0, nt - 1)], zl_s.at[1])
            sent(rows_out.at[pl.ds(0, fewer)], m_s)

        @pl.when(r != end_core)
        def _():
            sent(rows_out.at[pl.ds(0, half)], m_s)
        @pl.when(t == own_t)
        def _():
            sent(frecv.at[pl.ds(0, nt - 1)], f_s)

        @pl.when(t != own_t)
        def _():
            sent(frecv.at[pl.ds(0, nt - 2)], f_s)
            sent(ow.at[0, pl.ds(0, nt - 1)], o_s)

        @pl.when(jnp.logical_and(r == end_core, t == own_t))
        def _():
            sent(owt, v_s)

        @pl.when(jnp.logical_and(r == end_core, t != own_t))
        def _():
            sent(tin, w_s)


def emit_kernel(mixed_in, scores_in, mixed_out, scores_out, sem):
    copies = [
        pltpu.make_async_copy(mixed_in, mixed_out, sem.at[0]),
        pltpu.make_async_copy(scores_in, scores_out, sem.at[1]),
    ]
    for copy in copies:
        copy.start()
    for copy in copies:
        copy.wait()


def stay_device(requests, expert_ids, gate_values, w_up, w_down, tower_in, tower_bias, tower_out,
                out_bias):
    nx, nt, nr = lax.axis_size("expert"), lax.axis_size("tensor"), lax.axis_size("rep")
    experts, _, hid_cols = w_up.shape
    tok, feat = requests.shape
    tasks, th = tower_out.shape
    hcols = hid_cols // 2
    unit = tok // (nt * nr)
    sizes = (nr,) * (nt - 1) + (1,) * nr
    C = len(sizes)
    dims = (nx, nt, nr, experts, tok, feat, hcols, tasks, th, unit, sizes)
    vmem = pl.BlockSpec(memory_space=pltpu.VMEM)
    hbm = pl.BlockSpec(memory_space=pltpu.HBM)
    smem = pl.BlockSpec(memory_space=pltpu.SMEM)
    dma = pltpu.SemaphoreType.DMA
    wide = nr * feat
    scratch = [
        pltpu.VMEM((feat, tok), BF16), pltpu.VMEM((2, tok), jnp.int32), pltpu.VMEM((2, tok), F32),
        pltpu.VMEM(tower_bias.shape, F32), pltpu.VMEM(tower_out.shape, F32),
        pltpu.VMEM(w_up.shape, BF16), pltpu.VMEM(w_down.shape, BF16),
        pltpu.VMEM((wide, tower_in.shape[1]), BF16),
        pltpu.VMEM((8, tok), F32), pltpu.VMEM((nx, 8, tok), F32),
        pltpu.VMEM((tok * feat // 128, 128), BF16), pltpu.VMEM((nr, nx, tok * feat // 128, 128), BF16),
        pltpu.VMEM((2, nx, 2 * tok, hcols), BF16),
        pltpu.VMEM((2, 2, 2 * tok, hcols), BF16),
        pltpu.VMEM((2, 2 * tok, hcols), BF16), pltpu.VMEM((2, 2 * tok, hcols), BF16),
        pltpu.VMEM((2, nx, 2 * tok, hcols), BF16),
        pltpu.VMEM((nt, nx, unit, wide), F32), pltpu.VMEM((C, nx, unit, wide), BF16),
        pltpu.VMEM((nt, nx, unit, wide), BF16), pltpu.VMEM((nt, nx, unit, wide), BF16),
        pltpu.VMEM((nt, nx, unit, wide), BF16), pltpu.VMEM((nt, nt, unit, wide), BF16),
        pltpu.VMEM((nt, unit, tasks * th), BF16), pltpu.VMEM((nt, unit, tasks * th), BF16),
        pltpu.VMEM((tok, wide), BF16),
        pltpu.VMEM((nr, nx, unit, wide), BF16), pltpu.VMEM((nx, unit, wide), BF16),
        pltpu.VMEM((nt, unit, wide), BF16),
        pltpu.VMEM((nt - 1, nt, unit, wide), BF16),
        pltpu.VMEM((nt - 1, wide, tower_in.shape[1]), BF16),
        pltpu.VMEM((unit, tower_in.shape[1]), F32),
        dma((8,)), dma, dma, dma, dma((nr, C)), dma, dma((C,)),
        dma, dma((C,)), dma, dma((C,)), dma((2,)), dma((C, 2)),
        dma, dma((nt,)), dma, dma((nt,)), dma, dma((nt,)), dma, dma, dma, dma, dma, dma,
        dma, dma((nx,)), dma((2,)), dma, dma, dma, dma, dma, dma, dma,
    ]
    mixed, scores = pl.pallas_call(
        functools.partial(stay_kernel, dims),
        out_shape=(pltpu.VMEM((feat, tok), BF16), pltpu.VMEM((tasks, unit), F32)),
        in_specs=[hbm] * 8 + [smem],
        out_specs=(vmem, vmem),
        scratch_shapes=scratch,
        compiler_params=pltpu.CompilerParams(
            has_side_effects=True, collective_id=0, vmem_limit_bytes=60 << 20),
        name="stay",
    )(requests.T, expert_ids.T, gate_values.T, w_up, w_down, tower_in, tower_bias, tower_out, out_bias)
    mixed, scores = pl.pallas_call(
        emit_kernel,
        out_shape=(jax.ShapeDtypeStruct(mixed.shape, BF16), jax.ShapeDtypeStruct(scores.shape, F32)),
        in_specs=[vmem, vmem],
        out_specs=(hbm, hbm),
        scratch_shapes=[dma((2,))],
        name="emit",
    )(pltpu.with_memory_space_constraint(mixed, pltpu.VMEM), pltpu.with_memory_space_constraint(scores, pltpu.VMEM))
    return mixed.T, scores


def weights_stay(mesh):
    return mesh.shape["expert"] == 4 and mesh.shape["tensor"] == 4 and mesh.shape["rep"] == 2


def tower_head(pre, tower_bias, tower_out, out_bias):
    active = jax.nn.relu(pre + tower_bias[None, :])
    active = active.reshape(pre.shape[0], tower_out.shape[0], tower_out.shape[1])
    logits = jnp.sum(active * tower_out[None, :, :], axis=2) + out_bias[None, :]
    return jax.nn.sigmoid(logits).T


def per_device(
    requests, expert_ids, gate_values, w_up, w_down, tower_in, tower_bias, tower_out, out_bias
):
    groups = lax.axis_size("expert")
    experts = w_up.shape[0]
    local_experts = experts // groups
    tok_rows = requests.shape[0]
    capacity = 3 * tok_rows // experts
    serve_up, serve_down = (
        lax.all_to_all(w_up, "expert", split_axis=0, concat_axis=1, tiled=True),
        lax.all_to_all(w_down, "expert", split_axis=0, concat_axis=1, tiled=True),
    )
    flat_ids = expert_ids.reshape(-1)
    onehot = (flat_ids[:, None] == jnp.arange(experts, dtype=jnp.int32)[None, :]).astype(jnp.int32)
    before = jnp.cumsum(onehot, axis=0) - onehot
    slot_rank = jnp.sum(before * onehot, axis=1)
    slots = (flat_ids * capacity + slot_rank).reshape(tok_rows, 2)
    slot_index = jnp.arange(experts * capacity, dtype=jnp.int32)
    spread = (
        (slot_index[:, None] == slots[None, :, 0]) | (slot_index[:, None] == slots[None, :, 1])
    ).astype(jnp.bfloat16)
    full_rows = lax.all_gather(requests, ("tensor", "rep"), axis=1, tiled=True)
    outgoing = jnp.dot(spread, full_rows, preferred_element_type=jnp.float32).astype(jnp.bfloat16)
    incoming = lax.all_to_all(outgoing, "expert", split_axis=0, concat_axis=0, tiled=True)
    shaped = incoming.reshape(groups, local_experts, capacity, incoming.shape[1])
    hidden_pre = jnp.einsum("secd,edh->sech", shaped, serve_up, preferred_element_type=jnp.float32)
    hidden = jax.nn.relu(hidden_pre).astype(jnp.bfloat16)
    partial_value = jnp.einsum(
        "sech,edh->secd", hidden, serve_down, preferred_element_type=jnp.float32
    )
    summed = lax.psum_scatter(
        partial_value.astype(jnp.bfloat16), ("tensor", "rep"), scatter_dimension=3, tiled=True
    ).astype(jnp.float32)
    expert_out = summed.astype(jnp.bfloat16).reshape(
        groups * local_experts * capacity, summed.shape[3]
    )
    returned = lax.all_to_all(expert_out, "expert", split_axis=0, concat_axis=0, tiled=True)
    pick_first = (slots[:, 0:1] == slot_index[None, :]).astype(jnp.bfloat16)
    pick_second = (slots[:, 1:2] == slot_index[None, :]).astype(jnp.bfloat16)
    first = jnp.dot(pick_first, returned, preferred_element_type=jnp.float32)
    second = jnp.dot(pick_second, returned, preferred_element_type=jnp.float32)
    mixed = (gate_values[:, 0:1] * first + gate_values[:, 1:2] * second).astype(jnp.bfloat16)
    pre = lax.psum_scatter(
        jnp.dot(mixed, tower_in, preferred_element_type=jnp.float32).astype(jnp.bfloat16),
        ("tensor", "rep"),
        scatter_dimension=0,
        tiled=True,
    ).astype(jnp.float32)
    scores = tower_head(pre, tower_bias, tower_out, out_bias)
    return (mixed, scores)


def solution(mesh):
    in_specs = (
        P("expert", ("tensor", "rep")),
        P("expert", None),
        P("expert", None),
        P(None, "expert", ("tensor", "rep")),
        P(None, "expert", ("tensor", "rep")),
        P(("tensor", "rep"), None),
        P(),
        P(),
        P(),
    )
    out_specs = (P("expert", ("tensor", "rep")), P(None, ("expert", "tensor", "rep")))
    body = stay_device if weights_stay(mesh) else per_device
    return jax.shard_map(
        body, mesh=mesh, in_specs=in_specs, out_specs=out_specs, check_vma=False
    )
```

```python
import functools
import jax
import jax.numpy as jnp
from jax import lax
from jax.experimental import pallas as pl
from jax.experimental.pallas import tpu as pltpu
from jax.sharding import PartitionSpec as P

MESH = pl.DeviceIdType.MESH
F32 = jnp.float32
BF16 = jnp.bfloat16


def stay_kernel(
    dims, req_hbm, ids_hbm, gates_hbm, up_hbm, down_hbm, tin_hbm, bias_hbm, tout_hbm, ob_ref,
    mixed_ref, scores_ref,
    req_ref, ids_ref, gates_ref, bias_ref, tout_ref, up, down, tin, meta_ref, meta, rt, xs,
    hp, r1, s2, r2, hid, mine, dsend0, drecv0, dsend, gat, zrec, fsend, frecv, rows_out, lrec, lsum, zl, ow, owt, pre_ref,
    lsem, me_s, me_r, x_s, x_r, q_s, q_r, s1_s, s1_r, s2_s, s2_r, h_s, h_r,
    p_s, p_r, g_s, g_r, z_s, z_r, m_s, m_r, t_s, t_r, f_s, f_r, l_s, l_r, zl_s, zl_r, o_s, o_r, w_s, w_r, v_s, v_r,
):
    nx, nt, nr, experts, tok, feat, hcols, tasks, th, unit, sizes = dims
    xe, t, r = lax.axis_index("expert"), lax.axis_index("tensor"), lax.axis_index("rep")
    chunks = len(sizes)
    offs = [sum(sizes[:c]) * unit for c in range(chunks)]
    low = feat // 128 * 128
    rem = feat - low
    starts = [sum(sizes[:c]) for c in range(chunks)]
    extra = [unit if n > 1 or start % nr == 0 else 0 for n, start in zip(sizes, starts)]
    plan = [n * unit + e for n, e in zip(sizes, extra)]
    base = [sum(plan[:c]) for c in range(chunks)]
    subs = [n * unit for n in sizes]

    def remote(src, dst, ssem, rsem, dev):
        return pltpu.make_async_remote_copy(
            src_ref=src, dst_ref=dst, send_sem=ssem, recv_sem=rsem, device_id=dev,
            device_id_type=MESH)

    def send(src, dst, ssem, rsem, dev):
        remote(src, dst, ssem, rsem, dev).start()

    def got(ref, rsem):
        remote(ref, ref, lsem.at[0], rsem, (xe, t, r)).wait_recv()

    def sent(ref, ssem):
        remote(ref, ref, ssem, lsem.at[0], (xe, t, r)).wait_send()

    first = [
        pltpu.make_async_copy(req_hbm, req_ref, lsem.at[3]),
        pltpu.make_async_copy(ids_hbm, ids_ref, lsem.at[4]),
        pltpu.make_async_copy(gates_hbm, gates_ref, lsem.at[5]),
    ]

    def own_rows(ref, k):
        return ref.at[pl.ds(pl.multiple_of(k * feat, feat), feat)]

    loads = [
        pltpu.make_async_copy(up_hbm, up, lsem.at[0]),
        pltpu.make_async_copy(down_hbm, down, lsem.at[1]),
        pltpu.make_async_copy(tin_hbm, own_rows(tin, r), lsem.at[2]),
        pltpu.make_async_copy(bias_hbm, bias_ref, lsem.at[6]),
        pltpu.make_async_copy(tout_hbm, tout_ref, lsem.at[7]),
    ]
    first[0].start()
    here = t == xe
    away = jnp.logical_not(here)
    partner = (xe, t, 1 - r)
    barrier = pltpu.get_barrier_semaphore()

    def greet(dev):
        pl.semaphore_signal(barrier, inc=1, device_id=dev, device_id_type=MESH)

    hub = nr - 1

    @pl.when(r == hub)
    def _():
        for b in range(nx):
            for k in range(hub):
                greet((b, xe, k))

            @pl.when(jnp.logical_not(jnp.logical_and(here, xe == b)))
            def _():
                greet((b, xe, hub))
    me = t * nr + r
    for d in reversed(range(1, nt * nr)):
        other = me ^ d
        greet((xe, lax.div(other, nr), lax.rem(other, nr)))
    for d in range(1, nx):
        for k in range(nr):
            greet((xe ^ d, t, k))
    for load in first[1:] + loads:
        load.start()
    first[0].wait()
    full = req_ref[...].T
    for c in range(chunks):
        rt[base[c]:base[c] + subs[c], :] = full[offs[c]:offs[c] + subs[c], :low]
        if extra[c]:
            rt[base[c] + subs[c]:base[c] + plan[c], :] = jnp.concatenate(
                [full[offs[c] + k * unit:offs[c] + (k + 1) * unit, low:] for k in range(nr)], axis=1)
    greeted = (nt * nr - 1) + (nx - 1) * nr + nt

    with jax.named_scope("barr"):
        @pl.when(jnp.logical_and(here, r == hub))
        def _():
            pl.semaphore_wait(barrier, greeted - 1)

        @pl.when(jnp.logical_or(away, r != hub))
        def _():
            pl.semaphore_wait(barrier, greeted)

    def span(c):
        return pl.ds(base[c], plan[c])

    for c in range(chunks):
        for tt in reversed(range(nt)):
            @pl.when(jnp.logical_not(jnp.logical_and(jnp.logical_and(here, t == tt), r == hub)))
            def _():
                send(rt.at[span(c)], xs.at[r, xe, span(c)], x_s, x_r.at[r, c], (t, tt, hub))
        if c == 0:
            for load in first[1:]:
                load.wait()
            meta_ref[...] = jnp.concatenate(
                [ids_ref[...].astype(F32), gates_ref[...], jnp.zeros((4, tok), F32)], axis=0)
            for d in range(1, nx):
                send(meta_ref, meta.at[xe], me_s, me_r, (xe ^ d, t, r))
    send(tin_hbm, own_rows(tin, r), t_s, t_r, partner)
    meta[xe] = meta_ref[...]

    @pl.when(jnp.logical_and(here, r == hub))
    def _():
        xs[hub, xe] = rt[...]

    def take(c):
        @pl.when(r == hub)
        def _():
            for k in range(hub):
                got(xs.at[k, :, span(c)], x_r.at[k, c])

            @pl.when(here)
            def _():
                got(xs.at[hub, pl.ds(0, nx - 1), span(c)], x_r.at[hub, c])

            @pl.when(away)
            def _():
                got(xs.at[hub, :, span(c)], x_r.at[hub, c])
            send(xs.at[:, :, span(c)], xs.at[:, :, span(c)], q_s, q_r.at[c], partner)

    with jax.named_scope("take0"):
        take(0)
    with jax.named_scope("meta"):
        got(meta.at[pl.ds(0, nx - 1)], me_r)
        info = [meta[b].T for b in range(nx)]

    def column(c, j):
        return jnp.concatenate(
            [info[b][offs[c]:offs[c] + subs[c], j:j + 1] for b in range(nx)], axis=0)

    near = (1, 2)

    def picks(c, k=None):
        if k is None:
            return pl.ds(2 * offs[c], 2 * subs[c])
        return pl.ds(2 * offs[c] + k * subs[c], subs[c])

    def up_chunk(c):
        sub = subs[c]
        @pl.when(r != hub)
        def _():
            got(xs.at[:, :, span(c)], q_r.at[c])
        if c == 0:
            loads[0].wait()
        from_chunk = c if extra[c] else c - 1
        tail_at = base[from_chunk] + subs[from_chunk]
        first_unit = starts[c] % nr
        rows = []
        for k in range(nr):
            parts = []
            for b in range(nx):
                main = xs[k, b, base[c]:base[c] + sub, :]
                side = xs[k, b, tail_at:tail_at + unit, :]
                side = [side[:, u * rem:(u + 1) * rem] for u in range(first_unit, first_unit + sizes[c])]
                side = side[0] if len(side) == 1 else jnp.concatenate(side, axis=0)
                parts.append(jnp.concatenate([main, side], axis=1))
            rows.append(jnp.concatenate(parts, axis=0))
        ids = (column(c, 0), column(c, 1))
        for h in range(2):
            picked = [jnp.zeros((nx * sub, hcols), F32)] * 2
            for e in range(experts):
                part = None
                for k in range(nr):
                    one = jnp.dot(rows[k], up[e, k * feat:(k + 1) * feat, h * hcols:(h + 1) * hcols],
                                  preferred_element_type=F32)
                    part = one if part is None else part + one
                picked = [jnp.where(ids[k] == float(e), part, picked[k]) for k in range(2)]
            for k in range(2):
                hp[h, :, picks(c, k), :] = picked[k].astype(BF16).reshape(nx, sub, hcols)
            fa, fb = near[h], near[1 - h]
            for i, q, sem in ((0, xe ^ fa ^ fb, s1_r), (1, xe ^ fa, s2_r)):
                send(hp.at[h, q, picks(c)], r1.at[h, i, picks(c)], s1_s, sem.at[c],
                     (xe ^ fa, t, r))
        if c + 1 < chunks:
            take(c + 1)

    def reduce_first(c, h):
        fa, fb = near[h], near[1 - h]
        if h == 0:
            got(r1.at[:, 0, picks(c)], s1_r.at[c])
        s2[h, picks(c)] = (hp[h, xe ^ fb, picks(c)].astype(F32)
                           + r1[h, 0, picks(c)].astype(F32)).astype(BF16)
        send(s2.at[h, picks(c)], r2.at[h, picks(c)], s2_s, s2_r.at[c], (xe ^ fb, t, r))

    def reduce_second(c, h):
        fa, fb = near[h], near[1 - h]
        if h == 0:
            got(r1.at[:, :, picks(c)], s2_r.at[c])
        total = (hp[h, xe, picks(c)].astype(F32) + r1[h, 1, picks(c)].astype(F32)
                 + r2[h, picks(c)].astype(F32))
        hid[h, xe, picks(c)] = jnp.maximum(total, 0.0).astype(BF16)
        mine_ref = hid.at[h, xe, picks(c)]
        send(mine_ref, mine_ref, h_s.at[0], h_r.at[c, 0], (xe ^ fb, t, r))
        send(mine_ref, mine_ref, h_s.at[0], h_r.at[c, 1], (xe ^ fa, t, r))

    def forward(c, h):
        fa, fb = near[h], near[1 - h]
        ref = hid.at[h, xe ^ fb, picks(c)]
        if h == 0:
            got(hid.at[:, 0, picks(c)], h_r.at[c, 0])
        send(ref, ref, h_s.at[1], h_r.at[c, 1], (xe ^ fa, t, r))

    def collect(c, h):
        if h == 0:
            got(hid.at[:, pl.ds(0, 2), picks(c)], h_r.at[c, 1])

    last = chunks - 1
    own_t = nt - 1

    def to_owner(source):
        for q in range(own_t):
            @pl.when(t != own_t)
            def _():
                send(source(q), ow.at[q, t], o_s, o_r, (xe, own_t, r))

            @pl.when(t == own_t)
            def _():
                ow[q, own_t] = source(q)[...]

    def tower_rows(c):
        loads[2].wait()
        got(own_rows(tin, 1 - r), t_r)

        @pl.when(jnp.logical_and(r == end_core, t != own_t))
        def _():
            send(tin, owt.at[t], w_s, w_r, (xe, own_t, r))

    def share_rows(c):
        @pl.when(jnp.logical_and(r == end_core, t == own_t))
        def _():
            got(owt, w_r)
            send(owt, owt, v_s, v_r, partner)

    end_core = (sum(sizes) - 1) % nr
    final_rows = pl.ds((sum(sizes) - 1) * unit, unit)

    def parity(c):
        return sum(sizes[:c]) % nr if sizes[c] == 1 else None

    def slot(c, core):
        start = sum(sizes[:c])
        if sizes[c] == 1 or start % nr == 0:
            return start // nr
        return start // nr + 1 - core

    def if_core(c, other, body, only=None):
        p = parity(c)
        if p is None:
            if only is None:
                body()
            else:
                pl.when(r == only)(body)
        elif only is None or only == p:
            pl.when(r == (1 - p if other else p))(body)

    def down_chunk(c):
        sub = subs[c]
        ids = (column(c, 0), column(c, 1))
        gates = (column(c, 2), column(c, 3))
        total = jnp.zeros((nx * sub, nr * feat), F32)
        for e in range(experts):
            hit = (ids[0] == float(e), ids[1] == float(e))
            weight = jnp.where(hit[0], gates[0], 0.0) + jnp.where(hit[1], gates[1], 0.0)
            part = None
            for h in range(2):
                values = [hid[h, :, picks(c, k), :].reshape(nx * sub, hcols) for k in range(2)]
                chosen = jnp.where(hit[0], values[0], jnp.where(hit[1], values[1], jnp.zeros_like(values[1])))
                one = lax.dot_general(chosen, down[e, :, h * hcols:(h + 1) * hcols],
                                      (((1,), (1,)), ((), ())), preferred_element_type=F32)
                part = one if part is None else part + one
            total = total + weight * part
        total = total.reshape(nx, sub, nr * feat)
        if c == last:
            dsend0[c] = total.astype(BF16)
            for d in (3, 1, 2):
                send(dsend0.at[c, xe ^ d], lrec.at[r, xe], l_s, l_r.at[d], (xe ^ d, t, end_core))

            @pl.when(r == end_core)
            def _():
                lrec[r, xe] = dsend0[c, xe]

            @pl.when(r != end_core)
            def _():
                send(dsend0.at[c, xe], lrec.at[r, xe], l_s, l_r.at[0], partner)
            return
        if sizes[c] == 1:
            keep = give = total
        else:
            lead = sum(sizes[:c]) % nr
            keep = jnp.where(r == lead, total[:, :unit], total[:, unit:])
            give = jnp.where(r == lead, total[:, unit:], total[:, :unit])

        def store():
            mine[slot(c, r)] = keep

        def give_away():
            at = slot(c, 1 - r)
            dsend0[c] = give.astype(BF16)
            send(dsend0.at[c], drecv0.at[at], p_s, p_r.at[at], partner)
        if_core(c, True, give_away)
        if_core(c, False, store)

    def last_sum(q):
        lsum[q] = (lrec[0, q].astype(F32) + lrec[1, q].astype(F32)).astype(BF16)
        send(lsum.at[q], zl.at[t], zl_s.at[0], zl_r, (xe, q, 1 - r))

        @pl.when(q != t)
        def _():
            send(lsum.at[q], zl.at[t], zl_s.at[1], zl_r, (xe, q, r))

        @pl.when(q == t)
        def _():
            zl[t] = lsum[q]

    def last_own(c):
        @pl.when(r == end_core)
        def _():
            got(lrec.at[1 - r, xe], l_r.at[0])
            last_sum(xe)

    def last_pass():
        for k in reversed(range(nt)):
            q = t ^ k

            @pl.when(q != xe)
            def _():
                got(lrec.at[:, q], l_r.at[q ^ xe])
                last_sum(q)
        to_owner(lambda q: lsum.at[q])

    def last_mixed():
        @pl.when(r == end_core)
        def _():
            got(zl.at[pl.ds(0, nt - 1)], zl_r)

        @pl.when(r != end_core)
        def _():
            got(zl, zl_r)
        total = zl[0].astype(F32)
        for src in range(1, nt):
            total = total + zl[src].astype(F32)
        value = total.astype(BF16)
        rows_out[final_rows, :] = value

    def pair_chunk(c, only=None):
        if c == last:
            return

        def body():
            s = slot(c, r)
            got(drecv0.at[s], p_r.at[s])
            dsend[s] = (mine[s] + drecv0[s].astype(F32)).astype(BF16)
            for d in (3, 1, 2):
                send(dsend.at[s, xe ^ d], gat.at[s, xe], g_s, g_r.at[s], (xe ^ d, t, r))
            gat[s, xe] = dsend[s, xe]

            @pl.when(away)
            def _():
                send(dsend.at[s, xe], zrec.at[s, t], z_s, z_r.at[s], (xe, xe, r))
        if_core(c, False, body, only)

    def pass_chunk(c, only=None):
        if c == last:
            pl.when(r == end_core)(last_pass)
            return

        def body():
            s = slot(c, r)
            got(gat.at[s, pl.ds(0, nx - 1)], g_r.at[s])
            for d in (1, 2, 3):
                q = xe ^ d

                @pl.when(q != t)
                def _():
                    send(gat.at[s, q], zrec.at[s, t], z_s, z_r.at[s], (xe, q, r))
            if c == last - 1:
                to_owner(lambda q: gat.at[s, q])
        if_core(c, False, body, only)

    def mixed_chunk(c, only=None):
        if c == last:
            return last_mixed()

        def body():
            s = slot(c, r)
            got(zrec.at[s, pl.ds(0, nt - 1)], z_r.at[s])
            total = gat[s, t].astype(F32)
            for d in range(1, nt):
                total = total + zrec[s, t ^ d].astype(F32)
            value = total.astype(BF16)
            at = pl.ds(pl.multiple_of((s * nr + r) * unit, unit), unit)
            rows_out[at, :] = value
            send(rows_out.at[at], rows_out.at[at], m_s, m_r, partner)
            if c == last - 1:
                return
            fsend[s] = jnp.dot(value, tin[...], preferred_element_type=F32).astype(BF16)

            @pl.when(t != s)
            def _():
                send(fsend.at[s], frecv.at[t], f_s, f_r, (xe, s, r))
        if_core(c, False, body, only)

    def drain(c):
        sent(r1, s1_s)
        sent(r2, s2_s)
        sent(r1, h_s.at[0])
        sent(r2, h_s.at[1])
        sent(meta.at[pl.ds(0, nx - 1)], me_s)
        sent(own_rows(tin, r), t_s)

        @pl.when(r == hub)
        def _():
            sent(xs, q_s)


        @pl.when(r == end_core)
        def _():
            sent(lrec.at[0, pl.ds(0, nx - 1)], l_s)
            sent(drecv0, p_s)
            sent(gat.at[pl.ds(0, nt - 1), pl.ds(0, nx - 1)], g_s)
            sent(zrec.at[pl.ds(0, nt - 1), pl.ds(0, nt - 1)], z_s)

        @pl.when(r != end_core)
        def _():
            sent(lrec.at[0], l_s)
            sent(drecv0.at[pl.ds(0, nt - 1)], p_s)
            sent(gat.at[:, pl.ds(0, nx - 1)], g_s)
            sent(zrec.at[:, pl.ds(0, nt - 1)], z_s)

        @pl.when(jnp.logical_and(here, r == hub))
        def _():
            sent(xs.at[r, pl.ds(0, nx - 1)], x_s)

        @pl.when(jnp.logical_or(away, r != hub))
        def _():
            sent(xs.at[r], x_s)

    stages = {
        "fw": forward, "rb": reduce_second, "ra": reduce_first, "up": up_chunk, "co": collect,
        "dn": down_chunk, "pr": pair_chunk, "ps": pass_chunk, "mx": mixed_chunk, "drain": drain,
        "pe": last_own, "tw": tower_rows, "tf": share_rows,
    }
    for core in range(nr):
        for name in ("pr", "ps", "mx"):
            stages[f"{name}{core}"] = functools.partial(stages[name], only=core)
    order = []
    n = last
    for i in range(n):
        order += [("up", i), ("ra", i - 1), ("rb", i - 2), ("fw", i - 3)]
    order += [("up", n), ("ra", n - 1), ("rb", n - 2), ("fw", n - 3), ("ra", n), ("co", n - 4), ("dn", n - 4), ("pr0", n - 4),
              ("rb", n - 1), ("fw", n - 2), ("rb", n), ("co", n - 3), ("dn", n - 3), ("pr0", n - 3), ("pr1", n - 4), ("ps0", n - 4),
              ("fw", n - 1), ("fw", n), ("co", n - 2), ("dn", n - 2), ("pr0", n - 2), ("pr1", n - 3), ("ps0", n - 3), ("ps1", n - 4),
              ("co", n - 1), ("dn", n - 1), ("pr0", n - 1), ("pr1", n - 2), ("ps1", n - 3), ("mx0", n - 4), ("mx1", n - 4),
              ("co", n), ("dn", n)]
    order += [("pr1", n - 1), ("ps0", n - 2), ("ps1", n - 2), ("mx0", n - 3), ("ps0", n - 1), ("mx0", n - 2), ("mx1", n - 3),
              ("ps1", n - 1), ("pe", n), ("mx1", n - 2), ("ps", n), ("mx0", n - 1), ("mx1", n - 1), ("drain", n), ("mx", n)]
    order.insert(order.index(("up", 2)) + 1, ("tw", last))
    order.insert(order.index(("dn", last)) + 1, ("tf", last))
    for name, c in order:
        if not 0 <= c < chunks or (c == last and name[-1].isdigit()):
            continue
        if name == "dn" and c == 0:
            for load in loads[1:2] + loads[3:]:
                load.wait()
        with jax.named_scope(f"{name}_{c}"):
            if name in ("fw", "rb", "ra", "co"):
                for h in range(2):
                    stages[name](c, h)
            else:
                stages[name](c)
    half = tok // nr
    fewer = half - unit
    with jax.named_scope("mout"):
        @pl.when(r == end_core)
        def _():
            got(rows_out.at[pl.ds(0, half)], m_r)

        @pl.when(r != end_core)
        def _():
            got(rows_out.at[pl.ds(0, fewer)], m_r)
    out = rows_out[...].T
    mixed_ref[...] = jnp.where(r == 0, out[:feat], out[feat:])
    with jax.named_scope("fin"):
        @pl.when(t == own_t)
        def _():
            at = pl.ds(pl.multiple_of((own_t * nr + r) * unit, unit), unit)
            got(ow.at[:, pl.ds(0, nt - 1)], o_r)

            @pl.when(r != end_core)
            def _():
                got(owt, v_r)
            pre = jnp.dot(rows_out[at, :], tin[...], preferred_element_type=F32)
            for q in range(own_t):
                total = ow[q, 0].astype(F32)
                for src in range(1, nt):
                    total = total + ow[q, src].astype(F32)
                pre = pre + jnp.dot(total.astype(BF16), owt[q], preferred_element_type=F32)
            pre_ref[...] = pre

        @pl.when(t != own_t)
        def _():
            got(frecv.at[pl.ds(0, nt - 1)], f_r)
            pre = fsend[t].astype(F32)
            for d in range(1, nt):
                pre = pre + frecv[t ^ d].astype(F32)
            pre_ref[...] = pre
        pre = pre_ref[...]
    active = jnp.maximum(pre + bias_ref[...].reshape(1, tasks * th), 0.0)
    outs = []
    for j in range(tasks):
        outs.append(jnp.sum(active[:, j * th:(j + 1) * th] * tout_ref[j:j + 1, :], axis=1, keepdims=True))
    lane = lax.broadcasted_iota(jnp.int32, (unit, 128), 1)
    logits = jnp.zeros((unit, 128), F32)
    for j in range(tasks):
        logits = jnp.where(lane == j, outs[j] + ob_ref[j], logits)
    scores_ref[...] = jax.nn.sigmoid(logits.T[:tasks, :])
    with jax.named_scope("end"):
        @pl.when(r == end_core)
        def _():
            sent(zrec.at[0], zl_s.at[0])
            sent(zrec.at[1, pl.ds(0, nt - 1)], zl_s.at[1])
            sent(rows_out.at[pl.ds(0, fewer)], m_s)

        @pl.when(r != end_core)
        def _():
            sent(rows_out.at[pl.ds(0, half)], m_s)
        @pl.when(t == own_t)
        def _():
            sent(frecv.at[pl.ds(0, nt - 1)], f_s)

        @pl.when(t != own_t)
        def _():
            sent(frecv.at[pl.ds(0, nt - 2)], f_s)
            sent(ow.at[0, pl.ds(0, nt - 1)], o_s)

        @pl.when(jnp.logical_and(r == end_core, t == own_t))
        def _():
            sent(owt, v_s)

        @pl.when(jnp.logical_and(r == end_core, t != own_t))
        def _():
            sent(tin, w_s)


def emit_kernel(mixed_in, scores_in, mixed_out, scores_out, sem):
    copies = [
        pltpu.make_async_copy(mixed_in, mixed_out, sem.at[0]),
        pltpu.make_async_copy(scores_in, scores_out, sem.at[1]),
    ]
    for copy in copies:
        copy.start()
    for copy in copies:
        copy.wait()


def stay_device(requests, expert_ids, gate_values, w_up, w_down, tower_in, tower_bias, tower_out,
                out_bias):
    nx, nt, nr = lax.axis_size("expert"), lax.axis_size("tensor"), lax.axis_size("rep")
    experts, _, hid_cols = w_up.shape
    tok, feat = requests.shape
    tasks, th = tower_out.shape
    hcols = hid_cols // 2
    unit = tok // (nt * nr)
    sizes = (nr,) * (nt - 1) + (1,) * nr
    C = len(sizes)
    dims = (nx, nt, nr, experts, tok, feat, hcols, tasks, th, unit, sizes)
    vmem = pl.BlockSpec(memory_space=pltpu.VMEM)
    hbm = pl.BlockSpec(memory_space=pltpu.HBM)
    smem = pl.BlockSpec(memory_space=pltpu.SMEM)
    dma = pltpu.SemaphoreType.DMA
    wide = nr * feat
    scratch = [
        pltpu.VMEM((feat, tok), BF16), pltpu.VMEM((2, tok), jnp.int32), pltpu.VMEM((2, tok), F32),
        pltpu.VMEM(tower_bias.shape, F32), pltpu.VMEM(tower_out.shape, F32),
        pltpu.VMEM(w_up.shape, BF16), pltpu.VMEM(w_down.shape, BF16),
        pltpu.VMEM((wide, tower_in.shape[1]), BF16),
        pltpu.VMEM((8, tok), F32), pltpu.VMEM((nx, 8, tok), F32),
        pltpu.VMEM((tok * feat // 128, 128), BF16), pltpu.VMEM((nr, nx, tok * feat // 128, 128), BF16),
        pltpu.VMEM((2, nx, 2 * tok, hcols), BF16),
        pltpu.VMEM((2, 2, 2 * tok, hcols), BF16),
        pltpu.VMEM((2, 2 * tok, hcols), BF16), pltpu.VMEM((2, 2 * tok, hcols), BF16),
        pltpu.VMEM((2, nx, 2 * tok, hcols), BF16),
        pltpu.VMEM((nt, nx, unit, wide), F32), pltpu.VMEM((C, nx, unit, wide), BF16),
        pltpu.VMEM((nt, nx, unit, wide), BF16), pltpu.VMEM((nt, nx, unit, wide), BF16),
        pltpu.VMEM((nt, nx, unit, wide), BF16), pltpu.VMEM((nt, nt, unit, wide), BF16),
        pltpu.VMEM((nt, unit, tasks * th), BF16), pltpu.VMEM((nt, unit, tasks * th), BF16),
        pltpu.VMEM((tok, wide), BF16),
        pltpu.VMEM((nr, nx, unit, wide), BF16), pltpu.VMEM((nx, unit, wide), BF16),
        pltpu.VMEM((nt, unit, wide), BF16),
        pltpu.VMEM((nt - 1, nt, unit, wide), BF16),
        pltpu.VMEM((nt - 1, wide, tower_in.shape[1]), BF16),
        pltpu.VMEM((unit, tower_in.shape[1]), F32),
        dma((8,)), dma, dma, dma, dma((nr, C)), dma, dma((C,)),
        dma, dma((C,)), dma, dma((C,)), dma((2,)), dma((C, 2)),
        dma, dma((nt,)), dma, dma((nt,)), dma, dma((nt,)), dma, dma, dma, dma, dma, dma,
        dma, dma((nx,)), dma((2,)), dma, dma, dma, dma, dma, dma, dma,
    ]
    mixed, scores = pl.pallas_call(
        functools.partial(stay_kernel, dims),
        out_shape=(pltpu.VMEM((feat, tok), BF16), pltpu.VMEM((tasks, unit), F32)),
        in_specs=[hbm] * 8 + [smem],
        out_specs=(vmem, vmem),
        scratch_shapes=scratch,
        compiler_params=pltpu.CompilerParams(
            has_side_effects=True, collective_id=0, vmem_limit_bytes=60 << 20),
        name="stay",
    )(requests.T, expert_ids.T, gate_values.T, w_up, w_down, tower_in, tower_bias, tower_out, out_bias)
    mixed, scores = pl.pallas_call(
        emit_kernel,
        out_shape=(jax.ShapeDtypeStruct(mixed.shape, BF16), jax.ShapeDtypeStruct(scores.shape, F32)),
        in_specs=[vmem, vmem],
        out_specs=(hbm, hbm),
        scratch_shapes=[dma((2,))],
        name="emit",
    )(pltpu.with_memory_space_constraint(mixed, pltpu.VMEM), pltpu.with_memory_space_constraint(scores, pltpu.VMEM))
    return mixed.T, scores


def weights_stay(mesh):
    return mesh.shape["expert"] == 4 and mesh.shape["tensor"] == 4 and mesh.shape["rep"] == 2


def tower_head(pre, tower_bias, tower_out, out_bias):
    active = jax.nn.relu(pre + tower_bias[None, :])
    active = active.reshape(pre.shape[0], tower_out.shape[0], tower_out.shape[1])
    logits = jnp.sum(active * tower_out[None, :, :], axis=2) + out_bias[None, :]
    return jax.nn.sigmoid(logits).T


def per_device(
    requests, expert_ids, gate_values, w_up, w_down, tower_in, tower_bias, tower_out, out_bias
):
    groups = lax.axis_size("expert")
    experts = w_up.shape[0]
    local_experts = experts // groups
    tok_rows = requests.shape[0]
    capacity = 3 * tok_rows // experts
    serve_up, serve_down = (
        lax.all_to_all(w_up, "expert", split_axis=0, concat_axis=1, tiled=True),
        lax.all_to_all(w_down, "expert", split_axis=0, concat_axis=1, tiled=True),
    )
    flat_ids = expert_ids.reshape(-1)
    onehot = (flat_ids[:, None] == jnp.arange(experts, dtype=jnp.int32)[None, :]).astype(jnp.int32)
    before = jnp.cumsum(onehot, axis=0) - onehot
    slot_rank = jnp.sum(before * onehot, axis=1)
    slots = (flat_ids * capacity + slot_rank).reshape(tok_rows, 2)
    slot_index = jnp.arange(experts * capacity, dtype=jnp.int32)
    spread = (
        (slot_index[:, None] == slots[None, :, 0]) | (slot_index[:, None] == slots[None, :, 1])
    ).astype(jnp.bfloat16)
    full_rows = lax.all_gather(requests, ("tensor", "rep"), axis=1, tiled=True)
    outgoing = jnp.dot(spread, full_rows, preferred_element_type=jnp.float32).astype(jnp.bfloat16)
    incoming = lax.all_to_all(outgoing, "expert", split_axis=0, concat_axis=0, tiled=True)
    shaped = incoming.reshape(groups, local_experts, capacity, incoming.shape[1])
    hidden_pre = jnp.einsum("secd,edh->sech", shaped, serve_up, preferred_element_type=jnp.float32)
    hidden = jax.nn.relu(hidden_pre).astype(jnp.bfloat16)
    partial_value = jnp.einsum(
        "sech,edh->secd", hidden, serve_down, preferred_element_type=jnp.float32
    )
    summed = lax.psum_scatter(
        partial_value.astype(jnp.bfloat16), ("tensor", "rep"), scatter_dimension=3, tiled=True
    ).astype(jnp.float32)
    expert_out = summed.astype(jnp.bfloat16).reshape(
        groups * local_experts * capacity, summed.shape[3]
    )
    returned = lax.all_to_all(expert_out, "expert", split_axis=0, concat_axis=0, tiled=True)
    pick_first = (slots[:, 0:1] == slot_index[None, :]).astype(jnp.bfloat16)
    pick_second = (slots[:, 1:2] == slot_index[None, :]).astype(jnp.bfloat16)
    first = jnp.dot(pick_first, returned, preferred_element_type=jnp.float32)
    second = jnp.dot(pick_second, returned, preferred_element_type=jnp.float32)
    mixed = (gate_values[:, 0:1] * first + gate_values[:, 1:2] * second).astype(jnp.bfloat16)
    pre = lax.psum_scatter(
        jnp.dot(mixed, tower_in, preferred_element_type=jnp.float32).astype(jnp.bfloat16),
        ("tensor", "rep"),
        scatter_dimension=0,
        tiled=True,
    ).astype(jnp.float32)
    scores = tower_head(pre, tower_bias, tower_out, out_bias)
    return (mixed, scores)


def solution(mesh):
    in_specs = (
        P("expert", ("tensor", "rep")),
        P("expert", None),
        P("expert", None),
        P(None, "expert", ("tensor", "rep")),
        P(None, "expert", ("tensor", "rep")),
        P(("tensor", "rep"), None),
        P(),
        P(),
        P(),
    )
    out_specs = (P("expert", ("tensor", "rep")), P(None, ("expert", "tensor", "rep")))
    body = stay_device if weights_stay(mesh) else per_device
    return jax.shard_map(
        body, mesh=mesh, in_specs=in_specs, out_specs=out_specs, check_vma=False
    )
```
